256 devices in a mesh: groups: 4 (over x, y), space: 64 (over z, core).
Axes of the slice: x: 2, y: 2, z: 32, core: 2. Of those that a mesh axis runs over, the one named last changes fastest.
The devices are a block of a 4x8x32 slice.
Arguments:
- hidden: bfloat16 [32768, 512], P(('groups', 'space')), parts along dimension 0, may hold values from -130 to 130
- norm_gain: float32 [512], replicated, may hold values from 0.5 to 2
- norm_shift: float32 [512], replicated, may hold values from -3 to 3
- conv_weight: bfloat16 [3, 3, 3, 512, 512], P(None, None, None, 'space'), may hold values from -0.0546875 to 0.0546875
- conv_bias: bfloat16 [512], replicated, may hold values from -3 to 3
Outputs:
- decoded: bfloat16 [16, 32, 256, 512], P('groups', None, 'space'), parts along dimension 0
The draws below stay inside these ranges and needn't reach their ends.
There are 4 independent parts, one for each index of `groups`. The reference program is written for one: setup_inputs(seed, part) draws one part's arguments, and reference() takes and returns one part's arrays. A program takes and returns all parts, laid end to end along the dimension named above; an argument that names none is the same for every part. Nothing has to cross between parts.
All inputs are finite; a program needn't handle non-finite values.
Results may differ from the reference program's by a relative error of at most 0.0045.
Values may be sent and summed in bfloat16 or wider, within the bound.
A program may use at most 64 MiB of HBM per device.

```python
import math
import jax
import jax.numpy as jnp
from jax import lax

CHANNELS = 512
GROUPS = 32
FRAMES = 4
ROWS = 16
WIDTH = 128
TOKENS = 8192


def draw_hidden(key, part):
    keys = jax.random.split(jax.random.fold_in(key, 11), 3)
    column = (jnp.arange(TOKENS) % WIDTH).astype(jnp.float32)
    ramp = 1.0 + 2.0 * column / max(WIDTH - 1, 1)
    channel_scale = jnp.exp(jax.random.uniform(keys[1], (CHANNELS,), jnp.float32, 0.0, math.log(10.0)))
    channel_mean = jnp.clip(0.5 * jax.random.normal(keys[2], (CHANNELS,), jnp.float32), -1.5, 1.5)
    base = jnp.clip(jax.random.normal(keys[0], (TOKENS, CHANNELS), jnp.float32), -4.0, 4.0)
    return (base * ramp[:, None] * channel_scale[None, :] + channel_mean[None, :]).astype(jnp.bfloat16)


def level_of(own_key, dims, shards, smallest, high):
    factor_of, own = 1.0, jax.random.fold_in(own_key, 6)
    for axis_at, blocks in shards:
        steps = jnp.exp(jax.random.uniform(jax.random.fold_in(own, axis_at), (blocks,), jnp.float32, smallest / len(shards), high / len(shards)))
        factor_of = factor_of * jnp.repeat(steps, dims[axis_at] // blocks).reshape([-1 if axis == axis_at else 1 for axis in range(len(dims))])
    return factor_of


def bell_draw(own_key, shape, scale, bound, shards=(), dtype=jnp.bfloat16):
    values = scale * jax.random.normal(own_key, shape, jnp.float32)
    if shards:
        values = values * level_of(own_key, shape, shards, -0.22, 0.18)
    return jnp.clip(values, -bound, bound).astype(dtype)


def setup_inputs(seed: int = 0, part: int = 0) -> dict:
    streams_of = jax.random.split(jax.random.key(seed), 6)
    part_keys = jax.random.split(jax.random.fold_in(streams_of[5], part), 6)
    return {
        "hidden": draw_hidden(jax.random.fold_in(jax.random.fold_in(streams_of[5], part), 71), part),
        "norm_gain": jnp.clip(jnp.exp(jax.random.uniform(streams_of[1], (CHANNELS,), jnp.float32, math.log(0.5), math.log(2.0))), 0.5, 2.0),
        "norm_shift": bell_draw(streams_of[2], (CHANNELS,), 0.5, 3.0, (), jnp.float32),
        "conv_weight": bell_draw(streams_of[3], (3, 3, 3, CHANNELS, CHANNELS), (27 * CHANNELS) ** -0.5, 0.0546875, ((3, 64),)),
        "conv_bias": bell_draw(streams_of[4], (CHANNELS,), 0.5, 3.0),
    }


EPSILON = 1e-06

def reference(hidden, norm_gain, norm_shift, conv_weight, conv_bias):
    values = hidden.astype(jnp.float32).reshape(FRAMES, ROWS, WIDTH, GROUPS, CHANNELS // GROUPS)
    average = lax.optimization_barrier(jnp.mean(values, axis=(0, 1, 2, 4), keepdims=True))
    spread = lax.optimization_barrier(jnp.mean((values - average) ** 2, axis=(0, 1, 2, 4), keepdims=True))
    normed = ((values - average) * lax.rsqrt(spread + EPSILON)).reshape(FRAMES, ROWS, WIDTH, CHANNELS)
    active = jax.nn.silu(normed * norm_gain + norm_shift).astype(jnp.bfloat16)
    doubled = jnp.repeat(jnp.repeat(active, 2, axis=1), 2, axis=2)
    padded = jnp.pad(doubled, ((2, 0), (1, 1), (1, 1), (0, 0)), mode='edge')
    result = lax.conv_general_dilated(padded[None].astype(jnp.float32), conv_weight.astype(jnp.float32), (1, 1, 1), 'VALID', dimension_numbers=('NDHWC', 'DHWIO', 'NDHWC'))[0]
    return (result + conv_bias.astype(jnp.float32)).astype(jnp.bfloat16)
```

```python
import functools

import jax
import jax.numpy as jnp
from jax import lax
from jax.experimental import pallas as pl
from jax.experimental.pallas import tpu as pltpu
from jax.sharding import PartitionSpec as P

GROUP = 16
FRAMES = 4
ROWS = 16
LANES = 128
TEAM = 4
TAPS = 9
EPSILON = 1e-6
MIB = 1 << 20

DMA = pltpu.SemaphoreType.DMA
F32, BF16 = jnp.float32, jnp.bfloat16
SHIFTS = [(0, 0), (0, -1), (0, 1), (-1, 0), (1, 0), (-1, -1), (-1, 1), (1, -1), (1, 1)]


def phases_of(dr, dc):
    rows = {-1: (0,), 0: (0, 1), 1: (1,)}
    return [(a, b) for a in rows[dr] for b in rows[dc]]


COLUMNS = [(s, p) for s in SHIFTS for p in phases_of(*s)]


def remote(src, dst, send, recv, device):
    return pltpu.make_async_remote_copy(
        src_ref=src, dst_ref=dst, send_sem=send, recv_sem=recv,
        device_id=device, device_id_type=pl.DeviceIdType.MESH,
    )


def signal(sem, device):
    pl.semaphore_signal(sem, inc=1, device_id=device, device_id_type=pl.DeviceIdType.MESH)


def wait_bytes(ref, sem):
    pltpu.make_async_copy(ref, ref, sem).wait()


def team(ny):
    g = lax.axis_index("groups")
    x, y = g // ny, g % ny
    x0, y0 = x - x % 2, y - y % 2
    return (x % 2) * 2 + y % 2, lambda p: (x0 + p // 2) * ny + y0 + p % 2


def group_matrix():
    lane = lax.broadcasted_iota(jnp.int32, (LANES, LANES), 0)
    packed = lax.broadcasted_iota(jnp.int32, (LANES, LANES), 1)
    return jnp.where(lane // GROUP == packed % 8, 1.0, 0.0).astype(F32)


def packed_mask(which):
    row = lax.broadcasted_iota(jnp.int32, (8, LANES), 0)
    lane = lax.broadcasted_iota(jnp.int32, (8, LANES), 1)
    return (lane // 32 == which) & ((lane // 8) % 4 == row % 4)


def hdot(a, b):
    return jnp.dot(a, b, preferred_element_type=F32, precision=lax.Precision.HIGHEST)


def pack(sums, which):
    return jnp.sum(jnp.where(packed_mask(which), hdot(sums, group_matrix()), 0.0), axis=0, keepdims=True)


def unpack(row, which):
    spread = jnp.where(packed_mask(which), jnp.broadcast_to(row, (8, LANES)), 0.0)
    return hdot(spread, group_matrix().T)


def exchange(ny, nd, x_ref, wq_ref, w, acts, totals, xs, stats, row, tot,
             local, ringsend, ringrecv, give, giverecv, own, ask, a2asend, a2arecv,
             statsend, statrecv, partsend, partrecv, totsend, totrecv):
    me = lax.axis_index("space")
    z, c = me // 2, me % 2
    nz = nd // 2
    half = nz // 2
    near = max(1, nz // 8)
    q, group_at = team(ny)

    def at(zz, core):
        return {"space": lax.rem(zz + 2 * nz, nz) * 2 + core}

    sibling = {"space": z * 2 + 1 - c}
    barrier = pltpu.get_barrier_semaphore()

    @pl.when(c == 1)
    def _():
        signal(barrier, at(z + 1, 1))
        signal(barrier, at(z - 1, 1))
        signal(barrier, sibling)
        load = pltpu.make_async_copy(wq_ref.at[:, :, :, pl.ds(q * LANES, LANES)], w.at[:, me], local.at[0])
        load.start()
        pl.semaphore_wait(barrier, 3)
        mine = remote(x_ref, xs.at[:, 1], own.at[0, 0], own.at[1, 0], sibling)
        mine.start()
        load.wait()

        def piece(zz, j):
            return w.at[j, pl.ds(lax.rem(zz + 2 * nz, nz) * 2, 2)]

        def right(p, s, j):
            return remote(p, p, ringsend.at[0], ringrecv.at[0, s, j], at(z + 1, 1))

        def left(p, s, j):
            return remote(p, p, ringsend.at[1], ringrecv.at[1, s, j], at(z - 1, 1))

        for j in range(3):
            theirs = w.at[j, z * 2]
            remote(theirs, theirs, own.at[0, 1 + j], own.at[1, 1 + j], sibling).wait_recv()
            p = piece(z, j)
            right(p, 0, j).start()
            left(p, 0, j).start()
            m = w.at[j, me]
            remote(m, m, give, giverecv, sibling).start()

        @pl.loop(0, half)
        def _(s):
            for j in range(3):
                p = piece(z - s - 1, j)
                right(p, s, j).wait_recv()

                @pl.when(s < half - 1)
                def _():
                    right(p, s + 1, j).start()

                remote(p, p, give, giverecv, sibling).start()

                @pl.when(s < half - 1)
                def _():
                    o = piece(z + s + 1, j)
                    left(o, s, j).wait_recv()

                    @pl.when(s < half - 2)
                    def _():
                        left(o, s + 1, j).start()

                    remote(o, o, give, giverecv, sibling).start()

        mine.wait_send()
        for p in range(TEAM):
            remote(acts.at[p], acts.at[p], partsend.at[1], partrecv.at[1, p], sibling).wait_recv()
        remote(totals, totals, totsend.at[1], totrecv.at[1], sibling).wait_recv()
        wait_bytes(w.at[:, pl.ds(0, 2 * half)], ringsend.at[0])
        wait_bytes(w.at[:, pl.ds(0, 2 * half - 2)], ringsend.at[1])
        wait_bytes(w.at[:, pl.ds(0, nd - 1)], give)

    @pl.when(c == 0)
    def _():
        for d in range(1, near + 1):
            signal(barrier, at(z + d, 0))
            signal(barrier, at(z - d, 0))
        for k in range(1, TEAM):
            signal(barrier, {"groups": group_at((q + k) % TEAM)})
        signal(barrier, sibling)
        load = pltpu.make_async_copy(wq_ref.at[:, :, :, pl.ds(q * LANES, LANES)], w.at[:, me], local.at[0])
        load.start()
        mine = pltpu.make_async_copy(x_ref, xs.at[:, 0], local.at[1])
        mine.start()
        pl.semaphore_wait(barrier, 2 * near + TEAM)
        cover, k = near, 0
        if cover < half:
            signal(ask.at[k], at(z + near, 0))
            signal(ask.at[k], at(z - near, 0))
        load.wait()
        pieces = []
        for j in range(3):
            p = w.at[j, me]
            pieces.append(remote(p, p, own.at[0, 1 + j], own.at[1, 1 + j], sibling))
            pieces[-1].start()
        mine.wait()
        remote(x_ref, xs.at[:, 1], own.at[0, 0], own.at[1, 0], sibling).wait_recv()

        def summed(f):
            def body(i, acc):
                out = []
                for r in range(2):
                    v = xs[i, r].astype(F32).reshape(3, 8, LANES)
                    out.append(f(v))
                return acc + out[0] + out[1]
            acc = lax.fori_loop(0, nz, body, jnp.zeros((3, 8, LANES), F32))
            rows = lax.broadcasted_iota(jnp.int32, (8, LANES), 0)
            return jnp.where(rows >= 4, acc[0], 0.0) + acc[1] + jnp.where(rows < 4, acc[2], 0.0)

        count = float(2 * 4 * nz * GROUP)
        first = pack(summed(lambda v: v), 0)
        mean = unpack(first, 0) * (1.0 / count)
        second = pack(summed(lambda v: (v - mean[None]) ** 2), 1)
        row[...] = first + second

        while cover < half:
            pl.semaphore_wait(ask.at[k], 2)
            cover, k = cover + near, k + 1
            if cover < half:
                signal(ask.at[k], at(z + near, 0))
                signal(ask.at[k], at(z - near, 0))

        def send(d, batch):
            zz = lax.rem(z + d + 2 * nz, nz)
            remote(row, stats.at[z], statsend, statrecv, at(zz, 0)).start()
            remote(xs.at[zz], acts.at[q, z], a2asend, a2arecv.at[batch], at(zz, 0)).start()

        send(half, (half - 1) // near)

        @pl.loop(1, half)
        def _(i):
            d = half - i
            batch = (d - 1) // near
            send(d, batch)
            send(-d, batch)

        def share(zz, src, batch):
            for k in range(1, TEAM):
                remote(src, acts.at[q, zz], partsend.at[0], partrecv.at[0, batch],
                       {"groups": group_at((q + k) % TEAM)}).start()

        acts[q, z] = xs[z]
        stats[z] = row[...]
        batches = (half + near - 1) // near
        share(z, xs.at[z], 0)
        sizes = [2 * near] * batches
        sizes[-1] = nz - 1 - 2 * near * (batches - 1)
        for b in range(batches):
            wait_bytes(acts.at[0, pl.ds(0, sizes[b])], a2arecv.at[b])

            @pl.loop(b * near + 1, min((b + 1) * near, half - 1) + 1)
            def _(d):
                for zz in (lax.rem(z + d, nz), lax.rem(z - d + nz, nz)):
                    share(zz, acts.at[q, zz], b)

            if b == batches - 1:
                zz = lax.rem(z + half, nz)
                share(zz, acts.at[q, zz], b)
            if b == 0:
                pass
            if b == batches - 1:
                remote(acts.at[q], acts.at[q], partsend.at[1], partrecv.at[1, q], sibling).start()

        wait_bytes(stats.at[pl.ds(0, nz - 1)], statrecv)
        every = stats[...].reshape(nz, LANES)
        lane = lax.broadcasted_iota(jnp.int32, (nz, LANES), 1)
        mean = jnp.sum(every, axis=0, keepdims=True) * (1.0 / (count * nz))
        off = jnp.where(lane < 32, (every * (1.0 / count) - mean) ** 2 * count, 0.0)
        spread = jnp.where(lane < 32, 0.0, every)
        spread = jnp.sum(spread + pltpu.roll(off, 32, 1), axis=0, keepdims=True) * (1.0 / (count * nz))
        tot[...] = jnp.where(lane[:1] < 32, mean, spread)
        totals[q] = tot[...]
        for k in range(1, TEAM):
            remote(tot, totals.at[q], totsend.at[0], totrecv.at[0],
                   {"groups": group_at((q + k) % TEAM)}).start()
        wait_bytes(totals.at[pl.ds(0, TEAM - 1)], totrecv.at[0])
        remote(totals, totals, totsend.at[1], totrecv.at[1], sibling).start()

        for b in range(batches):
            n = sizes[b] + (1 if b == 0 else 0)
            wait_bytes(acts.at[pl.ds(0, TEAM - 1), pl.ds(0, n)], partrecv.at[0, b])
        for k in range(1, TEAM):
            p = lax.rem(q + k, TEAM)
            remote(acts.at[p], acts.at[p], partsend.at[1], partrecv.at[1, p], sibling).start()

        wait_bytes(w.at[:, pl.ds(0, nd - 1)], giverecv)
        for p in pieces:
            p.wait_send()
        wait_bytes(stats.at[pl.ds(0, nz - 1)], statsend)
        wait_bytes(acts.at[0, pl.ds(0, nz - 1)], a2asend)
        wait_bytes(acts.at[pl.ds(0, TEAM - 1)], partsend.at[0])
        wait_bytes(acts, partsend.at[1])
        wait_bytes(totals.at[pl.ds(0, TEAM - 1)], totsend.at[0])
        wait_bytes(totals, totsend.at[1])


def convolve(ny, nd, w, acts, totals, gain, shift, bias, out, ys, a, mix, acc, total, turn):
    me = lax.axis_index("space")
    c = me % 2
    q, _ = team(ny)
    k_dim = a.shape[-1]

    for p in range(TEAM):
        mean = unpack(totals[p], 0)
        var = unpack(totals[p], 1)
        g = jnp.concatenate([gain[...], gain[...]], axis=0)
        b = jnp.concatenate([shift[...], shift[...]], axis=0)
        scale = g * lax.rsqrt(var + EPSILON)
        move = b - mean * scale

        @pl.loop(0, ROWS)
        def _(r):
            for f in range(FRAMES):
                v = acts[p, f * ROWS + r, pl.ds(pl.multiple_of(c * 8, 8), 16)].astype(F32).reshape(2, 8, LANES)
                v = v * scale[None] + move[None]
                v = v / (1.0 + jnp.exp(-v))
                ys[pl.ds(pl.multiple_of(r * 256 + (p * FRAMES + f) * 16, 16), 16)] = v.reshape(16, LANES)

    tiles = k_dim // LANES

    @pl.loop(0, ROWS)
    def _(r):
        for col in range(4):
            for t in range(tiles):
                v = ys[pl.ds(r * 256 + col * tiles + t, 16, stride=16)].astype(BF16)
                a[r + 1, col, :, t * LANES:(t + 1) * LANES] = v

    a[0] = a[1]
    a[ROWS + 1] = a[ROWS]

    row = lax.broadcasted_iota(jnp.int32, (8, LANES), 0) % FRAMES

    for dt in (2, 1, 0):
        @pl.loop(0, nd // 8)
        def _(i):
            tap = [w[dt, pl.ds(i * 8, 8), n].reshape(64, LANES).astype(F32) for n in range(TAPS)]

            def sums(x):
                return {(0, -1): x[0], (0, 0): x[1] + x[2], (1, 0): x[0] + x[1], (1, 1): x[2]}

            by_row = [sums([tap[n * 3 + e] for n in range(3)]) for e in range(3)]
            both = {k: sums([by_row[e][k] for e in range(3)]) for k in by_row[0]}
            for n, ((dr, dc), (pr, pc)) in enumerate(COLUMNS):
                mix[pl.ds(pl.multiple_of(i * 64, 64), 64), n * LANES:(n + 1) * LANES] = both[(pr, dr)][(pc, dc)].astype(BF16)

        dst = total if dt == 2 else acc
        at = 0
        for dr, dc in SHIFTS:
            ps = phases_of(dr, dc)
            lhs = a[1 + dr:1 + dr + ROWS, 1 + dc:3 + dc].reshape(2 * ROWS * 16, k_dim)
            r = jnp.dot(lhs, mix[:, at:at + len(ps) * LANES], preferred_element_type=F32)
            at += len(ps) * LANES
            if (dr, dc) == (0, 0):
                dst[...] = r
            else:
                for n, (pr, pc) in enumerate(ps):
                    cols = slice((pr * 2 + pc) * LANES, (pr * 2 + pc + 1) * LANES)
                    dst[:, cols] += r[:, n * LANES:(n + 1) * LANES]
        if dt != 2:
            back = 2 - dt

            @pl.loop(0, acc.shape[0] // 8)
            def _(i):
                rows = pl.ds(pl.multiple_of(i * 8, 8), 8)
                for n in range(4):
                    cols = slice(n * LANES, (n + 1) * LANES)
                    v = acc[rows, cols]
                    moved = jnp.where(row >= 1, pltpu.roll(v, 1, 0), v)
                    if back == 2:
                        moved = jnp.where(row >= 2, pltpu.roll(v, 2, 0), moved)
                    total[rows, cols] += moved

    bias_row = bias[q]
    for r in range(ROWS):
        for cc in range(2):
            for n in range(4):
                pr, pc = n // 2, n % 2
                turn[((r * 2 + pr) * 2 + cc) * 2 + pc] = total[(r * 2 + cc) * 16:(r * 2 + cc + 1) * 16, n * LANES:(n + 1) * LANES] + bias_row
    flat = turn.reshape(ROWS * 8 * 16, LANES)
    for p in range(TEAM):
        for f in range(FRAMES):
            out[p, f] = flat[pl.ds(p * FRAMES + f, ROWS * 8, stride=16)].astype(BF16)


def swap(ny, mine, out, send, recv):
    q, group_at = team(ny)
    barrier = pltpu.get_barrier_semaphore()
    for k in range(1, TEAM):
        signal(barrier, {"groups": group_at((q + k) % TEAM)})
    pl.semaphore_wait(barrier, TEAM - 1)
    for k in (3, 2, 1):
        p = lax.rem(q + k, TEAM)
        remote(mine.at[p], out.at[q], send, recv, {"groups": group_at(p)}).start()
    out[q] = mine[q]
    wait_bytes(out.at[pl.ds(0, TEAM - 1)], recv)
    wait_bytes(out.at[pl.ds(0, TEAM - 1)], send)


VMEM = pl.BlockSpec(memory_space=pltpu.VMEM)
ANY = pl.BlockSpec(memory_space=pl.ANY)


def shards(ny, hidden, norm_gain, norm_shift, conv_weight, conv_bias):
    nd = lax.axis_size("space")
    nz = nd // 2
    channels = hidden.shape[1]
    tiles = channels // LANES
    cols = hidden.shape[0] // nz
    near = max(1, nz // 8)
    batches = (nz // 2 + near - 1) // near
    h = hidden.reshape(nz, cols, channels)
    before = jnp.concatenate([h[:1, :1], h[:-1, -1:]], axis=0)
    after = jnp.concatenate([h[1:, :1], h[-1:, -1:]], axis=0)
    x6 = jnp.concatenate([before, h, after], axis=1).reshape(nz, (cols + 2) * tiles, LANES)
    wide = (cols + 2) * tiles
    cin = conv_weight.shape[3]
    wq = conv_weight.reshape(3, TAPS, cin, conv_weight.shape[4])
    w, acts, totals = pl.pallas_call(
        functools.partial(exchange, ny, nd),
        out_shape=(
            jax.ShapeDtypeStruct((3, nd, TAPS, cin, LANES), BF16),
            jax.ShapeDtypeStruct((TEAM, nz, 2, wide, LANES), BF16),
            jax.ShapeDtypeStruct((TEAM, 1, LANES), F32),
        ),
        in_specs=[ANY, ANY],
        out_specs=(VMEM, VMEM, VMEM),
        scratch_shapes=[
            pltpu.VMEM((nz, 2, wide, LANES), BF16),
            pltpu.VMEM((nz, 1, LANES), F32),
            pltpu.VMEM((1, LANES), F32),
            pltpu.VMEM((1, LANES), F32),
            DMA((2,)), DMA((2,)), DMA((2, nz // 2, 3)), DMA, DMA, DMA((2, 4)),
            pltpu.SemaphoreType.REGULAR((max(1, batches),)),
            DMA, DMA((batches,)), DMA, DMA, DMA((2,)), DMA((2, max(batches, TEAM))), DMA((2,)), DMA((2,)),
        ],
        compiler_params=pltpu.CompilerParams(collective_id=0, has_side_effects=True, vmem_limit_bytes=24 * MIB),
        name="exchange",
    )(x6, wq)
    mine = pl.pallas_call(
        functools.partial(convolve, ny, nd),
        out_shape=jax.ShapeDtypeStruct((TEAM, FRAMES, ROWS * 8, LANES), BF16),
        in_specs=[VMEM] * 6,
        out_specs=VMEM,
        scratch_shapes=[
            pltpu.VMEM((ROWS * 256, LANES), F32),
            pltpu.VMEM((ROWS + 2, 4, 16, channels), BF16),
            pltpu.VMEM((channels, 16 * LANES), BF16),
            pltpu.VMEM((2 * ROWS * 16, 4 * LANES), F32),
            pltpu.VMEM((2 * ROWS * 16, 4 * LANES), F32),
            pltpu.VMEM((ROWS * 8, 16, LANES), F32),
        ],
        compiler_params=pltpu.CompilerParams(vmem_limit_bytes=48 * MIB),
        name="convolve",
    )(w, acts.reshape(TEAM, nd, wide, LANES), totals, norm_gain.reshape(tiles, LANES),
      norm_shift.reshape(tiles, LANES), conv_bias.astype(F32).reshape(tiles, 1, LANES))
    parts = pl.pallas_call(
        functools.partial(swap, ny),
        out_shape=jax.ShapeDtypeStruct((TEAM, FRAMES, ROWS * 8, LANES), BF16),
        in_specs=[VMEM],
        out_specs=VMEM,
        scratch_shapes=[DMA, DMA],
        compiler_params=pltpu.CompilerParams(collective_id=1, has_side_effects=True),
        name="swap",
    )(mine)
    parts = parts.reshape(TEAM, FRAMES, ROWS * 2, 4, LANES)
    return jnp.transpose(parts, (1, 2, 3, 0, 4)).reshape(FRAMES, ROWS * 2, 4, channels)


def solution(mesh):
    ny = len({d.coords[1] for d in mesh.devices.flat})
    return jax.shard_map(
        functools.partial(shards, ny),
        mesh=mesh,
        in_specs=(P(("groups", "space"), None), P(), P(), P(None, None, None, "space", None), P()),
        out_specs=P("groups", None, "space", None),
        check_vma=False,
    )
```

```python
import functools

import jax
import jax.numpy as jnp
from jax import lax
from jax.experimental import pallas as pl
from jax.experimental.pallas import tpu as pltpu
from jax.sharding import PartitionSpec as P

GROUP = 16
FRAMES = 4
ROWS = 16
LANES = 128
TEAM = 4
TAPS = 9
EPSILON = 1e-6
MIB = 1 << 20
YROWS = 40
TROWS = 24

DMA = pltpu.SemaphoreType.DMA
F32, BF16 = jnp.float32, jnp.bfloat16
SHIFTS = [(0, 0), (0, -1), (0, 1), (-1, 0), (1, 0), (-1, -1), (-1, 1), (1, -1), (1, 1)]


def phases_of(dr, dc):
    rows = {-1: (0,), 0: (0, 1), 1: (1,)}
    return [(a, b) for a in rows[dr] for b in rows[dc]]


COLUMNS = [(s, p) for s in SHIFTS for p in phases_of(*s)]


def remote(src, dst, send, recv, device):
    return pltpu.make_async_remote_copy(
        src_ref=src, dst_ref=dst, send_sem=send, recv_sem=recv,
        device_id=device, device_id_type=pl.DeviceIdType.MESH,
    )


def signal(sem, device):
    pl.semaphore_signal(sem, inc=1, device_id=device, device_id_type=pl.DeviceIdType.MESH)


def wait_bytes(ref, sem):
    pltpu.make_async_copy(ref, ref, sem).wait()


def team(ny):
    g = lax.axis_index("groups")
    x, y = g // ny, g % ny
    x0, y0 = x - x % 2, y - y % 2
    return (x % 2) * 2 + y % 2, lambda p: (x0 + p // 2) * ny + y0 + p % 2


def group_matrix():
    lane = lax.broadcasted_iota(jnp.int32, (LANES, LANES), 0)
    packed = lax.broadcasted_iota(jnp.int32, (LANES, LANES), 1)
    return jnp.where(lane // GROUP == packed % 8, 1.0, 0.0).astype(F32)


def packed_mask(which):
    row = lax.broadcasted_iota(jnp.int32, (8, LANES), 0)
    lane = lax.broadcasted_iota(jnp.int32, (8, LANES), 1)
    return (lane // 32 == which) & ((lane // 8) % 4 == row % 4)


def hdot(a, b):
    return jnp.dot(a, b, preferred_element_type=F32, precision=lax.Precision.HIGHEST)


def pack(sums, which):
    return jnp.sum(jnp.where(packed_mask(which), hdot(sums, group_matrix()), 0.0), axis=0, keepdims=True)


def unpack(row, which):
    spread = jnp.where(packed_mask(which), jnp.broadcast_to(row, (8, LANES)), 0.0)
    return hdot(spread, group_matrix().T)


def rounds_of(half):
    known, steps = 1, []
    while known < half:
        step = min(known, max(1, half // 4))
        known += step
        steps.append((step, min(known, half)))
    return steps


def kernel(ny, nd, h_ref, wq_ref, gain, shift, bias, out,
           w, mix, acts, totals, raw, cells, flat, stats, row, tot, ys, a, acc, total, turn, mine,
           local, ringsend, ringrecv, give, giverecv, own, ask, a2asend, a2arecv,
           statsend, statrecv, partsend, partrecv, northsend, northrecv, totsend, totrecv, outsend, outrecv):
    me = lax.axis_index("space")
    z, c = me // 2, me % 2
    nz = nd // 2
    half = nz // 2
    q, group_at = team(ny)
    rounds = rounds_of(half)
    spans, last = [], 0
    for known in [1] + [r[1] for r in rounds]:
        spans.append((last + 1, known))
        last = known
    sizes = [2 * (hi - lo + 1) - (1 if hi == half else 0) for lo, hi in spans]

    def at(zz, core):
        return {"space": lax.rem(zz + 2 * nz, nz) * 2 + core}

    sibling = {"space": z * 2 + 1 - c}
    barrier = pltpu.get_barrier_semaphore()

    def blend(zz):
        zz = lax.rem(zz + 2 * nz, nz)
        for dt in range(3):
            tap = [w[dt, pl.ds(zz * 2, 2), n].reshape(16, LANES).astype(F32) for n in range(TAPS)]

            def sums(x):
                return {(0, -1): x[0], (0, 0): x[1] + x[2], (1, 0): x[0] + x[1], (1, 1): x[2]}

            by_row = [sums([tap[n * 3 + e] for n in range(3)]) for e in range(3)]
            both = {k: sums([by_row[e][k] for e in range(3)]) for k in by_row[0]}
            for n, ((dr, dc), (pr, pc)) in enumerate(COLUMNS):
                mix[dt, pl.ds(pl.multiple_of(zz * 16, 16), 16), n * LANES:(n + 1) * LANES] = both[(pr, dr)][(pc, dc)].astype(BF16)

    load = pltpu.make_async_copy(wq_ref.at[:, :, :, pl.ds(q * LANES, LANES)], w.at[:, me], local.at[0])
    rows_in = pltpu.make_async_copy(h_ref, raw.at[0], local.at[1])

    @pl.when(c == 1)
    def _():
        signal(barrier, at(z + 1, 1))
        signal(barrier, at(z - 1, 1))
        signal(barrier, sibling)
        load.start()
        rows_in.start()
        pl.semaphore_wait(barrier, 3)
        rows_in.wait()
        rows_out = remote(raw.at[0], raw.at[1], own.at[0, 0], own.at[1, 0], sibling)
        rows_out.start()
        load.wait()

        def piece(zz, j):
            return w.at[j, pl.ds(lax.rem(zz + 2 * nz, nz) * 2, 2)]

        def right(p, s, j):
            return remote(p, p, ringsend.at[0], ringrecv.at[0, s, j], at(z + 1, 1))

        def left(p, s, j):
            return remote(p, p, ringsend.at[1], ringrecv.at[1, s, j], at(z - 1, 1))

        for j in range(3):
            theirs = w.at[j, z * 2]
            remote(theirs, theirs, own.at[0, 1 + j], own.at[1, 1 + j], sibling).wait_recv()
            p = piece(z, j)
            right(p, 0, j).start()
            left(p, 0, j).start()
            m = w.at[j, me]
            remote(m, m, give, giverecv.at[half], sibling).start()
        blend(z)

        @pl.loop(0, half)
        def _(s):
            for j in range(3):
                p = piece(z - s - 1, j)
                right(p, s, j).wait_recv()

                @pl.when(s < half - 1)
                def _():
                    right(p, s + 1, j).start()

                remote(p, p, give, giverecv.at[s], sibling).start()

                @pl.when(s < half - 1)
                def _():
                    o = piece(z + s + 1, j)
                    left(o, s, j).wait_recv()

                    @pl.when(s < half - 2)
                    def _():
                        left(o, s + 1, j).start()

                    remote(o, o, give, giverecv.at[s], sibling).start()

            blend(z - s - 1)

            @pl.when(s < half - 1)
            def _():
                blend(z + s + 1)

        rows_out.wait_send()
        wait_bytes(w.at[:, pl.ds(0, 2 * half)], ringsend.at[0])
        wait_bytes(w.at[:, pl.ds(0, 2 * half - 2)], ringsend.at[1])
        wait_bytes(w.at[:, pl.ds(0, nd - 1)], give)
        wait_bytes(acts, northrecv)
        remote(totals, totals, totsend.at[1], totrecv.at[1], sibling).wait_recv()

    @pl.when(c == 0)
    def _():
        signal(barrier, at(z + 1, 0))
        signal(barrier, at(z - 1, 0))
        signal(barrier, sibling)
        for k in range(1, TEAM):
            signal(barrier, {"groups": group_at((q + k) % TEAM)})
        load.start()
        rows_in.start()
        pl.semaphore_wait(barrier, 2 + TEAM)

        def tell(k):
            if k < len(rounds):
                signal(ask.at[k], at(z + rounds[k][0], 0))
                signal(ask.at[k], at(z - rounds[k][0], 0))

        tell(0)
        load.wait()
        pieces = []
        for j in range(3):
            p = w.at[j, me]
            pieces.append(remote(p, p, own.at[0, 1 + j], own.at[1, 1 + j], sibling))
            pieces[-1].start()
        rows_in.wait()
        remote(raw.at[0], raw.at[1], own.at[0, 0], own.at[1, 0], sibling).wait_recv()

        wide = raw.shape[1]
        tiles = raw.shape[2] // LANES
        for r in range(2):
            for t in range(tiles):
                flat[pl.ds(r * tiles + t, wide, stride=8)] = raw[r, :, t * LANES:(t + 1) * LANES].astype(F32)
        x = flat[...].reshape(wide, 8, LANES)
        cells[pl.ds(1, wide)] = x.astype(BF16)
        cells[0] = x[0].astype(BF16)
        cells[wide + 1] = x[wide - 1].astype(BF16)

        def each(b, body):
            lo, hi = spans[b]

            @pl.loop(lo, min(hi, half - 1) + 1)
            def _(d):
                body(d)
                body(-d)

            if hi == half:
                body(half)

        def for_chip(zz):
            return cells.at[pl.ds(zz * 4, 6)]

        def send_rows(b):
            def body(d):
                zz = lax.rem(z + d + nz, nz)
                remote(for_chip(zz), acts.at[q, z], a2asend, a2arecv.at[b], at(zz, 0)).start()
            each(b, body)

        def send_stats(b):
            each(b, lambda d: remote(row, stats.at[z], statsend, statrecv, at(z + d, 0)).start())

        def share(zz, src, b):
            for k in range(1, TEAM):
                remote(src, acts.at[q, zz], partsend, partrecv.at[b],
                       {"groups": group_at((q + k) % TEAM)}).start()

        def hand_over(p, zz, src):
            remote(src, acts.at[p, zz], northsend, northrecv, sibling).start()

        send_rows(0)
        share(z, for_chip(z), 0)
        hand_over(q, z, for_chip(z))

        count = float(2 * wide * GROUP)
        first = pack(jnp.sum(flat[...].reshape(wide, 8, LANES), axis=0), 0)
        mean = unpack(first, 0) * (1.0 / count)
        second = pack(jnp.sum((flat[...].reshape(wide, 8, LANES) - mean[None]) ** 2, axis=0), 1)
        row[...] = first + second
        stats[z] = row[...]
        acts[q, z] = cells[pl.ds(z * 4, 6)]
        send_stats(0)

        for k in range(len(rounds)):
            pl.semaphore_wait(ask.at[k], 2)
            tell(k + 1)
            send_rows(k + 1)
            send_stats(k + 1)

        for b in range(len(spans)):
            wait_bytes(acts.at[0, pl.ds(0, sizes[b])], a2arecv.at[b])

            def body(d):
                zz = lax.rem(z + d + nz, nz)
                share(zz, acts.at[q, zz], b)
                hand_over(q, zz, acts.at[q, zz])
            each(b, body)

        wait_bytes(stats.at[pl.ds(0, nz - 1)], statrecv)
        every = stats[...].reshape(nz, LANES)
        lane = lax.broadcasted_iota(jnp.int32, (nz, LANES), 1)
        mean = jnp.sum(every, axis=0, keepdims=True) * (1.0 / (count * nz))
        off = jnp.where(lane < 32, (every * (1.0 / count) - mean) ** 2 * count, 0.0)
        spread = jnp.where(lane < 32, 0.0, every)
        spread = jnp.sum(spread + pltpu.roll(off, 32, 1), axis=0, keepdims=True) * (1.0 / (count * nz))
        tot[...] = jnp.where(lane[:1] < 32, mean, spread)
        totals[q] = tot[...]
        for k in range(1, TEAM):
            remote(tot, totals.at[q], totsend.at[0], totrecv.at[0],
                   {"groups": group_at((q + k) % TEAM)}).start()
        wait_bytes(totals.at[pl.ds(0, TEAM - 1)], totrecv.at[0])
        remote(totals, totals, totsend.at[1], totrecv.at[1], sibling).start()

        for b in range(len(spans)):
            n = sizes[b] + (1 if b == 0 else 0)
            wait_bytes(acts.at[pl.ds(0, TEAM - 1), pl.ds(0, n)], partrecv.at[b])

            def body(d):
                zz = lax.rem(z + d + nz, nz)
                for k in range(1, TEAM):
                    p = lax.rem(q + k, TEAM)
                    hand_over(p, zz, acts.at[p, zz])
            if b == 0:
                body(0)
            each(b, body)

        wait_bytes(w.at[:, 0], giverecv.at[half])
        blend(z)

        @pl.loop(0, half - 1)
        def _(s):
            wait_bytes(w.at[:, pl.ds(0, 4)], giverecv.at[s])
            blend(z - s - 1)
            blend(z + s + 1)

        wait_bytes(w.at[:, pl.ds(0, 2)], giverecv.at[half - 1])
        blend(z + half)
        for p in pieces:
            p.wait_send()
        wait_bytes(stats.at[pl.ds(0, nz - 1)], statsend)
        wait_bytes(acts.at[0, pl.ds(0, nz - 1)], a2asend)
        wait_bytes(acts.at[pl.ds(0, TEAM - 1)], partsend)
        wait_bytes(acts, northsend)
        wait_bytes(totals.at[pl.ds(0, TEAM - 1)], totsend.at[0])
        wait_bytes(totals, totsend.at[1])

    channels = a.shape[-1]
    tiles = channels // LANES
    pairs = ROWS // 2
    g = jnp.concatenate([gain[t] for t in range(tiles)] * 2, axis=0)
    b = jnp.concatenate([shift[t] for t in range(tiles)] * 2, axis=0)
    for p in range(TEAM):
        mean = unpack(totals[p], 0)
        scale = g * lax.rsqrt(unpack(totals[p], 1) + EPSILON)
        move = b - mean * scale

        @pl.loop(0, pairs)
        def _(rp):
            for f in range(FRAMES):
                v = acts[p, f * pairs + rp, pl.ds(2 * c, 4)].astype(F32)
                v = v * scale[None] + move[None]
                v = v / (1.0 + jnp.exp(-v))
                start = rp * (16 * YROWS) + (p * FRAMES + f) * YROWS
                ys[pl.ds(pl.multiple_of(start, 8), 32)] = v.reshape(32, LANES)

    @pl.loop(0, pairs)
    def _(rp):
        for col in range(4):
            for r in range(2):
                for t in range(tiles):
                    v = ys[pl.ds(rp * (16 * YROWS) + col * 8 + r * tiles + t, 16, stride=YROWS)].astype(BF16)
                    a[rp * 2 + r + 1, col, :, t * LANES:(t + 1) * LANES] = v

    a[0] = a[1]
    a[ROWS + 1] = a[ROWS]

    frame = lax.broadcasted_iota(jnp.int32, (8, LANES), 0) % FRAMES
    few = ROWS // 2
    for h in range(2):
        for dt in (2, 1, 0):
            dst = total if dt == 2 else acc
            col0 = 0
            for dr, dc in SHIFTS:
                ps = phases_of(dr, dc)
                lhs = a[1 + dr + h * few:1 + dr + (h + 1) * few, 1 + dc:3 + dc].reshape(few * 2 * 16, channels)
                r = jnp.dot(lhs, mix[dt, :, col0:col0 + len(ps) * LANES], preferred_element_type=F32)
                col0 += len(ps) * LANES
                if (dr, dc) == (0, 0):
                    dst[...] = r
                else:
                    for n, (pr, pc) in enumerate(ps):
                        cols = slice((pr * 2 + pc) * LANES, (pr * 2 + pc + 1) * LANES)
                        dst[:, cols] += r[:, n * LANES:(n + 1) * LANES]
            if dt != 2:
                @pl.loop(0, acc.shape[0] // 8)
                def _(i):
                    rows = pl.ds(pl.multiple_of(i * 8, 8), 8)
                    for n in range(4):
                        cols = slice(n * LANES, (n + 1) * LANES)
                        v = acc[rows, cols]
                        moved = jnp.where(frame >= 1, pltpu.roll(v, 1, 0), v)
                        if dt == 0:
                            moved = jnp.where(frame >= 2, pltpu.roll(v, 2, 0), moved)
                        total[rows, cols] += moved

        bias_row = bias[q].astype(F32)
        for r in range(few):
            for cc in range(2):
                for n in range(4):
                    pr, pc = n // 2, n % 2
                    i = ((r * 2 + pr) * 2 + cc) * 2 + pc
                    turn[i * TROWS:i * TROWS + 16] = total[(r * 2 + cc) * 16:(r * 2 + cc + 1) * 16, n * LANES:(n + 1) * LANES] + bias_row
        put = slice(h * ROWS, (h + 1) * ROWS)
        for p in range(TEAM):
            for f in range(FRAMES):
                v = turn[pl.ds(p * FRAMES + f, few * 8, stride=TROWS)].astype(BF16)
                mine[p, f, put] = v.reshape(ROWS, 4, LANES)
        here = pl.ds(pl.multiple_of(q * LANES, LANES), LANES)
        for k in (3, 2, 1):
            p = lax.rem(q + k, TEAM)
            remote(mine.at[p, :, put], out.at[:, put, :, here], outsend, outrecv, {"groups": group_at(p)}).start()
        out[:, put, :, here] = mine[q, :, put]
    wait_bytes(mine.at[pl.ds(0, TEAM - 1)], outrecv)
    wait_bytes(mine.at[pl.ds(0, TEAM - 1)], outsend)


VMEM = pl.BlockSpec(memory_space=pltpu.VMEM)
ANY = pl.BlockSpec(memory_space=pl.ANY)


def shards(ny, hidden, norm_gain, norm_shift, conv_weight, conv_bias):
    nd = lax.axis_size("space")
    nz = nd // 2
    wide, channels = hidden.shape
    tiles = channels // LANES
    cin = conv_weight.shape[3]
    batches = len(rounds_of(nz // 2)) + 1
    wq = conv_weight.reshape(3, TAPS, cin, conv_weight.shape[4])
    scratch = [
        pltpu.VMEM((3, nd, TAPS, cin, LANES), BF16),
        pltpu.VMEM((3, channels, 16 * LANES), BF16),
        pltpu.VMEM((TEAM, nz, 6, 8, LANES), BF16),
        pltpu.VMEM((TEAM, 1, LANES), F32),
        pltpu.VMEM((2, wide, channels), BF16),
        pltpu.VMEM((wide + 2, 8, LANES), BF16),
        pltpu.VMEM((wide * 8, LANES), F32),
        pltpu.VMEM((nz, 1, LANES), F32),
        pltpu.VMEM((1, LANES), F32),
        pltpu.VMEM((1, LANES), F32),
        pltpu.VMEM((ROWS // 2 * 16 * YROWS, LANES), F32),
        pltpu.VMEM((ROWS + 2, 4, 16, channels), BF16),
        pltpu.VMEM((ROWS * 16, 4 * LANES), F32),
        pltpu.VMEM((ROWS * 16, 4 * LANES), F32),
        pltpu.VMEM((ROWS * 4 * TROWS, LANES), F32),
        pltpu.VMEM((TEAM, FRAMES, ROWS * 2, 4, LANES), BF16),
        DMA((2,)), DMA((2,)), DMA((2, nz // 2, 3)), DMA, DMA((nz // 2 + 1,)), DMA((2, 4)),
        pltpu.SemaphoreType.REGULAR((max(1, batches - 1),)),
        DMA, DMA((batches,)), DMA, DMA, DMA, DMA((batches,)), DMA, DMA, DMA((2,)), DMA((2,)), DMA, DMA,
    ]
    return pl.pallas_call(
        functools.partial(kernel, ny, nd),
        out_shape=jax.ShapeDtypeStruct((FRAMES, ROWS * 2, 4, channels), BF16),
        in_specs=[ANY, ANY, VMEM, VMEM, VMEM],
        out_specs=VMEM,
        scratch_shapes=scratch,
        compiler_params=pltpu.CompilerParams(collective_id=0, has_side_effects=True, vmem_limit_bytes=56 * MIB),
        name="decode",
    )(hidden, wq, norm_gain.reshape(tiles, 1, LANES), norm_shift.reshape(tiles, 1, LANES), conv_bias.reshape(tiles, 1, LANES))


def solution(mesh):
    ny = len({d.coords[1] for d in mesh.devices.flat})
    return jax.shard_map(
        functools.partial(shards, ny),
        mesh=mesh,
        in_specs=(P(("groups", "space"), None), P(), P(), P(None, None, None, "space", None), P()),
        out_specs=P("groups", None, "space", None),
        check_vma=False,
    )
```

```python
import functools

import jax
import jax.numpy as jnp
from jax import lax
from jax.experimental import pallas as pl
from jax.experimental.pallas import tpu as pltpu
from jax.sharding import PartitionSpec as P

GROUP = 16
FRAMES = 4
ROWS = 16
LANES = 128
TEAM = 4
TAPS = 9
EPSILON = 1e-6
MIB = 1 << 20
YROWS = 40
TROWS = 24
NEAR = 5

DMA = pltpu.SemaphoreType.DMA
F32, BF16 = jnp.float32, jnp.bfloat16
SHIFTS = [(0, 0), (0, -1), (0, 1), (-1, 0), (1, 0), (-1, -1), (-1, 1), (1, -1), (1, 1)]


def phases_of(dr, dc):
    rows = {-1: (0,), 0: (0, 1), 1: (1,)}
    return [(a, b) for a in rows[dr] for b in rows[dc]]


COLUMNS = [(s, p) for s in SHIFTS for p in phases_of(*s)]


def remote(src, dst, send, recv, device):
    return pltpu.make_async_remote_copy(
        src_ref=src, dst_ref=dst, send_sem=send, recv_sem=recv,
        device_id=device, device_id_type=pl.DeviceIdType.MESH,
    )


def signal(sem, device):
    pl.semaphore_signal(sem, inc=1, device_id=device, device_id_type=pl.DeviceIdType.MESH)


def wait_bytes(ref, sem):
    pltpu.make_async_copy(ref, ref, sem).wait()


def team(ny):
    g = lax.axis_index("groups")
    x, y = g // ny, g % ny
    x0, y0 = x - x % 2, y - y % 2
    return (x % 2) * 2 + y % 2, lambda p: (x0 + p // 2) * ny + y0 + p % 2


def group_matrix():
    lane = lax.broadcasted_iota(jnp.int32, (LANES, LANES), 0)
    packed = lax.broadcasted_iota(jnp.int32, (LANES, LANES), 1)
    return jnp.where(lane // GROUP == packed % 8, 1.0, 0.0).astype(F32)


def packed_mask(which):
    row = lax.broadcasted_iota(jnp.int32, (8, LANES), 0)
    lane = lax.broadcasted_iota(jnp.int32, (8, LANES), 1)
    return (lane // 32 == which) & ((lane // 8) % 4 == row % 4)


def hdot(a, b):
    return jnp.dot(a, b, preferred_element_type=F32, precision=lax.Precision.HIGHEST)


def pack(sums, which):
    return jnp.sum(jnp.where(packed_mask(which), hdot(sums, group_matrix()), 0.0), axis=0, keepdims=True)


def unpack(row, which):
    spread = jnp.where(packed_mask(which), jnp.broadcast_to(row, (8, LANES)), 0.0)
    return hdot(spread, group_matrix().T)


def rounds_of(half):
    known, steps = 1, []
    while known < half:
        step = min(known, max(1, half // 4))
        known += step
        steps.append((step, min(known, half)))
    return steps


def kernel(ny, nd, h_ref, wq_ref, gain_ref, shift_ref, bias_ref, out, gain, shift, bias,
           w, mix, acts, totals, raw, cells, flat, stats, row, tot, ys, a, acc, total, turn, mine,
           local, ringsend, ringrecv, give, giverecv, own, ask, a2asend, a2arecv,
           statsend, statrecv, partsend, partrecv, northsend, northrecv, edgesend, edgerecv, totsend, totrecv, outsend, outrecv):
    me = lax.axis_index("space")
    z, c = me // 2, me % 2
    nz = nd // 2
    half = nz // 2
    q, group_at = team(ny)
    leaps = (half - NEAR + 1) // 2
    assert NEAR + 2 * leaps == half + 1
    rounds = rounds_of(half)
    spans, last = [], 0
    for known in [1] + [r[1] for r in rounds]:
        spans.append((last + 1, known))
        last = known
    sizes = [2 * (hi - lo + 1) - (1 if hi == half else 0) for lo, hi in spans]

    def at(zz, core):
        return {"space": lax.rem(zz + 2 * nz, nz) * 2 + core}

    sibling = {"space": z * 2 + 1 - c}
    barrier = pltpu.get_barrier_semaphore()

    def blend(zz):
        zz = lax.rem(zz + 2 * nz, nz)
        for dt in range(3):
            tap = [w[dt, pl.ds(zz * 2, 2), n].reshape(16, LANES).astype(F32) for n in range(TAPS)]

            def sums(x):
                return {(0, -1): x[0], (0, 0): x[1] + x[2], (1, 0): x[0] + x[1], (1, 1): x[2]}

            by_row = [sums([tap[n * 3 + e] for n in range(3)]) for e in range(3)]
            both = {k: sums([by_row[e][k] for e in range(3)]) for k in by_row[0]}
            for n, ((dr, dc), (pr, pc)) in enumerate(COLUMNS):
                mix[dt, pl.ds(pl.multiple_of(zz * 16, 16), 16), n * LANES:(n + 1) * LANES] = both[(pr, dr)][(pc, dc)].astype(BF16)

    channels = a.shape[-1]
    tiles = channels // LANES
    pairs = ROWS // 2

    def activate():
        for copy in small:
            copy.wait()
        g = jnp.concatenate([gain[t] for t in range(tiles)] * 2, axis=0)
        b = jnp.concatenate([shift[t] for t in range(tiles)] * 2, axis=0)
        for p in range(TEAM):
            mean = unpack(totals[p], 0)
            scale = g * lax.rsqrt(unpack(totals[p], 1) + EPSILON)
            move = (b - mean * scale) * 0.5
            scale = scale * 0.5

            @pl.loop(0, pairs, unroll=4)
            def _(rp):
                for f in range(FRAMES):
                    v = acts[p, f * pairs + rp, pl.ds(2 * c, 4)].astype(F32)
                    v = v * scale[None] + move[None]
                    v = v * jnp.tanh(v) + v
                    start = rp * (16 * YROWS) + (p * FRAMES + f) * YROWS
                    ys[pl.ds(pl.multiple_of(start, 8), 32)] = v.reshape(32, LANES)

        @pl.loop(0, pairs)
        def _(rp):
            for col in range(4):
                for r in range(2):
                    for t in range(tiles):
                        v = ys[pl.ds(rp * (16 * YROWS) + col * 8 + r * tiles + t, 16, stride=YROWS)].astype(BF16)
                        a[rp * 2 + r + 1, col, :, t * LANES:(t + 1) * LANES] = v

        a[0] = a[1]
        a[ROWS + 1] = a[ROWS]

    load = pltpu.make_async_copy(wq_ref.at[:, :, :, pl.ds(q * LANES, LANES)], w.at[:, me], local.at[0])
    rows_in = pltpu.make_async_copy(h_ref, raw.at[0], local.at[1])
    small = [pltpu.make_async_copy(src, dst, local.at[2 + i])
             for i, (src, dst) in enumerate(((gain_ref, gain), (shift_ref, shift), (bias_ref, bias)))]

    @pl.when(c == 1)
    def _():
        signal(barrier, at(z + 1, 1))
        signal(barrier, at(z - 1, 1))
        signal(barrier, sibling)
        load.start()
        rows_in.start()
        for copy in small:
            copy.start()
        pl.semaphore_wait(barrier, 3)
        rows_in.wait()
        rows_out = remote(raw.at[0], raw.at[1], own.at[0, 0], own.at[1, 0], sibling)
        rows_out.start()
        load.wait()

        def piece(zz, j):
            return w.at[j, pl.ds(lax.rem(zz + 2 * nz, nz) * 2, 2)]

        def hop(way, p, d, j, step=1):
            to = z + step if way == 0 else z - step
            return remote(p, p, ringsend.at[way], ringrecv.at[way, d - 1, j], at(to, 1))

        for j in range(3):
            theirs = w.at[j, z * 2]
            remote(theirs, theirs, own.at[0, 1 + j], own.at[1, 1 + j], sibling).wait_recv()
            p = piece(z, j)
            for way in (0, 1):
                hop(way, p, 1, j).start()
            m = w.at[j, me]
            remote(m, m, give, giverecv.at[half], sibling).start()
        blend(z)

        def take(way, d, j, s, on):
            p = piece(z - d if way == 0 else z + d, j)
            hop(way, p, d, j).wait_recv()
            for step in on:
                hop(way, p, d + step, j, step).start()
            remote(p, p, give, giverecv.at[s], sibling).start()

        @pl.loop(0, NEAR - 1)
        def _(s):
            for j in range(3):
                take(0, s + 1, j, s, (1,))
                take(1, s + 1, j, s, (1,))
            blend(z - s - 1)
            blend(z + s + 1)

        @pl.loop(0, leaps - 1)
        def _(u):
            d, s = NEAR + 2 * u, NEAR - 1 + u
            for j in range(3):
                take(0, d, j, s, (2, 1))
                take(1, d, j, s, (2, 1))
            blend(z - d)
            blend(z + d)

            @pl.when(u > 0)
            def _():
                for j in range(3):
                    take(0, d - 1, j, s, ())
                    take(1, d - 1, j, s, ())
                blend(z - d + 1)
                blend(z + d - 1)

        d, s = half - 1, NEAR - 2 + leaps
        for j in range(3):
            take(0, d, j, s, (1,))
            take(1, d, j, s, ())
        blend(z - d)
        blend(z + d)
        for j in range(3):
            take(0, d - 1, j, s, ())
            take(1, d - 1, j, s, ())
        blend(z - d + 1)
        blend(z + d - 1)
        wait_bytes(acts.at[:, :, pl.ds(2, 3)], northrecv)
        remote(totals, totals, totsend.at[1], totrecv.at[1], sibling).wait_recv()

        @pl.when(z < nz - 1)
        def _():
            wait_bytes(acts.at[:, :, 5], edgerecv)

        @pl.when(z == nz - 1)
        def _():
            acts[:, :, 5] = acts[:, :, 4]

        activate()
        for j in range(3):
            take(0, half, j, s, ())
        blend(z + half)

        rows_out.wait_send()
        wait_bytes(w.at[:, pl.ds(0, 2 * half)], ringsend.at[0])
        wait_bytes(w.at[:, pl.ds(0, 2 * half - 2)], ringsend.at[1])
        wait_bytes(w.at[:, pl.ds(0, nd - 1)], give)

    @pl.when(c == 0)
    def _():
        signal(barrier, at(z + 1, 0))
        signal(barrier, at(z - 1, 0))
        signal(barrier, sibling)
        for k in range(1, TEAM):
            signal(barrier, {"groups": group_at((q + k) % TEAM)})
        load.start()
        rows_in.start()
        for copy in small:
            copy.start()
        pl.semaphore_wait(barrier, 2 + TEAM)

        def tell(k):
            if k < len(rounds):
                signal(ask.at[k], at(z + rounds[k][0], 0))
                signal(ask.at[k], at(z - rounds[k][0], 0))

        tell(0)
        load.wait()
        pieces = []
        for j in range(3):
            p = w.at[j, me]
            pieces.append(remote(p, p, own.at[0, 1 + j], own.at[1, 1 + j], sibling))
            pieces[-1].start()
        early = min(2, len(rounds))
        for k in range(early):
            pl.semaphore_wait(ask.at[k], 2)
            tell(k + 1)
        rows_in.wait()
        remote(raw.at[0], raw.at[1], own.at[0, 0], own.at[1, 0], sibling).wait_recv()

        wide = raw.shape[1]
        for r in range(2):
            for t in range(tiles):
                flat[pl.ds(r * tiles + t, wide, stride=8)] = raw[r, :, t * LANES:(t + 1) * LANES].astype(F32)
        x = flat[...].reshape(wide, 8, LANES)
        cells[...] = x.astype(BF16)

        def each(b, body):
            lo, hi = spans[b]

            @pl.loop(lo, min(hi, half - 1) + 1)
            def _(d):
                body(d)
                body(-d)

            if hi == half:
                body(half)

        middle = pl.ds(1, 4)
        norths = pl.ds(2, 3)

        def for_chip(zz):
            return cells.at[pl.ds(zz * 4, 4)]

        def send_rows(b):
            def body(d):
                zz = lax.rem(z + d + nz, nz)
                remote(for_chip(zz), acts.at[q, z, middle], a2asend, a2arecv.at[b], at(zz, 0)).start()
            each(b, body)

        def send_stats(b):
            each(b, lambda d: remote(row, stats.at[z], statsend, statrecv, at(z + d, 0)).start())

        def share(zz, src, b):
            for k in range(1, TEAM):
                remote(src, acts.at[q, zz, middle], partsend, partrecv.at[b],
                       {"groups": group_at((q + k) % TEAM)}).start()

        def hand_over(p, zz, src):
            remote(src, acts.at[p, zz, norths], northsend, northrecv, sibling).start()

        for b in range(early + 1):
            send_rows(b)
        share(z, for_chip(z), 0)
        hand_over(q, z, cells.at[pl.ds(z * 4 + 1, 3)])

        count = float(2 * wide * GROUP)
        first = pack(jnp.sum(flat[...].reshape(wide, 8, LANES), axis=0), 0)
        mean = unpack(first, 0) * (1.0 / count)
        second = pack(jnp.sum((flat[...].reshape(wide, 8, LANES) - mean[None]) ** 2, axis=0), 1)
        row[...] = first + second
        stats[z] = row[...]
        acts[q, z, 1:5] = cells[pl.ds(z * 4, 4)]
        for b in range(early + 1):
            send_stats(b)

        for k in range(early, len(rounds)):
            pl.semaphore_wait(ask.at[k], 2)
            tell(k + 1)
            send_rows(k + 1)
            send_stats(k + 1)

        for b in range(len(spans)):
            wait_bytes(acts.at[0, pl.ds(0, sizes[b]), middle], a2arecv.at[b])

            def body(d):
                zz = lax.rem(z + d + nz, nz)
                share(zz, acts.at[q, zz, middle], b)
                hand_over(q, zz, acts.at[q, zz, norths])
            each(b, body)

        def from_team(b):
            n = sizes[b] + (1 if b == 0 else 0)
            wait_bytes(acts.at[pl.ds(0, TEAM - 1), pl.ds(0, n), middle], partrecv.at[b])

            def body(d):
                zz = lax.rem(z + d + nz, nz)
                for k in range(1, TEAM):
                    p = lax.rem(q + k, TEAM)
                    hand_over(p, zz, acts.at[p, zz, norths])
            if b == 0:
                body(0)
            each(b, body)

        from_team(0)
        for k in range(TEAM):
            g = group_at((q + k) % TEAM)

            @pl.when(z < nz - 1)
            def _():
                remote(acts.at[q, :, 4], acts.at[q, :, 0], edgesend.at[0], edgerecv,
                       {"groups": g, "space": z * 2 + 2}).start()

            @pl.when(z > 0)
            def _():
                remote(acts.at[q, :, 1], acts.at[q, :, 5], edgesend.at[1], edgerecv,
                       {"groups": g, "space": z * 2 - 1}).start()

        wait_bytes(stats.at[pl.ds(0, nz - 1)], statrecv)
        every = stats[...].reshape(nz, LANES)
        lane = lax.broadcasted_iota(jnp.int32, (nz, LANES), 1)
        mean = jnp.sum(every, axis=0, keepdims=True) * (1.0 / (count * nz))
        off = jnp.where(lane < 32, (every * (1.0 / count) - mean) ** 2 * count, 0.0)
        spread = jnp.where(lane < 32, 0.0, every)
        spread = jnp.sum(spread + pltpu.roll(off, 32, 1), axis=0, keepdims=True) * (1.0 / (count * nz))
        tot[...] = jnp.where(lane[:1] < 32, mean, spread)
        totals[q] = tot[...]
        for k in range(1, TEAM):
            remote(tot, totals.at[q], totsend.at[0], totrecv.at[0],
                   {"groups": group_at((q + k) % TEAM)}).start()
        wait_bytes(totals.at[pl.ds(0, TEAM - 1)], totrecv.at[0])
        remote(totals, totals, totsend.at[1], totrecv.at[1], sibling).start()

        for b in range(1, len(spans)):
            from_team(b)

        @pl.when(z > 0)
        def _():
            wait_bytes(acts.at[:, :, 0], edgerecv)

        @pl.when(z == 0)
        def _():
            acts[:, :, 0] = acts[:, :, 1]

        activate()
        wait_bytes(w.at[:, 0], giverecv.at[half])
        blend(z)

        @pl.loop(0, NEAR - 1)
        def _(s):
            wait_bytes(w.at[:, pl.ds(0, 4)], giverecv.at[s])
            blend(z - s - 1)
            blend(z + s + 1)

        wait_bytes(w.at[:, pl.ds(0, 4)], giverecv.at[NEAR - 1])
        blend(z - NEAR)
        blend(z + NEAR)

        @pl.loop(1, leaps - 1)
        def _(u):
            wait_bytes(w.at[:, pl.ds(0, 8)], giverecv.at[NEAR - 1 + u])
            for d in (0, -1):
                blend(z - NEAR - 2 * u - d)
                blend(z + NEAR + 2 * u + d)

        wait_bytes(w.at[:, pl.ds(0, 10)], giverecv.at[NEAR - 2 + leaps])
        for d in (half - 2, half - 1):
            blend(z - d)
            blend(z + d)
        blend(z + half)
        for p in pieces:
            p.wait_send()
        wait_bytes(stats.at[pl.ds(0, nz - 1)], statsend)
        wait_bytes(acts.at[0, pl.ds(0, nz - 1), middle], a2asend)
        wait_bytes(acts.at[pl.ds(0, TEAM - 1), :, middle], partsend)
        wait_bytes(acts.at[:, :, norths], northsend)

        @pl.when(z < nz - 1)
        def _():
            wait_bytes(acts.at[:, :, 0], edgesend.at[0])

        @pl.when(z > 0)
        def _():
            wait_bytes(acts.at[:, :, 0], edgesend.at[1])
        wait_bytes(totals.at[pl.ds(0, TEAM - 1)], totsend.at[0])
        wait_bytes(totals, totsend.at[1])

    frame = lax.broadcasted_iota(jnp.int32, (8, LANES), 0) % FRAMES
    few = ROWS // 2
    for h in range(2):
        for dt in (2, 1, 0):
            dst = total if dt == 2 else acc
            col0 = 0
            for dr, dc in SHIFTS:
                ps = phases_of(dr, dc)
                lhs = a[1 + dr + h * few:1 + dr + (h + 1) * few, 1 + dc:3 + dc].reshape(few * 2 * 16, channels)
                r = jnp.dot(lhs, mix[dt, :, col0:col0 + len(ps) * LANES], preferred_element_type=F32)
                col0 += len(ps) * LANES
                if (dr, dc) == (0, 0):
                    dst[...] = r
                else:
                    for n, (pr, pc) in enumerate(ps):
                        cols = slice((pr * 2 + pc) * LANES, (pr * 2 + pc + 1) * LANES)
                        dst[:, cols] += r[:, n * LANES:(n + 1) * LANES]
            if dt != 2:
                @pl.loop(0, acc.shape[0] // 8)
                def _(i):
                    rows = pl.ds(pl.multiple_of(i * 8, 8), 8)
                    for n in range(4):
                        cols = slice(n * LANES, (n + 1) * LANES)
                        v = acc[rows, cols]
                        moved = jnp.where(frame >= 1, pltpu.roll(v, 1, 0), v)
                        if dt == 0:
                            moved = jnp.where(frame >= 2, pltpu.roll(v, 2, 0), moved)
                        total[rows, cols] += moved

        bias_row = bias[q]
        for r in range(few):
            for cc in range(2):
                for n in range(4):
                    pr, pc = n // 2, n % 2
                    i = ((r * 2 + pr) * 2 + cc) * 2 + pc
                    turn[i * TROWS:i * TROWS + 16] = total[(r * 2 + cc) * 16:(r * 2 + cc + 1) * 16, n * LANES:(n + 1) * LANES] + bias_row
        put = slice(h * ROWS, (h + 1) * ROWS)
        for p in range(TEAM):
            for f in range(FRAMES):
                v = turn[pl.ds(p * FRAMES + f, few * 8, stride=TROWS)].astype(BF16)
                mine[p, f, put] = v.reshape(ROWS, 4, LANES)
        here = pl.ds(pl.multiple_of(q * LANES, LANES), LANES)
        for k in (3, 2, 1):
            p = lax.rem(q + k, TEAM)
            remote(mine.at[p, :, put], out.at[:, put, :, here], outsend, outrecv, {"groups": group_at(p)}).start()
        out[:, put, :, here] = mine[q, :, put]
    wait_bytes(mine.at[pl.ds(0, TEAM - 1)], outrecv)
    wait_bytes(mine.at[pl.ds(0, TEAM - 1)], outsend)


VMEM = pl.BlockSpec(memory_space=pltpu.VMEM)
HBM = pl.BlockSpec(memory_space=pltpu.HBM)


def shards(ny, hidden, norm_gain, norm_shift, conv_weight, conv_bias):
    nd = lax.axis_size("space")
    nz = nd // 2
    wide, channels = hidden.shape
    tiles = channels // LANES
    cin = conv_weight.shape[3]
    batches = len(rounds_of(nz // 2)) + 1
    wq = conv_weight.reshape(3, TAPS, cin, conv_weight.shape[4])
    scratch = [pltpu.VMEM((tiles, 1, LANES), F32)] * 3 + [
        pltpu.VMEM((3, nd, TAPS, cin, LANES), BF16),
        pltpu.VMEM((3, channels, 16 * LANES), BF16),
        pltpu.VMEM((TEAM, nz, 6, 8, LANES), BF16),
        pltpu.VMEM((TEAM, 1, LANES), F32),
        pltpu.VMEM((2, wide, channels), BF16),
        pltpu.VMEM((wide, 8, LANES), BF16),
        pltpu.VMEM((wide * 8, LANES), F32),
        pltpu.VMEM((nz, 1, LANES), F32),
        pltpu.VMEM((1, LANES), F32),
        pltpu.VMEM((1, LANES), F32),
        pltpu.VMEM((ROWS // 2 * 16 * YROWS, LANES), F32),
        pltpu.VMEM((ROWS + 2, 4, 16, channels), BF16),
        pltpu.VMEM((ROWS * 16, 4 * LANES), F32),
        pltpu.VMEM((ROWS * 16, 4 * LANES), F32),
        pltpu.VMEM((ROWS * 4 * TROWS, LANES), F32),
        pltpu.VMEM((TEAM, FRAMES, ROWS * 2, 4, LANES), BF16),
        DMA((5,)), DMA((2,)), DMA((2, nz // 2, 3)), DMA, DMA((nz // 2 + 1,)), DMA((2, 4)),
        pltpu.SemaphoreType.REGULAR((max(1, batches - 1),)),
        DMA, DMA((batches,)), DMA, DMA, DMA, DMA((batches,)), DMA, DMA, DMA((2,)), DMA, DMA((2,)), DMA((2,)), DMA, DMA,
    ]
    return pl.pallas_call(
        functools.partial(kernel, ny, nd),
        out_shape=jax.ShapeDtypeStruct((FRAMES, ROWS * 2, 4, channels), BF16),
        in_specs=[HBM] * 5,
        out_specs=VMEM,
        scratch_shapes=scratch,
        compiler_params=pltpu.CompilerParams(collective_id=0, has_side_effects=True, vmem_limit_bytes=56 * MIB),
        name="decode",
    )(hidden, wq, norm_gain.reshape(tiles, 1, LANES), norm_shift.reshape(tiles, 1, LANES), conv_bias.astype(F32).reshape(tiles, 1, LANES))


def solution(mesh):
    ny = len({d.coords[1] for d in mesh.devices.flat})
    return jax.shard_map(
        functools.partial(shards, ny),
        mesh=mesh,
        in_specs=(P(("groups", "space"), None), P(), P(), P(None, None, None, "space", None), P()),
        out_specs=P("groups", None, "space", None),
        check_vma=False,
    )
```

```python
import functools

import jax
import jax.numpy as jnp
from jax import lax
from jax.experimental import pallas as pl
from jax.experimental.pallas import tpu as pltpu
from jax.sharding import PartitionSpec as P

GROUP = 16
FRAMES = 4
ROWS = 16
LANES = 128
TEAM = 4
TAPS = 9
EPSILON = 1e-6
MIB = 1 << 20
YROWS = 40
TROWS = 24
NEAR = 6

DMA = pltpu.SemaphoreType.DMA
F32, BF16 = jnp.float32, jnp.bfloat16
SHIFTS = [(0, 0), (0, -1), (0, 1), (-1, 0), (1, 0), (-1, -1), (-1, 1), (1, -1), (1, 1)]


def phases_of(dr, dc):
    rows = {-1: (0,), 0: (0, 1), 1: (1,)}
    return [(a, b) for a in rows[dr] for b in rows[dc]]


COLUMNS = [(s, p) for s in SHIFTS for p in phases_of(*s)]


def remote(src, dst, send, recv, device):
    return pltpu.make_async_remote_copy(
        src_ref=src, dst_ref=dst, send_sem=send, recv_sem=recv,
        device_id=device, device_id_type=pl.DeviceIdType.MESH,
    )


def signal(sem, device):
    pl.semaphore_signal(sem, inc=1, device_id=device, device_id_type=pl.DeviceIdType.MESH)


def wait_bytes(ref, sem):
    pltpu.make_async_copy(ref, ref, sem).wait()


def team(ny):
    g = lax.axis_index("groups")
    x, y = g // ny, g % ny
    x0, y0 = x - x % 2, y - y % 2
    return (x % 2) * 2 + y % 2, lambda p: (x0 + p // 2) * ny + y0 + p % 2


def group_matrix():
    lane = lax.broadcasted_iota(jnp.int32, (LANES, LANES), 0)
    packed = lax.broadcasted_iota(jnp.int32, (LANES, LANES), 1)
    return jnp.where(lane // GROUP == packed % 8, 1.0, 0.0).astype(F32)


def packed_mask(which):
    row = lax.broadcasted_iota(jnp.int32, (8, LANES), 0)
    lane = lax.broadcasted_iota(jnp.int32, (8, LANES), 1)
    return (lane // 32 == which) & ((lane // 8) % 4 == row % 4)


def hdot(a, b):
    return jnp.dot(a, b, preferred_element_type=F32, precision=lax.Precision.HIGHEST)


def pack(sums, which):
    return jnp.sum(jnp.where(packed_mask(which), hdot(sums, group_matrix()), 0.0), axis=0, keepdims=True)


def unpack(row, which):
    spread = jnp.where(packed_mask(which), jnp.broadcast_to(row, (8, LANES)), 0.0)
    return hdot(spread, group_matrix().T)


def rounds_of(half):
    known, steps = 1, []
    while known < half:
        step = min(known, max(1, half // 4))
        known += step
        steps.append((step, min(known, half)))
    return steps


def kernel(ny, nd, h_ref, wq_ref, gain_ref, shift_ref, bias_ref, out, gain, shift, bias,
           w, mix, acts, totals, raw, cells, flat, stats, row, tot, ys, a, acc, turn, mine,
           local, ringsend, ringrecv, give, giverecv, own, ask, a2asend, a2arecv,
           statsend, statrecv, partsend, partrecv, northsend, northrecv, edgesend, edgerecv, totsend, totrecv, outsend, outrecv):
    me = lax.axis_index("space")
    z, c = me // 2, me % 2
    nz = nd // 2
    half = nz // 2
    q, group_at = team(ny)
    leaps = (half - NEAR) // 2
    assert NEAR + 2 * leaps == half
    rounds = rounds_of(half)
    spans, last = [], 0
    for known in [1] + [r[1] for r in rounds]:
        spans.append((last + 1, known))
        last = known
    sizes = [2 * (hi - lo + 1) - (1 if hi == half else 0) for lo, hi in spans]

    def at(zz, core):
        return {"space": lax.rem(zz + 2 * nz, nz) * 2 + core}

    sibling = {"space": z * 2 + 1 - c}
    barrier = pltpu.get_barrier_semaphore()

    def blend(zz):
        zz = lax.rem(zz + 2 * nz, nz)
        for dt in range(3):
            tap = [w[dt, pl.ds(zz * 2, 2), n].astype(F32).reshape(16, LANES) for n in range(TAPS)]

            def sums(x):
                return {(0, -1): x[0], (0, 0): x[1] + x[2], (1, 0): x[0] + x[1], (1, 1): x[2]}

            by_row = [sums([tap[n * 3 + e] for n in range(3)]) for e in range(3)]
            both = {k: sums([by_row[e][k] for e in range(3)]) for k in by_row[0]}
            for n, ((dr, dc), (pr, pc)) in enumerate(COLUMNS):
                mix[dt, pl.ds(pl.multiple_of(zz * 16, 16), 16), n * LANES:(n + 1) * LANES] = both[(pr, dr)][(pc, dc)].astype(BF16)

    channels = a.shape[-1]
    tiles = channels // LANES
    pairs = ROWS // 2

    def activate(places):
        g = jnp.concatenate([gain[t] for t in range(tiles)] * 2, axis=0)
        b = jnp.concatenate([shift[t] for t in range(tiles)] * 2, axis=0)
        for p in places:
            mean = unpack(totals[p], 0)
            scale = g * lax.rsqrt(unpack(totals[p], 1) + EPSILON)
            move = (b - mean * scale) * 0.5
            scale = scale * 0.5

            @pl.loop(0, pairs, unroll=4)
            def _(rp):
                for f in range(FRAMES):
                    v = acts[p, f * pairs + rp, pl.ds(2 * c, 4)].astype(F32)
                    v = v * scale[None] + move[None]
                    v = v * jnp.tanh(v) + v
                    start = rp * (16 * YROWS) + (p * FRAMES + f) * YROWS
                    ys[pl.ds(pl.multiple_of(start, 8), 32)] = v.reshape(32, LANES)

    def arrange():
        @pl.loop(0, pairs)
        def _(rp):
            for col in range(4):
                for r in range(2):
                    for t in range(tiles):
                        v = ys[pl.ds(rp * (16 * YROWS) + col * 8 + r * tiles + t, 16, stride=YROWS)].astype(BF16)
                        a[rp * 2 + r + 1, col, :, t * LANES:(t + 1) * LANES] = v

        a[0] = a[1]
        a[ROWS + 1] = a[ROWS]

    few = ROWS // 2
    chips = LANES // 16
    first_block = z // chips + jnp.where(z % chips < chips // 2, tiles - 1, 0)
    assert half - 4 >= chips * 3 // 2 - 1 and tiles == 4

    def multiply(h, late):
        blocks = [pl.ds(pl.multiple_of(lax.rem(first_block + 2 * late + i, tiles) * LANES, LANES), LANES) for i in range(2)]
        for dt in range(3):
            col0 = 0
            for dr, dc in SHIFTS:
                ps = phases_of(dr, dc)
                rows, cols = slice(1 + dr + h * few, 1 + dr + (h + 1) * few), slice(1 + dc, 3 + dc)
                lhs = jnp.concatenate([a[rows, cols, :, k].reshape(few * 2 * 16, LANES) for k in blocks], axis=1)
                rhs = jnp.concatenate([mix[dt, k, col0:col0 + len(ps) * LANES] for k in blocks], axis=0)
                r = jnp.dot(lhs, rhs, preferred_element_type=F32)
                col0 += len(ps) * LANES
                if (dr, dc) == (0, 0):
                    acc[h, dt] = acc[h, dt] + r if late else r
                else:
                    for n, (pr, pc) in enumerate(ps):
                        to = slice((pr * 2 + pc) * LANES, (pr * 2 + pc + 1) * LANES)
                        acc[h, dt, :, to] += r[:, n * LANES:(n + 1) * LANES]

    load = pltpu.make_async_copy(wq_ref.at[:, :, :, pl.ds(q * LANES, LANES)], w.at[:, me], local.at[0])
    rows_in = pltpu.make_async_copy(h_ref, raw.at[0], local.at[1])
    small = [pltpu.make_async_copy(src, dst, local.at[2 + i])
             for i, (src, dst) in enumerate(((gain_ref, gain), (shift_ref, shift), (bias_ref, bias)))]

    @pl.when(c == 1)
    def _():
        signal(barrier, at(z + 1, 1))
        signal(barrier, at(z - 1, 1))
        signal(barrier, sibling)
        load.start()
        rows_in.start()
        for copy in small:
            copy.start()
        pl.semaphore_wait(barrier, 3)
        rows_in.wait()
        rows_out = remote(raw.at[0], raw.at[1], own.at[0, 0], own.at[1, 0], sibling)
        rows_out.start()
        load.wait()

        def piece(zz, j):
            return w.at[j, pl.ds(lax.rem(zz + 2 * nz, nz) * 2, 2)]

        def hop(way, p, d, j, step=1):
            to = z + step if way == 0 else z - step
            return remote(p, p, ringsend.at[way], ringrecv.at[way, d - 1, j], at(to, 1))

        def first(part, j):
            for way in (0, 1):
                hop(way, part, 1, j).start()

        for j in range(3):
            m = w.at[j, me]
            first(m, j)
            remote(m, m, give, giverecv.at[half], sibling).start()
        for j in range(3):
            theirs = w.at[j, z * 2]
            remote(theirs, theirs, own.at[0, 1 + j], own.at[1, 1 + j], sibling).wait_recv()
            first(theirs, j)
        blend(z)

        def take(way, d, j, s, on):
            p = piece(z - d if way == 0 else z + d, j)
            hop(way, p, d, j).wait_recv()
            for step in on:
                hop(way, p, d + step, j, step).start()
            remote(p, p, give, giverecv.at[s], sibling).start()

        @pl.loop(0, NEAR - 1)
        def _(s):
            for j in range(3):
                take(0, s + 1, j, s, (1,))
                take(1, s + 1, j, s, (1,))
            blend(z - s - 1)
            blend(z + s + 1)

        @pl.loop(0, leaps - 1)
        def _(u):
            d, s = NEAR + 2 * u, NEAR - 1 + u
            for j in range(3):
                take(0, d, j, s, (2, 1))
                take(1, d, j, s, (2, 1))
            blend(z - d)
            blend(z + d)

            @pl.when(u == leaps - 2)
            def _():
                wait_bytes(acts.at[:, :, pl.ds(2, 3)], northrecv)
                remote(totals, totals, totsend.at[1], totrecv.at[1], sibling).wait_recv()

                @pl.when(z < nz - 1)
                def _():
                    wait_bytes(acts.at[:, :, 5], edgerecv)

                @pl.when(z == nz - 1)
                def _():
                    acts[:, :, 5] = acts[:, :, 4]

                for copy in small:
                    copy.wait()
                activate((0, 1))

            @pl.when(u > 0)
            def _():
                for j in range(3):
                    take(0, d - 1, j, s, ())
                    take(1, d - 1, j, s, ())
                blend(z - d + 1)
                blend(z + d - 1)

        activate((2, 3))
        arrange()
        d, s = half - 2, NEAR - 2 + leaps
        for j in range(3):
            take(0, d, j, s, (2, 1) if j < 2 else (1,))
            take(1, d, j, s, (1,) if j < 2 else (2, 1))
        blend(z - d)
        blend(z + d)
        for j in range(3):
            take(0, d - 1, j, s, ())
            take(1, d - 1, j, s, ())
        blend(z - d + 1)
        blend(z + d - 1)
        multiply(0, 0)
        multiply(1, 0)
        s = NEAR - 1 + leaps
        for j in range(3):
            take(0, half - 1, j, s, ())
            take(1, half - 1, j, s, ())
        blend(z - half + 1)
        blend(z + half - 1)
        for j in range(3):
            take(0 if j < 2 else 1, half, j, s, ())
        blend(z + half)

        rows_out.wait_send()
        for way, rest in ((0, pl.ds(0, 2)), (1, pl.ds(0, 1))):
            wait_bytes(w.at[:, pl.ds(0, 2 * half - 2)], ringsend.at[way])
            wait_bytes(w.at[rest, pl.ds(0, 2)], ringsend.at[way])
        wait_bytes(w.at[:, pl.ds(0, nd - 1)], give)

    @pl.when(c == 0)
    def _():
        signal(barrier, at(z + 1, 0))
        signal(barrier, at(z - 1, 0))
        signal(barrier, sibling)
        for k in range(1, TEAM):
            signal(barrier, {"groups": group_at((q + k) % TEAM)})
        load.start()
        rows_in.start()
        for copy in small:
            copy.start()
        pl.semaphore_wait(barrier, 2 + TEAM)

        def tell(k):
            if k < len(rounds):
                signal(ask.at[k], at(z + rounds[k][0], 0))
                signal(ask.at[k], at(z - rounds[k][0], 0))

        tell(0)
        load.wait()
        pieces = []
        for j in range(3):
            p = w.at[j, me]
            pieces.append(remote(p, p, own.at[0, 1 + j], own.at[1, 1 + j], sibling))
            pieces[-1].start()
        early = min(2, len(rounds))
        for k in range(early):
            pl.semaphore_wait(ask.at[k], 2)
            tell(k + 1)
        rows_in.wait()
        remote(raw.at[0], raw.at[1], own.at[0, 0], own.at[1, 0], sibling).wait_recv()

        wide = raw.shape[1]
        for r in range(2):
            for t in range(tiles):
                flat[pl.ds(r * tiles + t, wide, stride=8)] = raw[r, :, t * LANES:(t + 1) * LANES].astype(F32)
        x = flat[...].reshape(wide, 8, LANES)
        cells[...] = x.astype(BF16)

        def each(b, body):
            lo, hi = spans[b]

            @pl.loop(lo, min(hi, half - 1) + 1)
            def _(d):
                body(d)
                body(-d)

            if hi == half:
                body(half)

        middle = pl.ds(1, 4)
        norths = pl.ds(2, 3)

        def for_chip(zz):
            return cells.at[pl.ds(zz * 4, 4)]

        def send_rows(b):
            def body(d):
                zz = lax.rem(z + d + nz, nz)
                remote(for_chip(zz), acts.at[q, z, middle], a2asend, a2arecv.at[b], at(zz, 0)).start()
            each(b, body)

        def send_stats(b):
            each(b, lambda d: remote(row, stats.at[z], statsend, statrecv, at(z + d, 0)).start())

        def edges(zz, first, last):
            @pl.when(z < nz - 1)
            def _():
                for k in range(TEAM):
                    remote(last, acts.at[q, zz, 0], edgesend.at[0], edgerecv,
                           {"groups": group_at((q + k) % TEAM), "space": z * 2 + 2}).start()

            @pl.when(z > 0)
            def _():
                for k in range(TEAM):
                    remote(first, acts.at[q, zz, 5], edgesend.at[1], edgerecv,
                           {"groups": group_at((q + k) % TEAM), "space": z * 2 - 1}).start()

        def share(zz, src, b):
            for k in range(1, TEAM):
                remote(src, acts.at[q, zz, middle], partsend, partrecv.at[b],
                       {"groups": group_at((q + k) % TEAM)}).start()

        def hand_over(p, zz, src):
            remote(src, acts.at[p, zz, norths], northsend, northrecv, sibling).start()

        for b in range(early + 1):
            send_rows(b)
        share(z, for_chip(z), len(spans))
        hand_over(q, z, cells.at[pl.ds(z * 4 + 1, 3)])

        count = float(2 * wide * GROUP)
        first = pack(jnp.sum(flat[...].reshape(wide, 8, LANES), axis=0), 0)
        mean = unpack(first, 0) * (1.0 / count)
        second = pack(jnp.sum((flat[...].reshape(wide, 8, LANES) - mean[None]) ** 2, axis=0), 1)
        row[...] = first + second
        stats[z] = row[...]
        acts[q, z, 1:5] = cells[pl.ds(z * 4, 4)]
        for b in range(early + 1):
            send_stats(b)

        for k in range(early, len(rounds)):
            pl.semaphore_wait(ask.at[k], 2)
            tell(k + 1)
            send_rows(k + 1)
            send_stats(k + 1)

        def from_team(b):
            n = sizes[b] if b < len(spans) else 1
            wait_bytes(acts.at[pl.ds(0, TEAM - 1), pl.ds(0, n), middle], partrecv.at[b])

            def body(d):
                zz = lax.rem(z + d + nz, nz)
                for k in range(1, TEAM):
                    p = lax.rem(q + k, TEAM)
                    hand_over(p, zz, acts.at[p, zz, norths])
            if b < len(spans):
                each(b, body)
            else:
                body(0)

        from_team(len(spans))
        edges(z, cells.at[z * 4], cells.at[z * 4 + 3])
        for b in range(len(spans)):
            if b == len(spans) - 1:
                wait_bytes(stats.at[pl.ds(0, nz - 1)], statrecv)
                every = stats[...].reshape(nz, LANES)
                lane = lax.broadcasted_iota(jnp.int32, (nz, LANES), 1)
                mean = jnp.sum(every, axis=0, keepdims=True) * (1.0 / (count * nz))
                off = jnp.where(lane < 32, (every * (1.0 / count) - mean) ** 2 * count, 0.0)
                spread = jnp.where(lane < 32, 0.0, every)
                spread = jnp.sum(spread + pltpu.roll(off, 32, 1), axis=0, keepdims=True) * (1.0 / (count * nz))
                tot[...] = jnp.where(lane[:1] < 32, mean, spread)
                totals[q] = tot[...]
                for k in range(1, TEAM):
                    remote(tot, totals.at[q], totsend.at[0], totrecv.at[0],
                           {"groups": group_at((q + k) % TEAM)}).start()
            wait_bytes(acts.at[0, pl.ds(0, sizes[b]), middle], a2arecv.at[b])

            def body(d):
                zz = lax.rem(z + d + nz, nz)
                share(zz, acts.at[q, zz, middle], b)
                edges(zz, acts.at[q, zz, 1], acts.at[q, zz, 4])
                hand_over(q, zz, acts.at[q, zz, norths])
            each(b, body)

        wait_bytes(totals.at[pl.ds(0, TEAM - 1)], totrecv.at[0])
        remote(totals, totals, totsend.at[1], totrecv.at[1], sibling).start()
        for b in range(len(spans)):
            from_team(b)

        @pl.when(z > 0)
        def _():
            wait_bytes(acts.at[:, :, 0], edgerecv)

        @pl.when(z == 0)
        def _():
            acts[:, :, 0] = acts[:, :, 1]

        for copy in small:
            copy.wait()
        activate(range(TEAM))
        arrange()
        wait_bytes(w.at[:, 0], giverecv.at[half])
        blend(z)

        @pl.loop(0, NEAR - 1)
        def _(s):
            wait_bytes(w.at[:, pl.ds(0, 4)], giverecv.at[s])
            blend(z - s - 1)
            blend(z + s + 1)

        wait_bytes(w.at[:, pl.ds(0, 4)], giverecv.at[NEAR - 1])
        blend(z - NEAR)
        blend(z + NEAR)

        @pl.loop(1, leaps)
        def _(u):
            wait_bytes(w.at[:, pl.ds(0, 8)], giverecv.at[NEAR - 1 + u])
            for d in (0, -1):
                blend(z - NEAR - 2 * u - d)
                blend(z + NEAR + 2 * u + d)

            @pl.when(u >= leaps - 2)
            def _():
                @pl.when(u == leaps - 2)
                def _():
                    multiply(0, 0)

                @pl.when(u == leaps - 1)
                def _():
                    multiply(1, 0)

        wait_bytes(w.at[:, pl.ds(0, 6)], giverecv.at[NEAR - 1 + leaps])
        blend(z - half + 1)
        blend(z + half - 1)
        blend(z + half)
        for p in pieces:
            p.wait_send()
        wait_bytes(stats.at[pl.ds(0, nz - 1)], statsend)
        wait_bytes(acts.at[0, pl.ds(0, nz - 1), middle], a2asend)
        wait_bytes(acts.at[pl.ds(0, TEAM - 1), :, middle], partsend)
        wait_bytes(acts.at[:, :, norths], northsend)

        @pl.when(z < nz - 1)
        def _():
            wait_bytes(acts.at[:, :, 0], edgesend.at[0])

        @pl.when(z > 0)
        def _():
            wait_bytes(acts.at[:, :, 0], edgesend.at[1])
        wait_bytes(totals.at[pl.ds(0, TEAM - 1)], totsend.at[0])
        wait_bytes(totals, totsend.at[1])

    frame = lax.broadcasted_iota(jnp.int32, (8, LANES), 0) % FRAMES
    which = lax.broadcasted_iota(jnp.int32, (tiles, LANES), 0)
    bias_row = jnp.sum(jnp.where(which == q, bias[...].astype(F32), 0.0), axis=0, keepdims=True)
    for h in range(2):
        multiply(h, 1)
        for r in range(few):
            for cc in range(2):
                for n in range(4):
                    i = ((r * 2 + n // 2) * 2 + cc) * 2 + n % 2
                    for half_tile in range(2):
                        at_row = (r * 2 + cc) * 16 + half_tile * 8
                        old, mid, new = (acc[h, dt, at_row:at_row + 8, n * LANES:(n + 1) * LANES] for dt in range(3))
                        mid = jnp.where(frame >= 1, pltpu.roll(mid, 1, 0), mid)
                        old = jnp.where(frame >= 2, pltpu.roll(old, 2, 0), jnp.where(frame >= 1, pltpu.roll(old, 1, 0), old))
                        turn[i * TROWS + half_tile * 8:i * TROWS + half_tile * 8 + 8] = old + mid + new + bias_row
        put = slice(h * ROWS, (h + 1) * ROWS)
        for p in range(TEAM):
            for f in range(FRAMES):
                v = turn[pl.ds(p * FRAMES + f, few * 8, stride=TROWS)].astype(BF16)
                mine[p, f, put] = v.reshape(ROWS, 4, LANES)
        here = pl.ds(pl.multiple_of(q * LANES, LANES), LANES)
        for k in (3, 2, 1):
            p = lax.rem(q + k, TEAM)
            remote(mine.at[p, :, put], out.at[:, put, :, here], outsend, outrecv, {"groups": group_at(p)}).start()
        out[:, put, :, here] = mine[q, :, put]
    wait_bytes(mine.at[pl.ds(0, TEAM - 1)], outrecv)
    wait_bytes(mine.at[pl.ds(0, TEAM - 1)], outsend)


VMEM = pl.BlockSpec(memory_space=pltpu.VMEM)
HBM = pl.BlockSpec(memory_space=pltpu.HBM)


def shards(ny, hidden, norm_gain, norm_shift, conv_weight, conv_bias):
    nd = lax.axis_size("space")
    nz = nd // 2
    wide, channels = hidden.shape
    tiles = channels // LANES
    cin = conv_weight.shape[3]
    batches = len(rounds_of(nz // 2)) + 1
    wq = conv_weight.reshape(3, TAPS, cin, conv_weight.shape[4])
    scratch = [pltpu.VMEM((tiles, 1, LANES), F32)] * 2 + [
        pltpu.VMEM((tiles, LANES), BF16),
        pltpu.VMEM((3, nd, TAPS, cin, LANES), BF16),
        pltpu.VMEM((3, channels, 16 * LANES), BF16),
        pltpu.VMEM((TEAM, nz, 6, 8, LANES), BF16),
        pltpu.VMEM((TEAM, 1, LANES), F32),
        pltpu.VMEM((2, wide, channels), BF16),
        pltpu.VMEM((wide, 8, LANES), BF16),
        pltpu.VMEM((wide * 8, LANES), F32),
        pltpu.VMEM((nz, 1, LANES), F32),
        pltpu.VMEM((1, LANES), F32),
        pltpu.VMEM((1, LANES), F32),
        pltpu.VMEM((ROWS // 2 * 16 * YROWS, LANES), F32),
        pltpu.VMEM((ROWS + 2, 4, 16, channels), BF16),
        pltpu.VMEM((2, 3, ROWS * 16, 4 * LANES), F32),
        pltpu.VMEM((ROWS * 4 * TROWS, LANES), F32),
        pltpu.VMEM((TEAM, FRAMES, ROWS * 2, 4, LANES), BF16),
        DMA((5,)), DMA((2,)), DMA((2, nz // 2, 3)), DMA, DMA((nz // 2 + 1,)), DMA((2, 4)),
        pltpu.SemaphoreType.REGULAR((max(1, batches - 1),)),
        DMA, DMA((batches,)), DMA, DMA, DMA, DMA((batches + 1,)), DMA, DMA, DMA((2,)), DMA, DMA((2,)), DMA((2,)), DMA, DMA,
    ]
    operands = (hidden, wq, norm_gain.reshape(tiles, 1, LANES), norm_shift.reshape(tiles, 1, LANES), conv_bias.reshape(tiles, LANES))
    return pl.pallas_call(
        functools.partial(kernel, ny, nd),
        out_shape=pltpu.VMEM((FRAMES, ROWS * 2, 4, channels), BF16),
        in_specs=[HBM] * 5,
        out_specs=VMEM,
        scratch_shapes=scratch,
        compiler_params=pltpu.CompilerParams(collective_id=0, has_side_effects=True, vmem_limit_bytes=40 * MIB),
        name="decode",
    )(*(pltpu.with_memory_space_constraint(v, pltpu.HBM) for v in operands))


def solution(mesh):
    ny = len({d.coords[1] for d in mesh.devices.flat})
    return jax.shard_map(
        functools.partial(shards, ny),
        mesh=mesh,
        in_specs=(P(("groups", "space"), None), P(), P(), P(None, None, None, "space", None), P()),
        out_specs=P("groups", None, "space", None),
        check_vma=False,
    )
```

```python
import functools

import jax
import jax.numpy as jnp
from jax import lax
from jax.experimental import pallas as pl
from jax.experimental.pallas import tpu as pltpu
from jax.sharding import PartitionSpec as P

GROUP = 16
FRAMES = 4
ROWS = 16
LANES = 128
TEAM = 4
TAPS = 9
EPSILON = 1e-6
PARTS = (4, 4, 4, 4)
MIB = 1 << 20
YROWS = 40
TROWS = 24
NEAR = 6

DMA = pltpu.SemaphoreType.DMA
F32, BF16 = jnp.float32, jnp.bfloat16
SHIFTS = [(0, 0), (0, -1), (0, 1), (-1, 0), (1, 0), (-1, -1), (-1, 1), (1, -1), (1, 1)]


def phases_of(dr, dc):
    rows = {-1: (0,), 0: (0, 1), 1: (1,)}
    return [(a, b) for a in rows[dr] for b in rows[dc]]


COLUMNS = [(s, p) for s in SHIFTS for p in phases_of(*s)]


def remote(src, dst, send, recv, device):
    return pltpu.make_async_remote_copy(
        src_ref=src, dst_ref=dst, send_sem=send, recv_sem=recv,
        device_id=device, device_id_type=pl.DeviceIdType.MESH,
    )


def signal(sem, device):
    pl.semaphore_signal(sem, inc=1, device_id=device, device_id_type=pl.DeviceIdType.MESH)


def wait_bytes(ref, sem):
    pltpu.make_async_copy(ref, ref, sem).wait()


def team(ny):
    g = lax.axis_index("groups")
    x, y = g // ny, g % ny
    x0, y0 = x - x % 2, y - y % 2
    q = (x % 2) * 2 + y % 2
    others = (3 - q, (q + 2) % TEAM, q + 1 - 2 * (q % 2))
    return q, others, lambda p: (x0 + p // 2) * ny + y0 + p % 2


def group_matrix():
    lane = lax.broadcasted_iota(jnp.int32, (LANES, LANES), 0)
    packed = lax.broadcasted_iota(jnp.int32, (LANES, LANES), 1)
    return jnp.where(lane // GROUP == packed % 8, 1.0, 0.0).astype(F32)


def packed_mask(which):
    row = lax.broadcasted_iota(jnp.int32, (8, LANES), 0)
    lane = lax.broadcasted_iota(jnp.int32, (8, LANES), 1)
    return (lane // 32 == which) & ((lane // 8) % 4 == row % 4)


def hdot(a, b):
    return jnp.dot(a, b, preferred_element_type=F32, precision=lax.Precision.HIGHEST)


def pack(sums, which):
    return jnp.sum(jnp.where(packed_mask(which), hdot(sums, group_matrix()), 0.0), axis=0, keepdims=True)


def unpack(row, which):
    spread = jnp.where(packed_mask(which), jnp.broadcast_to(row, (8, LANES)), 0.0)
    return hdot(spread, group_matrix().T)


def rounds_of(half):
    known, steps = 1, []
    while known < half:
        step = min(known, max(1, half // 4))
        known += step
        steps.append((step, min(known, half)))
    return steps


def kernel(ny, nd, h_ref, wq_ref, gain_ref, shift_ref, bias_ref, out, gain, shift, bias,
           w, mix, acts, totals, raw, cells, flat, stats, row, tot, ys, a, acc, turn, mine,
           local, ringsend, ringrecv, give, giverecv, own, ask, a2asend, a2arecv,
           statsend, statrecv, partsend, partrecv, northsend, northrecv, edgesend, edgerecv, outersend, outerrecv, totsend, totrecv, outsend, outrecv):
    me = lax.axis_index("space")
    z, c = me // 2, me % 2
    nz = nd // 2
    half = nz // 2
    q, others, group_at = team(ny)
    leaps = (half - NEAR) // 2
    assert NEAR + 2 * leaps == half
    rounds = rounds_of(half)
    spans, last = [], 0
    for known in [1] + [r[1] for r in rounds]:
        spans.append((last + 1, known))
        last = known
    sizes = [2 * (hi - lo + 1) - (1 if hi == half else 0) for lo, hi in spans]

    def at(zz, core):
        return {"space": lax.rem(zz + 2 * nz, nz) * 2 + core}

    sibling = {"space": z * 2 + 1 - c}
    middle = pl.ds(1, 4)
    norths = pl.ds(2, 3)
    barrier = pltpu.get_barrier_semaphore()

    def blend(zz):
        zz = lax.rem(zz + 2 * nz, nz)
        for dt in range(3):
            tap = [w[dt, pl.ds(zz * 2, 2), n].astype(F32).reshape(16, LANES) for n in range(TAPS)]

            def sums(x):
                return {(0, -1): x[0], (0, 0): x[1] + x[2], (1, 0): x[0] + x[1], (1, 1): x[2]}

            by_row = [sums([tap[n * 3 + e] for n in range(3)]) for e in range(3)]
            both = {k: sums([by_row[e][k] for e in range(3)]) for k in by_row[0]}
            for n, ((dr, dc), (pr, pc)) in enumerate(COLUMNS):
                mix[dt, pl.ds(pl.multiple_of(zz * 16, 16), 16), n * LANES:(n + 1) * LANES] = both[(pr, dr)][(pc, dc)].astype(BF16)

    channels = a.shape[-1]
    tiles = channels // LANES
    pairs = ROWS // 2

    def activate(places):
        g = jnp.concatenate([gain[t] for t in range(tiles)] * 2, axis=0)
        b = jnp.concatenate([shift[t] for t in range(tiles)] * 2, axis=0)
        for p in places:
            mean = unpack(totals[p], 0)
            scale = g * lax.rsqrt(unpack(totals[p], 1) + EPSILON)
            move = (b - mean * scale) * 0.5
            scale = scale * 0.5

            @pl.loop(0, pairs, unroll=4)
            def _(rp):
                for f in range(FRAMES):
                    v = acts[p, lax.rem(f * pairs + rp + nz - z, nz), pl.ds(2 * c, 4)].astype(F32)
                    v = v * scale[None] + move[None]
                    v = v * jnp.tanh(v) + v
                    start = rp * (16 * YROWS) + (p * FRAMES + f) * YROWS
                    ys[pl.ds(pl.multiple_of(start, 8), 32)] = v.reshape(32, LANES)

    def arrange():
        @pl.loop(0, pairs)
        def _(rp):
            for col in range(4):
                for r in range(2):
                    for t in range(tiles):
                        v = ys[pl.ds(rp * (16 * YROWS) + col * 8 + r * tiles + t, 16, stride=YROWS)].astype(BF16)
                        a[rp * 2 + r + 1, col, :, t * LANES:(t + 1) * LANES] = v

        a[0] = a[1]
        a[ROWS + 1] = a[ROWS]

    chips = LANES // 16
    first_block = z // chips + jnp.where(z % chips < chips // 2, tiles - 1, 0)
    assert half - 4 >= chips * 3 // 2 - 1 and tiles == 4

    def multiply(row0, few, late):
        part = slice(row0 * 32, (row0 + few) * 32)
        blocks = [pl.ds(pl.multiple_of(lax.rem(first_block + 2 * late + i, tiles) * LANES, LANES), LANES) for i in range(2)]
        for dt in range(3):
            col0 = 0
            for dr, dc in SHIFTS:
                ps = phases_of(dr, dc)
                rows, cols = slice(1 + dr + row0, 1 + dr + row0 + few), slice(1 + dc, 3 + dc)
                lhs = jnp.concatenate([a[rows, cols, :, k].reshape(few * 2 * 16, LANES) for k in blocks], axis=1)
                rhs = jnp.concatenate([mix[dt, k, col0:col0 + len(ps) * LANES] for k in blocks], axis=0)
                r = jnp.dot(lhs, rhs, preferred_element_type=F32)
                col0 += len(ps) * LANES
                if (dr, dc) == (0, 0):
                    acc[dt, part] = acc[dt, part] + r if late else r
                else:
                    for n, (pr, pc) in enumerate(ps):
                        to = slice((pr * 2 + pc) * LANES, (pr * 2 + pc + 1) * LANES)
                        acc[dt, part, to] += r[:, n * LANES:(n + 1) * LANES]

    load = pltpu.make_async_copy(wq_ref.at[:, :, :, pl.ds(q * LANES, LANES)], w.at[:, me], local.at[0])
    rows_in = pltpu.make_async_copy(h_ref, raw.at[0], local.at[1])
    small = [pltpu.make_async_copy(src, dst, local.at[2 + i])
             for i, (src, dst) in enumerate(((gain_ref, gain), (shift_ref, shift), (bias_ref, bias)))]

    @pl.when(c == 1)
    def _():
        signal(barrier, at(z + 1, 1))
        signal(barrier, at(z - 1, 1))
        signal(barrier, sibling)
        load.start()
        rows_in.start()
        for copy in small:
            copy.start()
        pl.semaphore_wait(barrier, 3)
        rows_in.wait()
        rows_out = remote(raw.at[0], raw.at[1], own.at[0, 0], own.at[1, 0], sibling)
        rows_out.start()
        load.wait()

        def piece(zz, j):
            return w.at[j, pl.ds(lax.rem(zz + 2 * nz, nz) * 2, 2)]

        def hop(way, p, d, j, step=1):
            to = z + step if way == 0 else z - step
            return remote(p, p, ringsend.at[way], ringrecv.at[way, d - 1, j], at(to, 1))

        def first(part, j):
            for way in (0, 1):
                hop(way, part, 1, j).start()

        for j in range(3):
            m = w.at[j, me]
            first(m, j)
            remote(m, m, give, giverecv.at[half], sibling).start()
        for j in range(3):
            theirs = w.at[j, z * 2]
            remote(theirs, theirs, own.at[0, 1 + j], own.at[1, 1 + j], sibling).wait_recv()
            first(theirs, j)
        blend(z)

        def take(way, d, j, s, on):
            p = piece(z - d if way == 0 else z + d, j)
            hop(way, p, d, j).wait_recv()
            for step in on:
                hop(way, p, d + step, j, step).start()
            remote(p, p, give, giverecv.at[s], sibling).start()

        @pl.loop(0, NEAR - 1)
        def _(s):
            for j in range(3):
                take(0, s + 1, j, s, (1,))
                take(1, s + 1, j, s, (1,))
            blend(z - s - 1)
            blend(z + s + 1)

        @pl.loop(0, leaps - 1)
        def _(u):
            d, s = NEAR + 2 * u, NEAR - 1 + u
            for j in range(3):
                take(0, d, j, s, (2, 1))
                take(1, d, j, s, (2, 1))
            blend(z - d)
            blend(z + d)

            @pl.when(u == leaps - 2)
            def _():
                wait_bytes(acts.at[:, :, pl.ds(2, 3)], northrecv)
                remote(totals, totals, totsend.at[1], totrecv.at[1], sibling).wait_recv()

                @pl.when(z < nz - 1)
                def _():
                    wait_bytes(acts.at[:, :, 5], outerrecv)

                @pl.when(z == nz - 1)
                def _():
                    acts[:, :, 5] = acts[:, :, 4]

                for copy in small:
                    copy.wait()
                activate((0, 1))

            @pl.when(u > 0)
            def _():
                for j in range(3):
                    take(0, d - 1, j, s, ())
                    take(1, d - 1, j, s, ())
                blend(z - d + 1)
                blend(z + d - 1)

        activate((2, 3))
        arrange()
        d, s = half - 2, NEAR - 2 + leaps
        for j in range(3):
            take(0, d, j, s, (2, 1) if j < 2 else (1,))
            take(1, d, j, s, (1,) if j < 2 else (2, 1))
        blend(z - d)
        blend(z + d)
        for j in range(3):
            take(0, d - 1, j, s, ())
            take(1, d - 1, j, s, ())
        blend(z - d + 1)
        blend(z + d - 1)
        multiply(0, ROWS // 2, 0)
        multiply(ROWS // 2, ROWS // 2, 0)
        s = NEAR - 1 + leaps
        for j in range(3):
            take(0, half - 1, j, s, ())
            take(1, half - 1, j, s, ())
        blend(z - half + 1)
        blend(z + half - 1)
        for j in range(3):
            take(0 if j < 2 else 1, half, j, s, ())
        blend(z + half)

    @pl.when(c == 0)
    def _():
        signal(barrier, at(z + 1, 0))
        signal(barrier, at(z - 1, 0))
        signal(barrier, sibling)
        for p in others:
            signal(barrier, {"groups": group_at(p)})
        load.start()
        rows_in.start()
        for copy in small:
            copy.start()
        pl.semaphore_wait(barrier, 2 + TEAM)

        def tell(k):
            if k < len(rounds):
                signal(ask.at[k], at(z + rounds[k][0], 0))
                signal(ask.at[k], at(z - rounds[k][0], 0))

        tell(0)
        load.wait()
        for j in range(3):
            p = w.at[j, me]
            remote(p, p, own.at[0, 1 + j], own.at[1, 1 + j], sibling).start()
        early = min(2, len(rounds))
        for k in range(early):
            pl.semaphore_wait(ask.at[k], 2)
            tell(k + 1)
        rows_in.wait()
        remote(raw.at[0], raw.at[1], own.at[0, 0], own.at[1, 0], sibling).wait_recv()

        wide = raw.shape[1]
        for r in range(2):
            for t in range(tiles):
                flat[pl.ds(r * tiles + t, wide, stride=8)] = raw[r, :, t * LANES:(t + 1) * LANES].astype(F32)
        x = flat[...].reshape(wide, 8, LANES)
        cells[...] = x.astype(BF16)

        def each(b, body):
            lo, hi = spans[b]

            @pl.loop(lo, min(hi, half - 1) + 1)
            def _(d):
                body(d)
                body(-d)

            if hi == half:
                body(half)

        def runs(b):
            if b == len(spans):
                return [(0, 1)]
            lo, hi = spans[b]
            low = min(hi, half - 1)
            return [(lo, hi - lo + 1), (nz - low, low - lo + 1)]

        def for_chip(zz):
            return cells.at[pl.ds(zz * 4, 4)]

        def send_rows(b):
            def body(d):
                zz = lax.rem(z + d + nz, nz)
                remote(for_chip(zz), acts.at[q, lax.rem(nz - d, nz), middle], a2asend, a2arecv.at[b], at(zz, 0)).start()
            each(b, body)

        def send_stats(b):
            each(b, lambda d: remote(row, stats.at[z], statsend, statrecv, at(z + d, 0)).start())

        def pass_on(b, at0, n, rows, first, last):
            for p in others:
                remote(rows(middle), acts.at[q, pl.ds(at0, n), middle], partsend, partrecv.at[b], {"groups": group_at(p)}).start()

            @pl.when(z < nz - 1)
            def _():
                remote(last, acts.at[q, pl.ds((at0 + nz - 1) % nz, n), 0], edgesend.at[0], edgerecv.at[0, b], at(z + 1, 0)).start()

            @pl.when(z > 0)
            def _():
                remote(first, acts.at[q, pl.ds((at0 + 1) % nz, n), 5], edgesend.at[1], edgerecv.at[1, b], at(z - 1, 0)).start()

            remote(rows(norths), acts.at[q, pl.ds(at0, n), norths], northsend, northrecv, sibling).start()

        def share_edges(b):
            total = sum(n for _, n in runs(b))

            @pl.when(z > 0)
            def _():
                wait_bytes(acts.at[0, pl.ds(0, total), 0], edgerecv.at[0, b])
                for at0, n in runs(b):
                    e = acts.at[q, pl.ds((at0 + nz - 1) % nz, n), 0]
                    for p in others:
                        remote(e, e, outersend.at[0], outerrecv, {"groups": group_at(p)}).start()

            @pl.when(z < nz - 1)
            def _():
                wait_bytes(acts.at[0, pl.ds(0, total), 5], edgerecv.at[1, b])
                for at0, n in runs(b):
                    e = acts.at[q, pl.ds((at0 + 1) % nz, n), 5]
                    for p in others:
                        remote(e, e, outersend.at[1], outerrecv, {"groups": group_at(p), "space": z * 2 + 1}).start()
                    remote(e, e, outersend.at[1], outerrecv, sibling).start()

        for b in range(early + 1):
            send_rows(b)
        own_cells = len(spans)
        for p in others:
            remote(for_chip(z), acts.at[q, 0, middle], partsend, partrecv.at[own_cells], {"groups": group_at(p)}).start()
        remote(cells.at[pl.ds(z * 4 + 1, 3)], acts.at[q, 0, norths], northsend, northrecv, sibling).start()

        count = float(2 * wide * GROUP)
        first = pack(jnp.sum(flat[...].reshape(wide, 8, LANES), axis=0), 0)
        mean = unpack(first, 0) * (1.0 / count)
        second = pack(jnp.sum((flat[...].reshape(wide, 8, LANES) - mean[None]) ** 2, axis=0), 1)
        row[...] = first + second
        stats[z] = row[...]
        acts[q, 0, 1:5] = cells[pl.ds(z * 4, 4)]
        for b in range(early + 1):
            send_stats(b)

        for k in range(early, len(rounds)):
            pl.semaphore_wait(ask.at[k], 2)
            tell(k + 1)
            send_rows(k + 1)
            send_stats(k + 1)

        def from_team(b):
            total = sum(n for _, n in runs(b))
            wait_bytes(acts.at[pl.ds(0, TEAM - 1), pl.ds(0, total), middle], partrecv.at[b])
            for at0, n in runs(b):
                for p in others:
                    c3 = acts.at[p, pl.ds(at0, n), norths]
                    remote(c3, c3, northsend, northrecv, sibling).start()

        from_team(own_cells)

        @pl.when(z < nz - 1)
        def _():
            remote(cells.at[z * 4 + 3], acts.at[q, nz - 1, 0], edgesend.at[0], edgerecv.at[0, own_cells], at(z + 1, 0)).start()

        @pl.when(z > 0)
        def _():
            remote(cells.at[z * 4], acts.at[q, 1, 5], edgesend.at[1], edgerecv.at[1, own_cells], at(z - 1, 0)).start()

        share_edges(own_cells)
        for b in range(len(spans)):
            if b == len(spans) - 1:
                wait_bytes(stats.at[pl.ds(0, nz - 1)], statrecv)
                every = stats[...].reshape(nz, LANES)
                lane = lax.broadcasted_iota(jnp.int32, (nz, LANES), 1)
                mean = jnp.sum(every, axis=0, keepdims=True) * (1.0 / (count * nz))
                off = jnp.where(lane < 32, (every * (1.0 / count) - mean) ** 2 * count, 0.0)
                spread = jnp.where(lane < 32, 0.0, every)
                spread = jnp.sum(spread + pltpu.roll(off, 32, 1), axis=0, keepdims=True) * (1.0 / (count * nz))
                tot[...] = jnp.where(lane[:1] < 32, mean, spread)
                totals[q] = tot[...]
                for p in others:
                    remote(tot, totals.at[q], totsend.at[0], totrecv.at[0], {"groups": group_at(p)}).start()
            wait_bytes(acts.at[0, pl.ds(0, sizes[b]), middle], a2arecv.at[b])

            for at0, n in runs(b):
                pass_on(b, at0, n, lambda cols, at0=at0, n=n: acts.at[q, pl.ds(at0, n), cols],
                        acts.at[q, pl.ds(at0, n), 1], acts.at[q, pl.ds(at0, n), 4])
            if b > 0:
                share_edges(b - 1)

        wait_bytes(totals.at[pl.ds(0, TEAM - 1)], totrecv.at[0])
        remote(totals, totals, totsend.at[1], totrecv.at[1], sibling).start()
        for b in range(len(spans) - 1):
            from_team(b)
        share_edges(len(spans) - 1)
        from_team(len(spans) - 1)

        @pl.when(z > 0)
        def _():
            wait_bytes(acts.at[pl.ds(0, TEAM - 1), :, 0], outerrecv)

        @pl.when(z == 0)
        def _():
            acts[:, :, 0] = acts[:, :, 1]

        for copy in small:
            copy.wait()
        activate(range(TEAM))
        arrange()
        wait_bytes(w.at[:, 0], giverecv.at[half])
        blend(z)

        @pl.loop(0, NEAR - 1)
        def _(s):
            wait_bytes(w.at[:, pl.ds(0, 4)], giverecv.at[s])
            blend(z - s - 1)
            blend(z + s + 1)

        wait_bytes(w.at[:, pl.ds(0, 4)], giverecv.at[NEAR - 1])
        blend(z - NEAR)
        blend(z + NEAR)

        @pl.loop(1, leaps)
        def _(u):
            wait_bytes(w.at[:, pl.ds(0, 8)], giverecv.at[NEAR - 1 + u])
            for d in (0, -1):
                blend(z - NEAR - 2 * u - d)
                blend(z + NEAR + 2 * u + d)

            @pl.when(u >= leaps - 2)
            def _():
                @pl.when(u == leaps - 2)
                def _():
                    multiply(0, ROWS // 2, 0)

                @pl.when(u == leaps - 1)
                def _():
                    multiply(ROWS // 2, ROWS // 2, 0)

        wait_bytes(w.at[:, pl.ds(0, 6)], giverecv.at[NEAR - 1 + leaps])
        blend(z - half + 1)
        blend(z + half - 1)
        blend(z + half)

    frame = lax.broadcasted_iota(jnp.int32, (8, LANES), 0) % FRAMES
    which = lax.broadcasted_iota(jnp.int32, (tiles, LANES), 0)
    bias_row = jnp.sum(jnp.where(which == q, bias[...].astype(F32), 0.0), axis=0, keepdims=True)
    row0 = 0
    for few in PARTS:
        multiply(row0, few, 1)
        for r in range(few):
            for cc in range(2):
                for n in range(4):
                    i = ((r * 2 + n // 2) * 2 + cc) * 2 + n % 2
                    for half_tile in range(2):
                        at_row = ((row0 + r) * 2 + cc) * 16 + half_tile * 8
                        old, mid, new = (acc[dt, at_row:at_row + 8, n * LANES:(n + 1) * LANES] for dt in range(3))
                        mid = jnp.where(frame >= 1, pltpu.roll(mid, 1, 0), mid)
                        old = jnp.where(frame >= 2, pltpu.roll(old, 2, 0), jnp.where(frame >= 1, pltpu.roll(old, 1, 0), old))
                        turn[i * TROWS + half_tile * 8:i * TROWS + half_tile * 8 + 8] = old + mid + new + bias_row
        put = slice(row0 * 2, (row0 + few) * 2)
        row0 += few
        for p in range(TEAM):
            for f in range(FRAMES):
                v = turn[pl.ds(p * FRAMES + f, few * 8, stride=TROWS)].astype(BF16)
                mine[p, f, put] = v.reshape(few * 2, 4, LANES)
        here = pl.ds(pl.multiple_of(q * LANES, LANES), LANES)
        for p in others:
            remote(mine.at[p, :, put], out.at[:, put, :, here], outsend, outrecv, {"groups": group_at(p)}).start()
        out[:, put, :, here] = mine[q, :, put]
    @pl.when(c == 1)
    def _():
        wait_bytes(raw.at[0], own.at[0, 0])
        for way, rest in ((0, pl.ds(0, 2)), (1, pl.ds(0, 1))):
            wait_bytes(w.at[:, pl.ds(0, 2 * half - 2)], ringsend.at[way])
            wait_bytes(w.at[rest, pl.ds(0, 2)], ringsend.at[way])
        wait_bytes(w.at[:, pl.ds(0, nd - 1)], give)

    @pl.when(c == 0)
    def _():
        for j in range(3):
            wait_bytes(w.at[j, me], own.at[0, 1 + j])
        wait_bytes(stats.at[pl.ds(0, nz - 1)], statsend)
        wait_bytes(acts.at[0, pl.ds(0, nz - 1), middle], a2asend)
        wait_bytes(acts.at[pl.ds(0, TEAM - 1), :, middle], partsend)
        wait_bytes(acts.at[:, :, norths], northsend)

        @pl.when(z < nz - 1)
        def _():
            wait_bytes(acts.at[0, :, 0], edgesend.at[0])
            wait_bytes(acts.at[:, :, 5], outersend.at[1])

        @pl.when(z > 0)
        def _():
            wait_bytes(acts.at[0, :, 5], edgesend.at[1])
            wait_bytes(acts.at[pl.ds(0, TEAM - 1), :, 0], outersend.at[0])
        wait_bytes(totals.at[pl.ds(0, TEAM - 1)], totsend.at[0])
        wait_bytes(totals, totsend.at[1])

    wait_bytes(mine.at[pl.ds(0, TEAM - 1)], outrecv)
    wait_bytes(mine.at[pl.ds(0, TEAM - 1)], outsend)


VMEM = pl.BlockSpec(memory_space=pltpu.VMEM)
HBM = pl.BlockSpec(memory_space=pltpu.HBM)


def shards(ny, hidden, norm_gain, norm_shift, conv_weight, conv_bias):
    nd = lax.axis_size("space")
    nz = nd // 2
    wide, channels = hidden.shape
    tiles = channels // LANES
    cin = conv_weight.shape[3]
    batches = len(rounds_of(nz // 2)) + 1
    wq = conv_weight.reshape(3, TAPS, cin, conv_weight.shape[4])
    scratch = [pltpu.VMEM((tiles, 1, LANES), F32)] * 2 + [
        pltpu.VMEM((tiles, LANES), BF16),
        pltpu.VMEM((3, nd, TAPS, cin, LANES), BF16),
        pltpu.VMEM((3, channels, 16 * LANES), BF16),
        pltpu.VMEM((TEAM, nz, 6, 8, LANES), BF16),
        pltpu.VMEM((TEAM, 1, LANES), F32),
        pltpu.VMEM((2, wide, channels), BF16),
        pltpu.VMEM((wide, 8, LANES), BF16),
        pltpu.VMEM((wide * 8, LANES), F32),
        pltpu.VMEM((nz, 1, LANES), F32),
        pltpu.VMEM((1, LANES), F32),
        pltpu.VMEM((1, LANES), F32),
        pltpu.VMEM((ROWS // 2 * 16 * YROWS, LANES), F32),
        pltpu.VMEM((ROWS + 2, 4, 16, channels), BF16),
        pltpu.VMEM((3, ROWS * 32, 4 * LANES), F32),
        pltpu.VMEM((ROWS * 4 * TROWS, LANES), F32),
        pltpu.VMEM((TEAM, FRAMES, ROWS * 2, 4, LANES), BF16),
        DMA((5,)), DMA((2,)), DMA((2, nz // 2, 3)), DMA, DMA((nz // 2 + 1,)), DMA((2, 4)),
        pltpu.SemaphoreType.REGULAR((max(1, batches - 1),)),
        DMA, DMA((batches,)), DMA, DMA, DMA, DMA((batches + 1,)), DMA, DMA, DMA((2,)), DMA((2, batches + 1)), DMA((2,)), DMA, DMA((2,)), DMA((2,)), DMA, DMA,
    ]
    operands = (hidden, wq, norm_gain.reshape(tiles, 1, LANES), norm_shift.reshape(tiles, 1, LANES), conv_bias.reshape(tiles, LANES))
    return pl.pallas_call(
        functools.partial(kernel, ny, nd),
        out_shape=pltpu.VMEM((FRAMES, ROWS * 2, 4, channels), BF16),
        in_specs=[HBM] * 5,
        out_specs=VMEM,
        scratch_shapes=scratch,
        compiler_params=pltpu.CompilerParams(collective_id=0, has_side_effects=True, vmem_limit_bytes=40 * MIB),
        name="decode",
    )(*(pltpu.with_memory_space_constraint(v, pltpu.HBM) for v in operands))


def solution(mesh):
    ny = len({d.coords[1] for d in mesh.devices.flat})
    return jax.shard_map(
        functools.partial(shards, ny),
        mesh=mesh,
        in_specs=(P(("groups", "space"), None), P(), P(), P(None, None, None, "space", None), P()),
        out_specs=P("groups", None, "space", None),
        check_vma=False,
    )
```

```python
import functools

import jax
import jax.numpy as jnp
from jax import lax
from jax.experimental import pallas as pl
from jax.experimental.pallas import tpu as pltpu
from jax.sharding import PartitionSpec as P

GROUP = 16
FRAMES = 4
ROWS = 16
LANES = 128
TEAM = 4
TAPS = 9
EPSILON = 1e-6
PARTS = (4, 4, 4, 4)
MIB = 1 << 20
YROWS = 40
TROWS = 24
NEAR = 6

DMA = pltpu.SemaphoreType.DMA
F32, BF16 = jnp.float32, jnp.bfloat16
SHIFTS = [(0, 0), (0, -1), (0, 1), (-1, 0), (1, 0), (-1, -1), (-1, 1), (1, -1), (1, 1)]


def phases_of(dr, dc):
    rows = {-1: (0,), 0: (0, 1), 1: (1,)}
    return [(a, b) for a in rows[dr] for b in rows[dc]]


COLUMNS = [(s, p) for s in SHIFTS for p in phases_of(*s)]


def remote(src, dst, send, recv, device):
    return pltpu.make_async_remote_copy(
        src_ref=src, dst_ref=dst, send_sem=send, recv_sem=recv,
        device_id=device, device_id_type=pl.DeviceIdType.MESH,
    )


def signal(sem, device):
    pl.semaphore_signal(sem, inc=1, device_id=device, device_id_type=pl.DeviceIdType.MESH)


def wait_bytes(ref, sem):
    pltpu.make_async_copy(ref, ref, sem).wait()


def team(ny):
    g = lax.axis_index("groups")
    x, y = g // ny, g % ny
    x0, y0 = x - x % 2, y - y % 2
    q = (x % 2) * 2 + y % 2
    others = (3 - q, (q + 2) % TEAM, q + 1 - 2 * (q % 2))
    return q, others, lambda p: (x0 + p // 2) * ny + y0 + p % 2


def group_matrix():
    lane = lax.broadcasted_iota(jnp.int32, (LANES, LANES), 0)
    packed = lax.broadcasted_iota(jnp.int32, (LANES, LANES), 1)
    return jnp.where(lane // GROUP == packed % 8, 1.0, 0.0).astype(F32)


def packed_mask(which):
    row = lax.broadcasted_iota(jnp.int32, (8, LANES), 0)
    lane = lax.broadcasted_iota(jnp.int32, (8, LANES), 1)
    return (lane // 32 == which) & ((lane // 8) % 4 == row % 4)


def hdot(a, b):
    return jnp.dot(a, b, preferred_element_type=F32, precision=lax.Precision.HIGHEST)


def pack(sums, which):
    return jnp.sum(jnp.where(packed_mask(which), hdot(sums, group_matrix()), 0.0), axis=0, keepdims=True)


def unpack(row, which):
    spread = jnp.where(packed_mask(which), jnp.broadcast_to(row, (8, LANES)), 0.0)
    return hdot(spread, group_matrix().T)


def rounds_of(half):
    known, steps = 1, []
    while known < half:
        step = min(known, max(1, half // 4))
        known += step
        steps.append((step, min(known, half)))
    return steps


def kernel(ny, nd, h_ref, wq_ref, gain_ref, shift_ref, bias_ref, out, gain, shift, bias,
           w, mix, acts, totals, raw, cells, flat, stats, row, tot, ys, a, acc, turn, mine,
           local, ringsend, ringrecv, give, giverecv, own, ask, a2asend, a2arecv,
           statsend, statrecv, partsend, partrecv, northsend, northrecv, edgesend, edgerecv, outersend, outerrecv, totsend, totrecv, outsend, outrecv):
    me = lax.axis_index("space")
    z, c = me // 2, me % 2
    nz = nd // 2
    half = nz // 2
    q, others, group_at = team(ny)
    leaps = (half - NEAR) // 2
    assert NEAR + 2 * leaps == half
    rounds = rounds_of(half)
    spans, last = [], 0
    for known in [1] + [r[1] for r in rounds]:
        spans.append((last + 1, known))
        last = known
    sizes = [2 * (hi - lo + 1) - (1 if hi == half else 0) for lo, hi in spans]

    def at(zz, core):
        return {"space": lax.rem(zz + 2 * nz, nz) * 2 + core}

    sibling = {"space": z * 2 + 1 - c}
    middle = pl.ds(1, 4)
    norths = pl.ds(2, 3)
    barrier = pltpu.get_barrier_semaphore()

    def blend(zz):
        zz = lax.rem(zz + 2 * nz, nz)
        for dt in range(3):
            tap = [w[dt, pl.ds(zz * 2, 2), n].astype(F32).reshape(16, LANES) for n in range(TAPS)]

            def sums(x):
                return {(0, -1): x[0], (0, 0): x[1] + x[2], (1, 0): x[0] + x[1], (1, 1): x[2]}

            by_row = [sums([tap[n * 3 + e] for n in range(3)]) for e in range(3)]
            both = {k: sums([by_row[e][k] for e in range(3)]) for k in by_row[0]}
            for n, ((dr, dc), (pr, pc)) in enumerate(COLUMNS):
                mix[dt, pl.ds(pl.multiple_of(zz * 16, 16), 16), n * LANES:(n + 1) * LANES] = both[(pr, dr)][(pc, dc)].astype(BF16)

    channels = a.shape[-1]
    tiles = channels // LANES
    pairs = ROWS // 2

    def activate(places):
        g = jnp.concatenate([gain[t] for t in range(tiles)] * 2, axis=0)
        b = jnp.concatenate([shift[t] for t in range(tiles)] * 2, axis=0)
        for p in places:
            mean = unpack(totals[p], 0)
            scale = g * lax.rsqrt(unpack(totals[p], 1) + EPSILON)
            scale, move = scale * 0.5, b * 0.5

            @pl.loop(0, pairs, unroll=4)
            def _(rp):
                for f in range(FRAMES):
                    v = acts[p, lax.rem(f * pairs + rp + nz - z, nz), pl.ds(2 * c, 4)].astype(F32)
                    v = (v - mean[None]) * scale[None] + move[None]
                    v = v * jnp.tanh(v) + v
                    start = rp * (16 * YROWS) + (p * FRAMES + f) * YROWS
                    ys[pl.ds(pl.multiple_of(start, 8), 32)] = v.reshape(32, LANES)

    def arrange():
        @pl.loop(0, pairs)
        def _(rp):
            for col in range(4):
                for r in range(2):
                    for t in range(tiles):
                        v = ys[pl.ds(rp * (16 * YROWS) + col * 8 + r * tiles + t, 16, stride=YROWS)].astype(BF16)
                        a[rp * 2 + r + 1, col, :, t * LANES:(t + 1) * LANES] = v

        a[0] = a[1]
        a[ROWS + 1] = a[ROWS]

    chips = LANES // 16
    first_block = z // chips + jnp.where(z % chips < chips // 2, tiles - 1, 0)
    assert half - 4 >= chips * 3 // 2 - 1 and tiles == 4

    def multiply(row0, few, late):
        part = slice(row0 * 32, (row0 + few) * 32)
        blocks = [pl.ds(pl.multiple_of(lax.rem(first_block + 2 * late + i, tiles) * LANES, LANES), LANES) for i in range(2)]
        for dt in range(3):
            col0 = 0
            for dr, dc in SHIFTS:
                ps = phases_of(dr, dc)
                rows, cols = slice(1 + dr + row0, 1 + dr + row0 + few), slice(1 + dc, 3 + dc)
                lhs = jnp.concatenate([a[rows, cols, :, k].reshape(few * 2 * 16, LANES) for k in blocks], axis=1)
                rhs = jnp.concatenate([mix[dt, k, col0:col0 + len(ps) * LANES] for k in blocks], axis=0)
                r = jnp.dot(lhs, rhs, preferred_element_type=F32)
                col0 += len(ps) * LANES
                if (dr, dc) == (0, 0):
                    acc[dt, part] = acc[dt, part] + r if late else r
                else:
                    for n, (pr, pc) in enumerate(ps):
                        to = slice((pr * 2 + pc) * LANES, (pr * 2 + pc + 1) * LANES)
                        acc[dt, part, to] += r[:, n * LANES:(n + 1) * LANES]

    load = pltpu.make_async_copy(wq_ref.at[:, :, :, pl.ds(q * LANES, LANES)], w.at[:, me], local.at[0])
    rows_in = pltpu.make_async_copy(h_ref, raw.at[0], local.at[1])
    small = [pltpu.make_async_copy(src, dst, local.at[2 + i])
             for i, (src, dst) in enumerate(((gain_ref, gain), (shift_ref, shift), (bias_ref, bias)))]

    @pl.when(c == 1)
    def _():
        signal(barrier, at(z + 1, 1))
        signal(barrier, at(z - 1, 1))
        signal(barrier, sibling)
        load.start()
        rows_in.start()
        for copy in small:
            copy.start()
        pl.semaphore_wait(barrier, 3)
        rows_in.wait()
        rows_out = remote(raw.at[0], raw.at[1], own.at[0, 0], own.at[1, 0], sibling)
        rows_out.start()
        load.wait()

        def piece(zz, j):
            return w.at[j, pl.ds(lax.rem(zz + 2 * nz, nz) * 2, 2)]

        def hop(way, p, d, j, step=1):
            to = z + step if way == 0 else z - step
            return remote(p, p, ringsend.at[way], ringrecv.at[way, d - 1, j], at(to, 1))

        def first(part, j):
            for way in (0, 1):
                hop(way, part, 1, j).start()

        for j in range(3):
            m = w.at[j, me]
            first(m, j)
            remote(m, m, give, giverecv.at[half], sibling).start()
        for j in range(3):
            theirs = w.at[j, z * 2]
            remote(theirs, theirs, own.at[0, 1 + j], own.at[1, 1 + j], sibling).wait_recv()
            first(theirs, j)
        blend(z)

        def take(way, d, j, s, on):
            p = piece(z - d if way == 0 else z + d, j)
            hop(way, p, d, j).wait_recv()
            for step in on:
                hop(way, p, d + step, j, step).start()
            remote(p, p, give, giverecv.at[s], sibling).start()

        @pl.loop(0, NEAR - 1)
        def _(s):
            for j in range(3):
                take(0, s + 1, j, s, (1,))
                take(1, s + 1, j, s, (1,))
            blend(z - s - 1)
            blend(z + s + 1)

        @pl.loop(0, leaps - 1)
        def _(u):
            d, s = NEAR + 2 * u, NEAR - 1 + u
            for j in range(3):
                take(0, d, j, s, (2,))
                take(1, d, j, s, (2,))
            for j in range(3):
                hop(0, piece(z - d, j), d + 1, j).start()
                hop(1, piece(z + d, j), d + 1, j).start()
            blend(z - d)
            blend(z + d)

            @pl.when(u == leaps - 2)
            def _():
                wait_bytes(acts.at[:, :, pl.ds(2, 3)], northrecv)
                remote(totals, totals, totsend.at[1], totrecv.at[1], sibling).wait_recv()

                @pl.when(z < nz - 1)
                def _():
                    wait_bytes(acts.at[:, :, 5], outerrecv)

                @pl.when(z == nz - 1)
                def _():
                    acts[:, :, 5] = acts[:, :, 4]

                for copy in small:
                    copy.wait()
                activate((0, 1))

            @pl.when(u > 0)
            def _():
                for j in range(3):
                    take(0, d - 1, j, s, ())
                    take(1, d - 1, j, s, ())
                blend(z - d + 1)
                blend(z + d - 1)

        activate((2, 3))
        arrange()
        d, s = half - 2, NEAR - 2 + leaps
        for j in range(3):
            take(0, d, j, s, (2,) if j < 2 else ())
            take(1, d, j, s, () if j < 2 else (2,))
        for j in range(3):
            hop(0, piece(z - d, j), d + 1, j).start()
            hop(1, piece(z + d, j), d + 1, j).start()
        blend(z - d)
        blend(z + d)
        for j in range(3):
            take(0, d - 1, j, s, ())
            take(1, d - 1, j, s, ())
        blend(z - d + 1)
        blend(z + d - 1)
        multiply(0, ROWS // 2, 0)
        multiply(ROWS // 2, ROWS // 2, 0)
        s = NEAR - 1 + leaps
        for j in range(3):
            take(0, half - 1, j, s, ())
            take(1, half - 1, j, s, ())
        blend(z - half + 1)
        blend(z + half - 1)
        for j in range(3):
            take(0 if j < 2 else 1, half, j, s, ())
        blend(z + half)

    @pl.when(c == 0)
    def _():
        signal(barrier, at(z + 1, 0))
        signal(barrier, at(z - 1, 0))
        signal(barrier, sibling)
        for p in others:
            signal(barrier, {"groups": group_at(p)})
        load.start()
        rows_in.start()
        for copy in small:
            copy.start()
        pl.semaphore_wait(barrier, 2 + TEAM)

        def tell(k):
            if k < len(rounds):
                signal(ask.at[k], at(z + rounds[k][0], 0))
                signal(ask.at[k], at(z - rounds[k][0], 0))

        tell(0)
        load.wait()
        for j in range(3):
            p = w.at[j, me]
            remote(p, p, own.at[0, 1 + j], own.at[1, 1 + j], sibling).start()
        early = min(2, len(rounds))
        for k in range(early):
            pl.semaphore_wait(ask.at[k], 2)
            tell(k + 1)
        rows_in.wait()
        remote(raw.at[0], raw.at[1], own.at[0, 0], own.at[1, 0], sibling).wait_recv()

        wide = raw.shape[1]
        for r in range(2):
            for t in range(tiles):
                flat[pl.ds(r * tiles + t, wide, stride=8)] = raw[r, :, t * LANES:(t + 1) * LANES].astype(F32)
        x = flat[:wide * 8].reshape(wide, 8, LANES)
        cells[...] = x.astype(BF16)

        def each(b, body):
            lo, hi = spans[b]

            @pl.loop(lo, min(hi, half - 1) + 1)
            def _(d):
                body(d)
                body(-d)

            if hi == half:
                body(half)

        def runs(b):
            if b == len(spans):
                return [(0, 1)]
            lo, hi = spans[b]
            low = min(hi, half - 1)
            return [(lo, hi - lo + 1), (nz - low, low - lo + 1)]

        def for_chip(zz):
            return cells.at[pl.ds(zz * 4, 4)]

        def send_rows(b):
            def body(d):
                zz = lax.rem(z + d + nz, nz)
                remote(for_chip(zz), acts.at[q, lax.rem(nz - d, nz), middle], a2asend, a2arecv.at[b], at(zz, 0)).start()
            each(b, body)

        def send_stats(b):
            each(b, lambda d: remote(row, stats.at[z], statsend, statrecv, at(z + d, 0)).start())

        def pass_on(b, at0, n, rows, first, last):
            for p in others:
                remote(rows(middle), acts.at[q, pl.ds(at0, n), middle], partsend, partrecv.at[b], {"groups": group_at(p)}).start()

            @pl.when(z < nz - 1)
            def _():
                remote(last, acts.at[q, pl.ds((at0 + nz - 1) % nz, n), 0], edgesend.at[0], edgerecv.at[0, b], at(z + 1, 0)).start()

            @pl.when(z > 0)
            def _():
                remote(first, acts.at[q, pl.ds((at0 + 1) % nz, n), 5], edgesend.at[1], edgerecv.at[1, b], at(z - 1, 0)).start()

            remote(rows(norths), acts.at[q, pl.ds(at0, n), norths], northsend, northrecv, sibling).start()

        def share_edges(b):
            total = sum(n for _, n in runs(b))

            @pl.when(z > 0)
            def _():
                wait_bytes(acts.at[0, pl.ds(0, total), 0], edgerecv.at[0, b])
                for at0, n in runs(b):
                    e = acts.at[q, pl.ds((at0 + nz - 1) % nz, n), 0]
                    for p in others:
                        remote(e, e, outersend.at[0], outerrecv, {"groups": group_at(p)}).start()

            @pl.when(z < nz - 1)
            def _():
                wait_bytes(acts.at[0, pl.ds(0, total), 5], edgerecv.at[1, b])
                for at0, n in runs(b):
                    e = acts.at[q, pl.ds((at0 + 1) % nz, n), 5]
                    for p in others:
                        remote(e, e, outersend.at[1], outerrecv, {"groups": group_at(p), "space": z * 2 + 1}).start()
                    remote(e, e, outersend.at[1], outerrecv, sibling).start()

        acts[q, 0, 1:5] = cells[pl.ds(z * 4, 4)]
        for b in range(early + 1):
            send_rows(b)
        own_cells = len(spans)
        for p in others:
            remote(for_chip(z), acts.at[q, 0, middle], partsend, partrecv.at[own_cells], {"groups": group_at(p)}).start()
        remote(cells.at[pl.ds(z * 4 + 1, 3)], acts.at[q, 0, norths], northsend, northrecv, sibling).start()

        count = float(2 * wide * GROUP)
        first = pack(jnp.sum(flat[:wide * 8].reshape(wide, 8, LANES), axis=0), 0)
        mean = unpack(first, 0) * (1.0 / count)
        second = pack(jnp.sum((flat[:wide * 8].reshape(wide, 8, LANES) - mean[None]) ** 2, axis=0), 1)
        row[...] = first + second
        stats[z] = row[...]
        for b in range(early + 1):
            send_stats(b)

        for k in range(early, len(rounds)):
            pl.semaphore_wait(ask.at[k], 2)
            tell(k + 1)
            send_rows(k + 1)
            send_stats(k + 1)

        def from_team(b):
            total = sum(n for _, n in runs(b))
            wait_bytes(acts.at[pl.ds(0, TEAM - 1), pl.ds(0, total), middle], partrecv.at[b])
            for at0, n in runs(b):
                for p in others:
                    c3 = acts.at[p, pl.ds(at0, n), norths]
                    remote(c3, c3, northsend, northrecv, sibling).start()

        from_team(own_cells)

        @pl.when(z < nz - 1)
        def _():
            remote(cells.at[z * 4 + 3], acts.at[q, nz - 1, 0], edgesend.at[0], edgerecv.at[0, own_cells], at(z + 1, 0)).start()

        @pl.when(z > 0)
        def _():
            remote(cells.at[z * 4], acts.at[q, 1, 5], edgesend.at[1], edgerecv.at[1, own_cells], at(z - 1, 0)).start()

        share_edges(own_cells)
        for b in range(len(spans)):
            if b == len(spans) - 1:
                wait_bytes(stats.at[pl.ds(0, nz - 1)], statrecv)
                every = stats[...].reshape(nz, LANES)
                lane = lax.broadcasted_iota(jnp.int32, (nz, LANES), 1)
                mean = jnp.sum(every, axis=0, keepdims=True) * (1.0 / (count * nz))
                off = jnp.where(lane < 32, (every * (1.0 / count) - mean) ** 2 * count, 0.0)
                spread = jnp.where(lane < 32, 0.0, every)
                spread = jnp.sum(spread + pltpu.roll(off, 32, 1), axis=0, keepdims=True) * (1.0 / (count * nz))
                tot[...] = jnp.where(lane[:1] < 32, mean, spread)
                totals[q] = tot[...]
                for p in others:
                    remote(tot, totals.at[q], totsend.at[0], totrecv.at[0], {"groups": group_at(p)}).start()
            wait_bytes(acts.at[0, pl.ds(0, sizes[b]), middle], a2arecv.at[b])

            for at0, n in runs(b):
                pass_on(b, at0, n, lambda cols, at0=at0, n=n: acts.at[q, pl.ds(at0, n), cols],
                        acts.at[q, pl.ds(at0, n), 1], acts.at[q, pl.ds(at0, n), 4])
            if b > 0:
                share_edges(b - 1)

        wait_bytes(totals.at[pl.ds(0, TEAM - 1)], totrecv.at[0])
        remote(totals, totals, totsend.at[1], totrecv.at[1], sibling).start()
        for b in range(len(spans) - 1):
            from_team(b)
        share_edges(len(spans) - 1)
        from_team(len(spans) - 1)

        @pl.when(z > 0)
        def _():
            wait_bytes(acts.at[pl.ds(0, TEAM - 1), :, 0], outerrecv)

        @pl.when(z == 0)
        def _():
            acts[:, :, 0] = acts[:, :, 1]

        for copy in small:
            copy.wait()
        activate(range(TEAM))
        arrange()
        wait_bytes(w.at[:, 0], giverecv.at[half])
        blend(z)

        @pl.loop(0, NEAR - 1)
        def _(s):
            wait_bytes(w.at[:, pl.ds(0, 4)], giverecv.at[s])
            blend(z - s - 1)
            blend(z + s + 1)

        wait_bytes(w.at[:, pl.ds(0, 4)], giverecv.at[NEAR - 1])
        blend(z - NEAR)
        blend(z + NEAR)

        @pl.loop(1, leaps)
        def _(u):
            wait_bytes(w.at[:, pl.ds(0, 8)], giverecv.at[NEAR - 1 + u])
            for d in (0, -1):
                blend(z - NEAR - 2 * u - d)
                blend(z + NEAR + 2 * u + d)

            @pl.when(u >= leaps - 2)
            def _():
                @pl.when(u == leaps - 2)
                def _():
                    multiply(0, ROWS // 2, 0)

                @pl.when(u == leaps - 1)
                def _():
                    multiply(ROWS // 2, ROWS // 2, 0)

        wait_bytes(w.at[:, pl.ds(0, 6)], giverecv.at[NEAR - 1 + leaps])
        blend(z - half + 1)
        blend(z + half - 1)
        blend(z + half)

    frame = lax.broadcasted_iota(jnp.int32, (8, LANES), 0) % FRAMES
    which = lax.broadcasted_iota(jnp.int32, (tiles, LANES), 0)
    bias_row = jnp.sum(jnp.where(which == q, bias[...].astype(F32), 0.0), axis=0, keepdims=True)
    row0 = 0
    for few in PARTS:
        multiply(row0, few, 1)
        for r in range(few):
            for cc in range(2):
                for n in range(4):
                    i = ((r * 2 + n // 2) * 2 + cc) * 2 + n % 2
                    for half_tile in range(2):
                        at_row = ((row0 + r) * 2 + cc) * 16 + half_tile * 8
                        old, mid, new = (acc[dt, at_row:at_row + 8, n * LANES:(n + 1) * LANES] for dt in range(3))
                        mid = jnp.where(frame >= 1, pltpu.roll(mid, 1, 0), mid)
                        old = jnp.where(frame >= 2, pltpu.roll(old, 2, 0), jnp.where(frame >= 1, pltpu.roll(old, 1, 0), old))
                        turn[i * TROWS + half_tile * 8:i * TROWS + half_tile * 8 + 8] = old + mid + new + bias_row
        put = slice(row0 * 2, (row0 + few) * 2)
        row0 += few
        for p in range(TEAM):
            for f in range(FRAMES):
                v = turn[pl.ds(p * FRAMES + f, few * 8, stride=TROWS)].astype(BF16)
                mine[p, f, put] = v.reshape(few * 2, 4, LANES)
        here = pl.ds(pl.multiple_of(q * LANES, LANES), LANES)
        out[:, put, :, here] = mine[q, :, put]
        for p in others:
            remote(mine.at[p, :, put], out.at[:, put, :, here], outsend, outrecv, {"groups": group_at(p)}).start()
    @pl.when(c == 1)
    def _():
        wait_bytes(raw.at[0], own.at[0, 0])
        for way, rest in ((0, pl.ds(0, 2)), (1, pl.ds(0, 1))):
            wait_bytes(w.at[:, pl.ds(0, 2 * half - 2)], ringsend.at[way])
            wait_bytes(w.at[rest, pl.ds(0, 2)], ringsend.at[way])
        wait_bytes(w.at[:, pl.ds(0, nd - 1)], give)

    @pl.when(c == 0)
    def _():
        for j in range(3):
            wait_bytes(w.at[j, me], own.at[0, 1 + j])
        wait_bytes(stats.at[pl.ds(0, nz - 1)], statsend)
        wait_bytes(acts.at[0, pl.ds(0, nz - 1), middle], a2asend)
        wait_bytes(acts.at[pl.ds(0, TEAM - 1), :, middle], partsend)
        wait_bytes(acts.at[:, :, norths], northsend)

        @pl.when(z < nz - 1)
        def _():
            wait_bytes(acts.at[0, :, 0], edgesend.at[0])
            wait_bytes(acts.at[:, :, 5], outersend.at[1])

        @pl.when(z > 0)
        def _():
            wait_bytes(acts.at[0, :, 5], edgesend.at[1])
            wait_bytes(acts.at[pl.ds(0, TEAM - 1), :, 0], outersend.at[0])
        wait_bytes(totals.at[pl.ds(0, TEAM - 1)], totsend.at[0])
        wait_bytes(totals, totsend.at[1])

    wait_bytes(mine.at[pl.ds(0, TEAM - 1)], outrecv)
    wait_bytes(mine.at[pl.ds(0, TEAM - 1)], outsend)


VMEM = pl.BlockSpec(memory_space=pltpu.VMEM)
HBM = pl.BlockSpec(memory_space=pltpu.HBM)


def shards(ny, hidden, norm_gain, norm_shift, conv_weight, conv_bias):
    nd = lax.axis_size("space")
    nz = nd // 2
    wide, channels = hidden.shape
    tiles = channels // LANES
    cin = conv_weight.shape[3]
    batches = len(rounds_of(nz // 2)) + 1
    wq = conv_weight.reshape(3, TAPS, cin, conv_weight.shape[4])
    scratch = [pltpu.VMEM((tiles, 1, LANES), F32)] * 2 + [
        pltpu.VMEM((tiles, LANES), BF16),
        pltpu.VMEM((3, nd, TAPS, cin, LANES), BF16),
        pltpu.VMEM((3, channels, 16 * LANES), BF16),
        pltpu.VMEM((TEAM, nz, 6, 8, LANES), BF16),
        pltpu.VMEM((TEAM, 1, LANES), F32),
        pltpu.VMEM((2, wide, channels), BF16),
        pltpu.VMEM((wide, 8, LANES), BF16),
        pltpu.VMEM((wide * 8 + 8, LANES), F32),
        pltpu.VMEM((nz, 1, LANES), F32),
        pltpu.VMEM((1, LANES), F32),
        pltpu.VMEM((1, LANES), F32),
        pltpu.VMEM((ROWS // 2 * 16 * YROWS + YROWS, LANES), F32),
        pltpu.VMEM((ROWS + 2, 4, 16, channels), BF16),
        pltpu.VMEM((3, ROWS * 32, 4 * LANES), F32),
        pltpu.VMEM((max(PARTS) * 8 * TROWS + TROWS, LANES), F32),
        pltpu.VMEM((TEAM, FRAMES, ROWS * 2, 4, LANES), BF16),
        DMA((5,)), DMA((2,)), DMA((2, nz // 2, 3)), DMA, DMA((nz // 2 + 1,)), DMA((2, 4)),
        pltpu.SemaphoreType.REGULAR((max(1, batches - 1),)),
        DMA, DMA((batches,)), DMA, DMA, DMA, DMA((batches + 1,)), DMA, DMA, DMA((2,)), DMA((2, batches + 1)), DMA((2,)), DMA, DMA((2,)), DMA((2,)), DMA, DMA,
    ]
    operands = (hidden, wq, norm_gain.reshape(tiles, 1, LANES), norm_shift.reshape(tiles, 1, LANES), conv_bias.reshape(tiles, LANES))
    return pl.pallas_call(
        functools.partial(kernel, ny, nd),
        out_shape=pltpu.VMEM((FRAMES, ROWS * 2, 4, channels), BF16),
        in_specs=[HBM] * 5,
        out_specs=VMEM,
        scratch_shapes=scratch,
        compiler_params=pltpu.CompilerParams(collective_id=0, has_side_effects=True, vmem_limit_bytes=40 * MIB),
        name="decode",
    )(*(pltpu.with_memory_space_constraint(v, pltpu.HBM) for v in operands))


def solution(mesh):
    ny = len({d.coords[1] for d in mesh.devices.flat})
    return jax.shard_map(
        functools.partial(shards, ny),
        mesh=mesh,
        in_specs=(P(("groups", "space"), None), P(), P(), P(None, None, None, "space", None), P()),
        out_specs=P("groups", None, "space", None),
        check_vma=False,
    )
```

```python
import functools

import jax
import jax.numpy as jnp
from jax import lax
from jax.experimental import pallas as pl
from jax.experimental.pallas import tpu as pltpu
from jax.sharding import PartitionSpec as P

GROUP = 16
FRAMES = 4
ROWS = 16
LANES = 128
TEAM = 4
TAPS = 9
EPSILON = 1e-6
PARTS = (4, 4, 4, 4)
MIB = 1 << 20
YROWS = 40
TROWS = 24
NEAR = 6

DMA = pltpu.SemaphoreType.DMA
F32, BF16 = jnp.float32, jnp.bfloat16
SHIFTS = [(0, 0), (0, -1), (0, 1), (-1, 0), (1, 0), (-1, -1), (-1, 1), (1, -1), (1, 1)]


def phases_of(dr, dc):
    rows = {-1: (0,), 0: (0, 1), 1: (1,)}
    return [(a, b) for a in rows[dr] for b in rows[dc]]


COLUMNS = [(s, p) for s in SHIFTS for p in phases_of(*s)]


def remote(src, dst, send, recv, device):
    return pltpu.make_async_remote_copy(
        src_ref=src, dst_ref=dst, send_sem=send, recv_sem=recv,
        device_id=device, device_id_type=pl.DeviceIdType.MESH,
    )


def signal(sem, device):
    pl.semaphore_signal(sem, inc=1, device_id=device, device_id_type=pl.DeviceIdType.MESH)


def wait_bytes(ref, sem):
    pltpu.make_async_copy(ref, ref, sem).wait()


def team(ny):
    g = lax.axis_index("groups")
    x, y = g // ny, g % ny
    x0, y0 = x - x % 2, y - y % 2
    q = (x % 2) * 2 + y % 2
    others = (3 - q, (q + 2) % TEAM, q + 1 - 2 * (q % 2))
    return q, others, lambda p: (x0 + p // 2) * ny + y0 + p % 2


def group_matrix():
    lane = lax.broadcasted_iota(jnp.int32, (LANES, LANES), 0)
    packed = lax.broadcasted_iota(jnp.int32, (LANES, LANES), 1)
    return jnp.where(lane // GROUP == packed % 8, 1.0, 0.0).astype(F32)


def packed_mask(which):
    row = lax.broadcasted_iota(jnp.int32, (8, LANES), 0)
    lane = lax.broadcasted_iota(jnp.int32, (8, LANES), 1)
    return (lane // 32 == which) & ((lane // 8) % 4 == row % 4)


def hdot(a, b):
    return jnp.dot(a, b, preferred_element_type=F32, precision=lax.Precision.HIGHEST)


def pack(sums, which):
    return jnp.sum(jnp.where(packed_mask(which), hdot(sums, group_matrix()), 0.0), axis=0, keepdims=True)


def unpack(row, which):
    spread = jnp.where(packed_mask(which), jnp.broadcast_to(row, (8, LANES)), 0.0)
    return hdot(spread, group_matrix().T)


def rounds_of(half):
    known, steps = 1, []
    while known < half:
        step = min(known, max(1, half // 4))
        known += step
        steps.append((step, min(known, half)))
    return steps


def kernel(ny, nd, h_ref, wq_ref, gain_ref, shift_ref, bias_ref, out, gain, shift, bias,
           w, mix, acts, totals, raw, cells, flat, stats, row, tot, ys, a, acc, turn, mine,
           local, southsend, ringsend, ringrecv, give, giverecv, own, ask, a2asend, a2arecv,
           statsend, statrecv, partsend, partrecv, northsend, northrecv, edgesend, edgerecv, outersend, outerrecv, totsend, totrecv, outsend, outrecv):
    me = lax.axis_index("space")
    z, c = me // 2, me % 2
    nz = nd // 2
    half = nz // 2
    q, others, group_at = team(ny)
    leaps = (half - NEAR) // 2
    assert NEAR + 2 * leaps == half
    rounds = rounds_of(half)
    spans, last = [], 0
    for known in [1] + [r[1] for r in rounds]:
        spans.append((last + 1, known))
        last = known
    sizes = [2 * (hi - lo + 1) - (1 if hi == half else 0) for lo, hi in spans]

    def at(zz, core):
        return {"space": lax.rem(zz + 2 * nz, nz) * 2 + core}

    sibling = {"space": z * 2 + 1 - c}
    middle = pl.ds(1, 4)
    norths = pl.ds(2, 3)
    barrier = pltpu.get_barrier_semaphore()

    def blend(zz):
        zz = lax.rem(zz + 2 * nz, nz)
        for dt in range(3):
            tap = [w[dt, pl.ds(zz * 2, 2), n].astype(F32).reshape(16, LANES) for n in range(TAPS)]

            def sums(x):
                return {(0, -1): x[0], (0, 0): x[1] + x[2], (1, 0): x[0] + x[1], (1, 1): x[2]}

            by_row = [sums([tap[n * 3 + e] for n in range(3)]) for e in range(3)]
            both = {k: sums([by_row[e][k] for e in range(3)]) for k in by_row[0]}
            for n, ((dr, dc), (pr, pc)) in enumerate(COLUMNS):
                mix[dt, pl.ds(pl.multiple_of(zz * 16, 16), 16), n * LANES:(n + 1) * LANES] = both[(pr, dr)][(pc, dc)].astype(BF16)

    channels = a.shape[-1]
    tiles = channels // LANES
    pairs = ROWS // 2

    def activate(places):
        g = jnp.concatenate([gain[t] for t in range(tiles)] * 2, axis=0)
        b = jnp.concatenate([shift[t] for t in range(tiles)] * 2, axis=0)
        for p in places:
            mean = unpack(totals[p], 0)
            scale = g * lax.rsqrt(unpack(totals[p], 1) + EPSILON)
            scale, move = scale * 0.5, b * 0.5

            @pl.loop(0, pairs, unroll=4)
            def _(rp):
                for f in range(FRAMES):
                    v = acts[p, lax.rem(f * pairs + rp + nz - z, nz), pl.ds(2 * c, 4)].astype(F32)
                    v = (v - mean[None]) * scale[None] + move[None]
                    v = v * jnp.tanh(v) + v
                    start = rp * (16 * YROWS) + (p * FRAMES + f) * YROWS
                    ys[pl.ds(pl.multiple_of(start, 8), 32)] = v.reshape(32, LANES)

    def arrange():
        @pl.loop(0, pairs)
        def _(rp):
            for col in range(4):
                for r in range(2):
                    for t in range(tiles):
                        v = ys[pl.ds(rp * (16 * YROWS) + col * 8 + r * tiles + t, 16, stride=YROWS)].astype(BF16)
                        a[rp * 2 + r + 1, col, :, t * LANES:(t + 1) * LANES] = v

        a[0] = a[1]
        a[ROWS + 1] = a[ROWS]

    chips = LANES // 16
    first_block = z // chips + jnp.where(z % chips < chips // 2, tiles - 1, 0)
    assert half - 4 >= chips * 3 // 2 - 1 and tiles == 4

    def multiply(row0, few, late):
        part = slice(row0 * 32, (row0 + few) * 32)
        blocks = [pl.ds(pl.multiple_of(lax.rem(first_block + 2 * late + i, tiles) * LANES, LANES), LANES) for i in range(2)]
        for dt in range(3):
            col0 = 0
            for dr, dc in SHIFTS:
                ps = phases_of(dr, dc)
                rows, cols = slice(1 + dr + row0, 1 + dr + row0 + few), slice(1 + dc, 3 + dc)
                lhs = jnp.concatenate([a[rows, cols, :, k].reshape(few * 2 * 16, LANES) for k in blocks], axis=1)
                rhs = jnp.concatenate([mix[dt, k, col0:col0 + len(ps) * LANES] for k in blocks], axis=0)
                r = jnp.dot(lhs, rhs, preferred_element_type=F32)
                col0 += len(ps) * LANES
                if (dr, dc) == (0, 0):
                    acc[dt, part] = acc[dt, part] + r if late else r
                else:
                    for n, (pr, pc) in enumerate(ps):
                        to = slice((pr * 2 + pc) * LANES, (pr * 2 + pc + 1) * LANES)
                        acc[dt, part, to] += r[:, n * LANES:(n + 1) * LANES]

    load = pltpu.make_async_copy(wq_ref.at[:, :, :, pl.ds(q * LANES, LANES)], w.at[:, me], local.at[0])
    rows_in = pltpu.make_async_copy(h_ref, raw.at[0], local.at[1])
    small = [pltpu.make_async_copy(src, dst, local.at[2 + i])
             for i, (src, dst) in enumerate(((gain_ref, gain), (shift_ref, shift), (bias_ref, bias)))]

    @pl.when(c == 1)
    def _():
        for d in (1, -1):
            for core in (1, 0):
                signal(barrier, at(z + d, core))
        signal(barrier, sibling)
        load.start()
        rows_in.start()
        for copy in small:
            copy.start()
        pl.semaphore_wait(barrier, 5)
        rows_in.wait()
        rows_out = remote(raw.at[0], raw.at[1], own.at[0, 0], own.at[1, 0], sibling)
        rows_out.start()
        load.wait()

        def piece(zz, j):
            return w.at[j, pl.ds(lax.rem(zz + 2 * nz, nz) * 2, 2)]

        def hop(way, p, d, j, step=1):
            to = z + step if way == 0 else z - step
            return remote(p, p, ringsend.at[way], ringrecv.at[way, d - 1, j], at(to, 1))

        def first(part, j):
            for way in (0, 1):
                hop(way, part, 1, j).start()

        for j in range(3):
            m = w.at[j, me]
            first(m, j)
            remote(m, m, give, giverecv.at[half], sibling).start()
        for j in range(3):
            theirs = w.at[j, z * 2]
            remote(theirs, theirs, own.at[0, 1 + j], own.at[1, 1 + j], sibling).wait_recv()
        blend(z)

        def take(way, d, j, s, on):
            p = piece(z - d if way == 0 else z + d, j)
            hop(way, p, d, j).wait_recv()
            for step in on:
                hop(way, p, d + step, j, step).start()
            remote(p, p, give, giverecv.at[s], sibling).start()

        @pl.loop(0, NEAR - 1)
        def _(s):
            for j in range(3):
                take(0, s + 1, j, s, (1,))
                take(1, s + 1, j, s, (1,))
            blend(z - s - 1)
            blend(z + s + 1)

        @pl.loop(0, leaps - 1)
        def _(u):
            d, s = NEAR + 2 * u, NEAR - 1 + u
            for j in range(3):
                take(0, d, j, s, (2,))
                take(1, d, j, s, (2,))
            for j in range(3):
                hop(0, piece(z - d, j), d + 1, j).start()
                hop(1, piece(z + d, j), d + 1, j).start()
            blend(z - d)
            blend(z + d)

            @pl.when(u == leaps - 2)
            def _():
                wait_bytes(acts.at[:, :, pl.ds(2, 3)], northrecv)
                remote(totals, totals, totsend.at[1], totrecv.at[1], sibling).wait_recv()

                @pl.when(z < nz - 1)
                def _():
                    wait_bytes(acts.at[:, :, 5], outerrecv)

                @pl.when(z == nz - 1)
                def _():
                    acts[:, :, 5] = acts[:, :, 4]

                for copy in small:
                    copy.wait()
                activate((0, 1))

            @pl.when(u > 0)
            def _():
                for j in range(3):
                    take(0, d - 1, j, s, ())
                    take(1, d - 1, j, s, ())
                blend(z - d + 1)
                blend(z + d - 1)

        activate((2, 3))
        arrange()
        d, s = half - 2, NEAR - 2 + leaps
        for j in range(3):
            take(0, d, j, s, (2,) if j < 2 else ())
            take(1, d, j, s, () if j < 2 else (2,))
        for j in range(3):
            hop(0, piece(z - d, j), d + 1, j).start()
            hop(1, piece(z + d, j), d + 1, j).start()
        blend(z - d)
        blend(z + d)
        for j in range(3):
            take(0, d - 1, j, s, ())
            take(1, d - 1, j, s, ())
        blend(z - d + 1)
        blend(z + d - 1)
        multiply(0, ROWS // 2, 0)
        multiply(ROWS // 2, ROWS // 2, 0)
        s = NEAR - 1 + leaps
        for j in range(3):
            take(0, half - 1, j, s, ())
            take(1, half - 1, j, s, ())
        blend(z - half + 1)
        blend(z + half - 1)
        for j in range(3):
            take(0 if j < 2 else 1, half, j, s, ())
        blend(z + half)

    @pl.when(c == 0)
    def _():
        for d in (1, -1):
            for core in (1, 0):
                signal(barrier, at(z + d, core))
        signal(barrier, sibling)
        for p in others:
            signal(barrier, {"groups": group_at(p)})
        load.start()
        rows_in.start()
        for copy in small:
            copy.start()
        pl.semaphore_wait(barrier, 4 + TEAM)

        def tell(k):
            if k < len(rounds):
                signal(ask.at[k], at(z + rounds[k][0], 0))
                signal(ask.at[k], at(z - rounds[k][0], 0))

        tell(0)
        load.wait()
        for j in range(3):
            p = w.at[j, me]
            remote(p, p, southsend, ringrecv.at[0, 0, j], at(z + 1, 1)).start()
            remote(p, p, southsend, ringrecv.at[1, 0, j], at(z - 1, 1)).start()
        for j in range(3):
            p = w.at[j, me]
            remote(p, p, own.at[0, 1 + j], own.at[1, 1 + j], sibling).start()
        early = min(2, len(rounds))
        for k in range(early):
            pl.semaphore_wait(ask.at[k], 2)
            tell(k + 1)
        rows_in.wait()
        remote(raw.at[0], raw.at[1], own.at[0, 0], own.at[1, 0], sibling).wait_recv()

        wide = raw.shape[1]
        for r in range(2):
            for t in range(tiles):
                flat[pl.ds(r * tiles + t, wide, stride=8)] = raw[r, :, t * LANES:(t + 1) * LANES].astype(F32)
        x = flat[:wide * 8].reshape(wide, 8, LANES)
        cells[...] = x.astype(BF16)

        def each(b, body):
            lo, hi = spans[b]

            @pl.loop(lo, min(hi, half - 1) + 1)
            def _(d):
                body(d)
                body(-d)

            if hi == half:
                body(half)

        def runs(b):
            if b == len(spans):
                return [(0, 1)]
            lo, hi = spans[b]
            low = min(hi, half - 1)
            return [(lo, hi - lo + 1), (nz - low, low - lo + 1)]

        def for_chip(zz):
            return cells.at[pl.ds(zz * 4, 4)]

        def send_rows(b):
            def body(d):
                zz = lax.rem(z + d + nz, nz)
                remote(for_chip(zz), acts.at[q, lax.rem(nz - d, nz), middle], a2asend, a2arecv.at[b], at(zz, 0)).start()
            each(b, body)

        def send_stats(b):
            each(b, lambda d: remote(row, stats.at[z], statsend, statrecv, at(z + d, 0)).start())

        def pass_on(b, at0, n, rows, first, last):
            for p in others:
                remote(rows(middle), acts.at[q, pl.ds(at0, n), middle], partsend, partrecv.at[b], {"groups": group_at(p)}).start()

            @pl.when(z < nz - 1)
            def _():
                remote(last, acts.at[q, pl.ds((at0 + nz - 1) % nz, n), 0], edgesend.at[0], edgerecv.at[0, b], at(z + 1, 0)).start()

            @pl.when(z > 0)
            def _():
                remote(first, acts.at[q, pl.ds((at0 + 1) % nz, n), 5], edgesend.at[1], edgerecv.at[1, b], at(z - 1, 0)).start()

            remote(rows(norths), acts.at[q, pl.ds(at0, n), norths], northsend, northrecv, sibling).start()

        def share_edges(b):
            total = sum(n for _, n in runs(b))

            @pl.when(z > 0)
            def _():
                wait_bytes(acts.at[0, pl.ds(0, total), 0], edgerecv.at[0, b])
                for at0, n in runs(b):
                    e = acts.at[q, pl.ds((at0 + nz - 1) % nz, n), 0]
                    for p in others:
                        remote(e, e, outersend.at[0], outerrecv, {"groups": group_at(p)}).start()

            @pl.when(z < nz - 1)
            def _():
                wait_bytes(acts.at[0, pl.ds(0, total), 5], edgerecv.at[1, b])
                for at0, n in runs(b):
                    e = acts.at[q, pl.ds((at0 + 1) % nz, n), 5]
                    for p in others:
                        remote(e, e, outersend.at[1], outerrecv, {"groups": group_at(p), "space": z * 2 + 1}).start()
                    remote(e, e, outersend.at[1], outerrecv, sibling).start()

        acts[q, 0, 1:5] = cells[pl.ds(z * 4, 4)]
        for b in range(early + 1):
            send_rows(b)
        own_cells = len(spans)
        for p in others:
            remote(for_chip(z), acts.at[q, 0, middle], partsend, partrecv.at[own_cells], {"groups": group_at(p)}).start()
        remote(cells.at[pl.ds(z * 4 + 1, 3)], acts.at[q, 0, norths], northsend, northrecv, sibling).start()

        count = float(2 * wide * GROUP)
        first = pack(jnp.sum(flat[:wide * 8].reshape(wide, 8, LANES), axis=0), 0)
        mean = unpack(first, 0) * (1.0 / count)
        second = pack(jnp.sum((flat[:wide * 8].reshape(wide, 8, LANES) - mean[None]) ** 2, axis=0), 1)
        row[...] = first + second
        stats[z] = row[...]
        for b in range(early + 1):
            send_stats(b)

        for k in range(early, len(rounds)):
            pl.semaphore_wait(ask.at[k], 2)
            tell(k + 1)
            send_rows(k + 1)
            send_stats(k + 1)

        def from_team(b):
            total = sum(n for _, n in runs(b))
            wait_bytes(acts.at[pl.ds(0, TEAM - 1), pl.ds(0, total), middle], partrecv.at[b])
            for at0, n in runs(b):
                for p in others:
                    c3 = acts.at[p, pl.ds(at0, n), norths]
                    remote(c3, c3, northsend, northrecv, sibling).start()

        from_team(own_cells)

        @pl.when(z < nz - 1)
        def _():
            remote(cells.at[z * 4 + 3], acts.at[q, nz - 1, 0], edgesend.at[0], edgerecv.at[0, own_cells], at(z + 1, 0)).start()

        @pl.when(z > 0)
        def _():
            remote(cells.at[z * 4], acts.at[q, 1, 5], edgesend.at[1], edgerecv.at[1, own_cells], at(z - 1, 0)).start()

        share_edges(own_cells)
        for b in range(len(spans)):
            if b == len(spans) - 1:
                wait_bytes(stats.at[pl.ds(0, nz - 1)], statrecv)
                every = stats[...].reshape(nz, LANES)
                lane = lax.broadcasted_iota(jnp.int32, (nz, LANES), 1)
                mean = jnp.sum(every, axis=0, keepdims=True) * (1.0 / (count * nz))
                off = jnp.where(lane < 32, (every * (1.0 / count) - mean) ** 2 * count, 0.0)
                spread = jnp.where(lane < 32, 0.0, every)
                spread = jnp.sum(spread + pltpu.roll(off, 32, 1), axis=0, keepdims=True) * (1.0 / (count * nz))
                tot[...] = jnp.where(lane[:1] < 32, mean, spread)
                totals[q] = tot[...]
                for p in others:
                    remote(tot, totals.at[q], totsend.at[0], totrecv.at[0], {"groups": group_at(p)}).start()
            wait_bytes(acts.at[0, pl.ds(0, sizes[b]), middle], a2arecv.at[b])

            for at0, n in runs(b):
                pass_on(b, at0, n, lambda cols, at0=at0, n=n: acts.at[q, pl.ds(at0, n), cols],
                        acts.at[q, pl.ds(at0, n), 1], acts.at[q, pl.ds(at0, n), 4])
            if b > 0:
                share_edges(b - 1)

        wait_bytes(totals.at[pl.ds(0, TEAM - 1)], totrecv.at[0])
        remote(totals, totals, totsend.at[1], totrecv.at[1], sibling).start()
        for b in range(len(spans) - 1):
            from_team(b)
        share_edges(len(spans) - 1)
        from_team(len(spans) - 1)

        @pl.when(z > 0)
        def _():
            wait_bytes(acts.at[pl.ds(0, TEAM - 1), :, 0], outerrecv)

        @pl.when(z == 0)
        def _():
            acts[:, :, 0] = acts[:, :, 1]

        for copy in small:
            copy.wait()
        activate(range(TEAM))
        arrange()
        wait_bytes(w.at[:, 0], giverecv.at[half])
        blend(z)

        @pl.loop(0, NEAR - 1)
        def _(s):
            wait_bytes(w.at[:, pl.ds(0, 4)], giverecv.at[s])
            blend(z - s - 1)
            blend(z + s + 1)

        wait_bytes(w.at[:, pl.ds(0, 4)], giverecv.at[NEAR - 1])
        blend(z - NEAR)
        blend(z + NEAR)

        @pl.loop(1, leaps)
        def _(u):
            wait_bytes(w.at[:, pl.ds(0, 8)], giverecv.at[NEAR - 1 + u])
            for d in (0, -1):
                blend(z - NEAR - 2 * u - d)
                blend(z + NEAR + 2 * u + d)

            @pl.when(u >= leaps - 2)
            def _():
                @pl.when(u == leaps - 2)
                def _():
                    multiply(0, ROWS // 2, 0)

                @pl.when(u == leaps - 1)
                def _():
                    multiply(ROWS // 2, ROWS // 2, 0)

        wait_bytes(w.at[:, pl.ds(0, 6)], giverecv.at[NEAR - 1 + leaps])
        blend(z - half + 1)
        blend(z + half - 1)
        blend(z + half)

    frame = lax.broadcasted_iota(jnp.int32, (8, LANES), 0) % FRAMES
    which = lax.broadcasted_iota(jnp.int32, (tiles, LANES), 0)
    bias_row = jnp.sum(jnp.where(which == q, bias[...].astype(F32), 0.0), axis=0, keepdims=True)
    row0 = 0
    for few in PARTS:
        multiply(row0, few, 1)
        for r in range(few):
            for cc in range(2):
                for n in range(4):
                    i = ((r * 2 + n // 2) * 2 + cc) * 2 + n % 2
                    for half_tile in range(2):
                        at_row = ((row0 + r) * 2 + cc) * 16 + half_tile * 8
                        old, mid, new = (acc[dt, at_row:at_row + 8, n * LANES:(n + 1) * LANES] for dt in range(3))
                        mid = jnp.where(frame >= 1, pltpu.roll(mid, 1, 0), mid)
                        old = jnp.where(frame >= 2, pltpu.roll(old, 2, 0), jnp.where(frame >= 1, pltpu.roll(old, 1, 0), old))
                        turn[i * TROWS + half_tile * 8:i * TROWS + half_tile * 8 + 8] = old + mid + new + bias_row
        put = slice(row0 * 2, (row0 + few) * 2)
        row0 += few
        for p in range(TEAM):
            for f in range(FRAMES):
                v = turn[pl.ds(p * FRAMES + f, few * 8, stride=TROWS)].astype(BF16)
                mine[p, f, put] = v.reshape(few * 2, 4, LANES)
        here = pl.ds(pl.multiple_of(q * LANES, LANES), LANES)
        out[:, put, :, here] = mine[q, :, put]
        for p in others:
            remote(mine.at[p, :, put], out.at[:, put, :, here], outsend, outrecv, {"groups": group_at(p)}).start()
    @pl.when(c == 1)
    def _():
        wait_bytes(raw.at[0], own.at[0, 0])
        wait_bytes(w.at[:, pl.ds(0, 2 * half - 2)], ringsend.at[0])
        wait_bytes(w.at[0, pl.ds(0, 1)], ringsend.at[0])
        wait_bytes(w.at[:, pl.ds(0, 2 * half - 3)], ringsend.at[1])
        wait_bytes(w.at[0, pl.ds(0, 2)], ringsend.at[1])
        wait_bytes(w.at[:, pl.ds(0, nd - 1)], give)

    @pl.when(c == 0)
    def _():
        for j in range(3):
            wait_bytes(w.at[j, me], own.at[0, 1 + j])
        wait_bytes(w.at[:, pl.ds(0, 2)], southsend)
        wait_bytes(stats.at[pl.ds(0, nz - 1)], statsend)
        wait_bytes(acts.at[0, pl.ds(0, nz - 1), middle], a2asend)
        wait_bytes(acts.at[pl.ds(0, TEAM - 1), :, middle], partsend)
        wait_bytes(acts.at[:, :, norths], northsend)

        @pl.when(z < nz - 1)
        def _():
            wait_bytes(acts.at[0, :, 0], edgesend.at[0])
            wait_bytes(acts.at[:, :, 5], outersend.at[1])

        @pl.when(z > 0)
        def _():
            wait_bytes(acts.at[0, :, 5], edgesend.at[1])
            wait_bytes(acts.at[pl.ds(0, TEAM - 1), :, 0], outersend.at[0])
        wait_bytes(totals.at[pl.ds(0, TEAM - 1)], totsend.at[0])
        wait_bytes(totals, totsend.at[1])

    wait_bytes(mine.at[pl.ds(0, TEAM - 1)], outrecv)
    wait_bytes(mine.at[pl.ds(0, TEAM - 1)], outsend)


VMEM = pl.BlockSpec(memory_space=pltpu.VMEM)
HBM = pl.BlockSpec(memory_space=pltpu.HBM)


def shards(ny, hidden, norm_gain, norm_shift, conv_weight, conv_bias):
    nd = lax.axis_size("space")
    nz = nd // 2
    wide, channels = hidden.shape
    tiles = channels // LANES
    cin = conv_weight.shape[3]
    batches = len(rounds_of(nz // 2)) + 1
    wq = conv_weight.reshape(3, TAPS, cin, conv_weight.shape[4])
    scratch = [pltpu.VMEM((tiles, 1, LANES), F32)] * 2 + [
        pltpu.VMEM((tiles, LANES), BF16),
        pltpu.VMEM((3, nd, TAPS, cin, LANES), BF16),
        pltpu.VMEM((3, channels, 16 * LANES), BF16),
        pltpu.VMEM((TEAM, nz, 6, 8, LANES), BF16),
        pltpu.VMEM((TEAM, 1, LANES), F32),
        pltpu.VMEM((2, wide, channels), BF16),
        pltpu.VMEM((wide, 8, LANES), BF16),
        pltpu.VMEM((wide * 8 + 8, LANES), F32),
        pltpu.VMEM((nz, 1, LANES), F32),
        pltpu.VMEM((1, LANES), F32),
        pltpu.VMEM((1, LANES), F32),
        pltpu.VMEM((ROWS // 2 * 16 * YROWS + YROWS, LANES), F32),
        pltpu.VMEM((ROWS + 2, 4, 16, channels), BF16),
        pltpu.VMEM((3, ROWS * 32, 4 * LANES), F32),
        pltpu.VMEM((max(PARTS) * 8 * TROWS + TROWS, LANES), F32),
        pltpu.VMEM((TEAM, FRAMES, ROWS * 2, 4, LANES), BF16),
        DMA((5,)), DMA, DMA((2,)), DMA((2, nz // 2, 3)), DMA, DMA((nz // 2 + 1,)), DMA((2, 4)),
        pltpu.SemaphoreType.REGULAR((max(1, batches - 1),)),
        DMA, DMA((batches,)), DMA, DMA, DMA, DMA((batches + 1,)), DMA, DMA, DMA((2,)), DMA((2, batches + 1)), DMA((2,)), DMA, DMA((2,)), DMA((2,)), DMA, DMA,
    ]
    operands = (hidden, wq, norm_gain.reshape(tiles, 1, LANES), norm_shift.reshape(tiles, 1, LANES), conv_bias.reshape(tiles, LANES))
    return pl.pallas_call(
        functools.partial(kernel, ny, nd),
        out_shape=pltpu.VMEM((FRAMES, ROWS * 2, 4, channels), BF16),
        in_specs=[HBM] * 5,
        out_specs=VMEM,
        scratch_shapes=scratch,
        compiler_params=pltpu.CompilerParams(collective_id=0, has_side_effects=True, vmem_limit_bytes=40 * MIB),
        name="decode",
    )(*(pltpu.with_memory_space_constraint(v, pltpu.HBM) for v in operands))


def solution(mesh):
    ny = len({d.coords[1] for d in mesh.devices.flat})
    return jax.shard_map(
        functools.partial(shards, ny),
        mesh=mesh,
        in_specs=(P(("groups", "space"), None), P(), P(), P(None, None, None, "space", None), P()),
        out_specs=P("groups", None, "space", None),
        check_vma=False,
    )
```

```python
import functools

import jax
import jax.numpy as jnp
from jax import lax
from jax.experimental import pallas as pl
from jax.experimental.pallas import tpu as pltpu
from jax.sharding import PartitionSpec as P

GROUP = 16
FRAMES = 4
ROWS = 16
LANES = 128
TEAM = 4
TAPS = 9
EPSILON = 1e-6
PARTS = (4, 4, 4, 4)
MIB = 1 << 20
YROWS = 40
TROWS = 24
NEAR = 6

DMA = pltpu.SemaphoreType.DMA
F32, BF16 = jnp.float32, jnp.bfloat16
SHIFTS = [(0, 0), (0, -1), (0, 1), (-1, 0), (1, 0), (-1, -1), (-1, 1), (1, -1), (1, 1)]


def phases_of(dr, dc):
    rows = {-1: (0,), 0: (0, 1), 1: (1,)}
    return [(a, b) for a in rows[dr] for b in rows[dc]]


COLUMNS = [(s, p) for s in SHIFTS for p in phases_of(*s)]


def remote(src, dst, send, recv, device):
    return pltpu.make_async_remote_copy(
        src_ref=src, dst_ref=dst, send_sem=send, recv_sem=recv,
        device_id=device, device_id_type=pl.DeviceIdType.MESH,
    )


def signal(sem, device):
    pl.semaphore_signal(sem, inc=1, device_id=device, device_id_type=pl.DeviceIdType.MESH)


def wait_bytes(ref, sem):
    pltpu.make_async_copy(ref, ref, sem).wait()


def team(ny):
    g = lax.axis_index("groups")
    x, y = g // ny, g % ny
    x0, y0 = x - x % 2, y - y % 2
    q = (x % 2) * 2 + y % 2
    others = (3 - q, (q + 2) % TEAM, q + 1 - 2 * (q % 2))
    return q, others, lambda p: (x0 + p // 2) * ny + y0 + p % 2


def group_matrix():
    lane = lax.broadcasted_iota(jnp.int32, (LANES, LANES), 0)
    packed = lax.broadcasted_iota(jnp.int32, (LANES, LANES), 1)
    return jnp.where(lane // GROUP == packed % 8, 1.0, 0.0).astype(F32)


def packed_mask(which):
    row = lax.broadcasted_iota(jnp.int32, (8, LANES), 0)
    lane = lax.broadcasted_iota(jnp.int32, (8, LANES), 1)
    return (lane // 32 == which) & ((lane // 8) % 4 == row % 4)


def hdot(a, b):
    return jnp.dot(a, b, preferred_element_type=F32, precision=lax.Precision.HIGHEST)


def pack(sums, which):
    return jnp.sum(jnp.where(packed_mask(which), hdot(sums, group_matrix()), 0.0), axis=0, keepdims=True)


def unpack(row, which):
    spread = jnp.where(packed_mask(which), jnp.broadcast_to(row, (8, LANES)), 0.0)
    return hdot(spread, group_matrix().T)


def rounds_of(half):
    known, steps = 1, []
    while known < half:
        step = min(known, max(1, half // 4))
        known += step
        steps.append((step, min(known, half)))
    return steps


def kernel(ny, nd, h_ref, wq_ref, gain_ref, shift_ref, bias_ref, out, gain, shift, bias,
           w, mix, acts, totals, raw, cells, flat, stats, row, tot, ys, a, acc, turn, mine,
           local, southsend, ringsend, ringrecv, give, giverecv, own, ask, a2asend, a2arecv,
           statsend, statrecv, partsend, partrecv, northsend, northrecv, edgesend, edgerecv, outersend, outerrecv, totsend, totrecv, outsend, outrecv):
    me = lax.axis_index("space")
    z, c = me // 2, me % 2
    nz = nd // 2
    half = nz // 2
    q, others, group_at = team(ny)
    leaps = (half - NEAR) // 2
    assert NEAR + 2 * leaps == half and leaps > 0
    rounds = rounds_of(half)
    spans, last = [], 0
    for known in [1] + [r[1] for r in rounds]:
        spans.append((last + 1, known))
        last = known
    sizes = [2 * (hi - lo + 1) - (1 if hi == half else 0) for lo, hi in spans]

    def at(zz, core):
        return {"space": lax.rem(zz + 2 * nz, nz) * 2 + core}

    sibling = {"space": z * 2 + 1 - c}
    middle = pl.ds(1, 4)
    norths = pl.ds(2, 3)
    barrier = pltpu.get_barrier_semaphore()

    def blend(zz):
        zz = lax.rem(zz + 2 * nz, nz)
        for dt in range(3):
            tap = [w[dt, pl.ds(zz * 2, 2), n].astype(F32).reshape(16, LANES) for n in range(TAPS)]

            def sums(x):
                return {(0, -1): x[0], (0, 0): x[1] + x[2], (1, 0): x[0] + x[1], (1, 1): x[2]}

            by_row = [sums([tap[n * 3 + e] for n in range(3)]) for e in range(3)]
            both = {k: sums([by_row[e][k] for e in range(3)]) for k in by_row[0]}
            for n, ((dr, dc), (pr, pc)) in enumerate(COLUMNS):
                mix[dt, pl.ds(pl.multiple_of(zz * 16, 16), 16), n * LANES:(n + 1) * LANES] = both[(pr, dr)][(pc, dc)].astype(BF16)

    channels = a.shape[-1]
    tiles = channels // LANES
    pairs = ROWS // 2

    def activate(places):
        g = jnp.concatenate([gain[t] for t in range(tiles)] * 2, axis=0)
        b = jnp.concatenate([shift[t] for t in range(tiles)] * 2, axis=0)
        for p in places:
            mean = unpack(totals[p], 0)
            scale = g * lax.rsqrt(unpack(totals[p], 1) + EPSILON)
            scale, move = scale * 0.5, b * 0.5

            @pl.loop(0, pairs, unroll=4)
            def _(rp):
                for f in range(FRAMES):
                    v = acts[p, lax.rem(f * pairs + rp + nz - z, nz), pl.ds(2 * c, 4)].astype(F32)
                    v = (v - mean[None]) * scale[None] + move[None]
                    v = v * jnp.tanh(v) + v
                    start = rp * (16 * YROWS) + (p * FRAMES + f) * YROWS
                    ys[pl.ds(pl.multiple_of(start, 8), 32)] = v.reshape(32, LANES)

    def arrange():
        @pl.loop(0, pairs)
        def _(rp):
            for col in range(4):
                for r in range(2):
                    for t in range(tiles):
                        v = ys[pl.ds(rp * (16 * YROWS) + col * 8 + r * tiles + t, 16, stride=YROWS)].astype(BF16)
                        a[rp * 2 + r + 1, col, :, t * LANES:(t + 1) * LANES] = v

        a[0] = a[1]
        a[ROWS + 1] = a[ROWS]

    chips = LANES // 16
    first_block = z // chips + jnp.where(z % chips < chips // 2, tiles - 1, 0)
    assert half - 4 >= chips * 3 // 2 - 1 and tiles == 4

    def multiply(row0, few, late):
        part = slice(row0 * 32, (row0 + few) * 32)
        blocks = [pl.ds(pl.multiple_of(lax.rem(first_block + 2 * late + i, tiles) * LANES, LANES), LANES) for i in range(2)]
        for dt in range(3):
            col0 = 0
            for dr, dc in SHIFTS:
                ps = phases_of(dr, dc)
                rows, cols = slice(1 + dr + row0, 1 + dr + row0 + few), slice(1 + dc, 3 + dc)
                lhs = jnp.concatenate([a[rows, cols, :, k].reshape(few * 2 * 16, LANES) for k in blocks], axis=1)
                rhs = jnp.concatenate([mix[dt, k, col0:col0 + len(ps) * LANES] for k in blocks], axis=0)
                r = jnp.dot(lhs, rhs, preferred_element_type=F32)
                col0 += len(ps) * LANES
                if (dr, dc) == (0, 0):
                    acc[dt, part] = acc[dt, part] + r if late else r
                else:
                    for n, (pr, pc) in enumerate(ps):
                        to = slice((pr * 2 + pc) * LANES, (pr * 2 + pc + 1) * LANES)
                        acc[dt, part, to] += r[:, n * LANES:(n + 1) * LANES]

    load = pltpu.make_async_copy(wq_ref.at[:, :, :, pl.ds(q * LANES, LANES)], w.at[:, me], local.at[0])
    rows_in = pltpu.make_async_copy(h_ref, raw.at[0], local.at[1])
    small = [pltpu.make_async_copy(src, dst, local.at[2 + i])
             for i, (src, dst) in enumerate(((gain_ref, gain), (shift_ref, shift), (bias_ref, bias)))]

    @pl.when(c == 1)
    def _():
        for d in (1, -1):
            for core in (1, 0):
                signal(barrier, at(z + d, core))
        signal(barrier, sibling)
        load.start()
        rows_in.start()
        for copy in small:
            copy.start()
        pl.semaphore_wait(barrier, 5)
        rows_in.wait()
        rows_out = remote(raw.at[0], raw.at[1], own.at[0, 0], own.at[1, 0], sibling)
        rows_out.start()
        load.wait()

        def piece(zz, j):
            return w.at[j, pl.ds(lax.rem(zz + 2 * nz, nz) * 2, 2)]

        def hop(way, p, d, j, step=1):
            to = z + step if way == 0 else z - step
            return remote(p, p, ringsend.at[way], ringrecv.at[way, d - 1, j], at(to, 1))

        def first(part, j):
            for way in (0, 1):
                hop(way, part, 1, j).start()

        for j in range(3):
            m = w.at[j, me]
            first(m, j)
            remote(m, m, give, giverecv.at[half], sibling).start()
        def take(way, d, j, s, on):
            p = piece(z - d if way == 0 else z + d, j)
            hop(way, p, d, j).wait_recv()
            for step in on:
                hop(way, p, d + step, j, step).start()
            remote(p, p, give, giverecv.at[s], sibling).start()

        @pl.loop(0, NEAR - 1)
        def _(s):
            for j in range(3):
                take(0, s + 1, j, s, (1,))
                take(1, s + 1, j, s, (1,))
            blend(z - s - 1)
            blend(z + s + 1)

        for j in range(3):
            theirs = w.at[j, z * 2]
            remote(theirs, theirs, own.at[0, 1 + j], own.at[1, 1 + j], sibling).wait_recv()
        blend(z)

        @pl.loop(0, leaps - 1)
        def _(u):
            d, s = NEAR + 2 * u, NEAR - 1 + u
            for j in range(3):
                take(0, d, j, s, (2,))
                take(1, d, j, s, (2,))
            for j in range(3):
                hop(0, piece(z - d, j), d + 1, j).start()
                hop(1, piece(z + d, j), d + 1, j).start()
            blend(z - d)
            blend(z + d)

            @pl.when(u == leaps - 2)
            def _():
                wait_bytes(acts.at[:, :, pl.ds(2, 3)], northrecv)
                remote(totals, totals, totsend.at[1], totrecv.at[1], sibling).wait_recv()

                @pl.when(z < nz - 1)
                def _():
                    wait_bytes(acts.at[:, :, 5], outerrecv)

                @pl.when(z == nz - 1)
                def _():
                    acts[:, :, 5] = acts[:, :, 4]

                for copy in small:
                    copy.wait()
                activate((0, 1))

            @pl.when(u > 0)
            def _():
                for j in range(3):
                    take(0, d - 1, j, s, ())
                    take(1, d - 1, j, s, ())
                blend(z - d + 1)
                blend(z + d - 1)

        activate((2, 3))
        arrange()
        d, s = half - 2, NEAR - 2 + leaps
        def side(way, zz):
            return w.at[1, pl.ds(lax.rem(zz + 2 * nz, nz) * 2, 2), pl.ds(0, 5) if way == 0 else pl.ds(5, 4)]

        for j in range(3):
            take(0, d, j, s, (2,) if j == 0 else ())
            take(1, d, j, s, (2,) if j == 2 else ())
            if j == 1:
                hop(0, side(0, z - d), half, j, 2).start()
                hop(1, side(1, z + d), half, j, 2).start()
        for j in range(3):
            hop(0, piece(z - d, j), d + 1, j).start()
            hop(1, piece(z + d, j), d + 1, j).start()
        blend(z - d)
        blend(z + d)
        for j in range(3):
            take(0, d - 1, j, s, ())
            take(1, d - 1, j, s, ())
        blend(z - d + 1)
        blend(z + d - 1)
        multiply(0, ROWS // 2, 0)
        multiply(ROWS // 2, ROWS // 2, 0)
        s = NEAR - 1 + leaps
        for j in range(3):
            take(0, half - 1, j, s, ())
            take(1, half - 1, j, s, ())
        blend(z - half + 1)
        blend(z + half - 1)
        take(0, half, 0, s + 1, ())
        for way in (0, 1):
            part = side(way, z + half)
            hop(way, part, half, 1).wait_recv()
            remote(part, part, give, giverecv.at[s + 1], sibling).start()
        take(1, half, 2, s + 1, ())
        blend(z + half)

    @pl.when(c == 0)
    def _():
        for d in (1, -1):
            for core in (1, 0):
                signal(barrier, at(z + d, core))
        signal(barrier, sibling)
        for p in others:
            signal(barrier, {"groups": group_at(p)})
        load.start()
        rows_in.start()
        for copy in small:
            copy.start()
        pl.semaphore_wait(barrier, 4 + TEAM)

        def tell(k):
            if k < len(rounds):
                signal(ask.at[k], at(z + rounds[k][0], 0))
                signal(ask.at[k], at(z - rounds[k][0], 0))

        tell(0)
        load.wait()
        for j in range(3):
            p = w.at[j, me]
            remote(p, p, southsend, ringrecv.at[0, 0, j], at(z + 1, 1)).start()
            remote(p, p, southsend, ringrecv.at[1, 0, j], at(z - 1, 1)).start()
        for j in range(3):
            p = w.at[j, me]
            remote(p, p, own.at[0, 1 + j], own.at[1, 1 + j], sibling).start()
        early = min(2, len(rounds))
        for k in range(early):
            pl.semaphore_wait(ask.at[k], 2)
            tell(k + 1)
        rows_in.wait()
        remote(raw.at[0], raw.at[1], own.at[0, 0], own.at[1, 0], sibling).wait_recv()

        wide = raw.shape[1]
        for r in range(2):
            for t in range(tiles):
                flat[pl.ds(r * tiles + t, wide, stride=8)] = raw[r, :, t * LANES:(t + 1) * LANES].astype(F32)
        x = flat[:wide * 8].reshape(wide, 8, LANES)
        cells[...] = x.astype(BF16)

        def each(b, body):
            lo, hi = spans[b]

            @pl.loop(lo, min(hi, half - 1) + 1)
            def _(d):
                body(d)
                body(-d)

            if hi == half:
                body(half)

        def runs(b):
            if b == len(spans):
                return [(0, 1)]
            lo, hi = spans[b]
            low = min(hi, half - 1)
            return [(lo, hi - lo + 1), (nz - low, low - lo + 1)]

        def for_chip(zz):
            return cells.at[pl.ds(zz * 4, 4)]

        def send_rows(b):
            def body(d):
                zz = lax.rem(z + d + nz, nz)
                remote(for_chip(zz), acts.at[q, lax.rem(nz - d, nz), middle], a2asend, a2arecv.at[b], at(zz, 0)).start()
            each(b, body)

        def send_stats(b):
            each(b, lambda d: remote(row, stats.at[z], statsend, statrecv, at(z + d, 0)).start())

        def pass_on(b, at0, n, rows, first, last):
            for p in others:
                remote(rows(middle), acts.at[q, pl.ds(at0, n), middle], partsend, partrecv.at[b], {"groups": group_at(p)}).start()

            @pl.when(z < nz - 1)
            def _():
                remote(last, acts.at[q, pl.ds((at0 + nz - 1) % nz, n), 0], edgesend.at[0], edgerecv.at[0, b], at(z + 1, 0)).start()

            @pl.when(z > 0)
            def _():
                remote(first, acts.at[q, pl.ds((at0 + 1) % nz, n), 5], edgesend.at[1], edgerecv.at[1, b], at(z - 1, 0)).start()

            remote(rows(norths), acts.at[q, pl.ds(at0, n), norths], northsend, northrecv, sibling).start()

        def share_edges(b):
            total = sum(n for _, n in runs(b))

            @pl.when(z > 0)
            def _():
                wait_bytes(acts.at[0, pl.ds(0, total), 0], edgerecv.at[0, b])
                for at0, n in runs(b):
                    e = acts.at[q, pl.ds((at0 + nz - 1) % nz, n), 0]
                    for p in others:
                        remote(e, e, outersend.at[0], outerrecv, {"groups": group_at(p)}).start()

            @pl.when(z < nz - 1)
            def _():
                wait_bytes(acts.at[0, pl.ds(0, total), 5], edgerecv.at[1, b])
                for at0, n in runs(b):
                    e = acts.at[q, pl.ds((at0 + 1) % nz, n), 5]
                    for p in others:
                        remote(e, e, outersend.at[1], outerrecv, {"groups": group_at(p), "space": z * 2 + 1}).start()
                    remote(e, e, outersend.at[1], outerrecv, sibling).start()

        acts[q, 0, 1:5] = cells[pl.ds(z * 4, 4)]
        for b in range(early + 1):
            send_rows(b)
        own_cells = len(spans)
        for p in others:
            remote(for_chip(z), acts.at[q, 0, middle], partsend, partrecv.at[own_cells], {"groups": group_at(p)}).start()
        remote(cells.at[pl.ds(z * 4 + 1, 3)], acts.at[q, 0, norths], northsend, northrecv, sibling).start()

        count = float(2 * wide * GROUP)
        first = pack(jnp.sum(flat[:wide * 8].reshape(wide, 8, LANES), axis=0), 0)
        mean = unpack(first, 0) * (1.0 / count)
        second = pack(jnp.sum((flat[:wide * 8].reshape(wide, 8, LANES) - mean[None]) ** 2, axis=0), 1)
        row[...] = first + second
        stats[z] = row[...]
        for b in range(early + 1):
            send_stats(b)

        for k in range(early, len(rounds)):
            pl.semaphore_wait(ask.at[k], 2)
            tell(k + 1)
            send_rows(k + 1)
            send_stats(k + 1)

        def from_team(b):
            total = sum(n for _, n in runs(b))
            wait_bytes(acts.at[pl.ds(0, TEAM - 1), pl.ds(0, total), middle], partrecv.at[b])
            for at0, n in runs(b):
                for p in others:
                    c3 = acts.at[p, pl.ds(at0, n), norths]
                    remote(c3, c3, northsend, northrecv, sibling).start()

        from_team(own_cells)

        @pl.when(z < nz - 1)
        def _():
            remote(cells.at[z * 4 + 3], acts.at[q, nz - 1, 0], edgesend.at[0], edgerecv.at[0, own_cells], at(z + 1, 0)).start()

        @pl.when(z > 0)
        def _():
            remote(cells.at[z * 4], acts.at[q, 1, 5], edgesend.at[1], edgerecv.at[1, own_cells], at(z - 1, 0)).start()

        share_edges(own_cells)
        for b in range(len(spans)):
            if b == len(spans) - 1:
                wait_bytes(stats.at[pl.ds(0, nz - 1)], statrecv)
                every = stats[...].reshape(nz, LANES)
                lane = lax.broadcasted_iota(jnp.int32, (nz, LANES), 1)
                mean = jnp.sum(every, axis=0, keepdims=True) * (1.0 / (count * nz))
                off = jnp.where(lane < 32, (every * (1.0 / count) - mean) ** 2 * count, 0.0)
                spread = jnp.where(lane < 32, 0.0, every)
                spread = jnp.sum(spread + pltpu.roll(off, 32, 1), axis=0, keepdims=True) * (1.0 / (count * nz))
                tot[...] = jnp.where(lane[:1] < 32, mean, spread)
                totals[q] = tot[...]
                for p in others:
                    remote(tot, totals.at[q], totsend.at[0], totrecv.at[0], {"groups": group_at(p)}).start()
            wait_bytes(acts.at[0, pl.ds(0, sizes[b]), middle], a2arecv.at[b])

            for at0, n in runs(b):
                pass_on(b, at0, n, lambda cols, at0=at0, n=n: acts.at[q, pl.ds(at0, n), cols],
                        acts.at[q, pl.ds(at0, n), 1], acts.at[q, pl.ds(at0, n), 4])
            if b > 0:
                share_edges(b - 1)

        wait_bytes(totals.at[pl.ds(0, TEAM - 1)], totrecv.at[0])
        remote(totals, totals, totsend.at[1], totrecv.at[1], sibling).start()
        for b in range(len(spans) - 1):
            from_team(b)
        share_edges(len(spans) - 1)
        from_team(len(spans) - 1)

        @pl.when(z > 0)
        def _():
            wait_bytes(acts.at[pl.ds(0, TEAM - 1), :, 0], outerrecv)

        @pl.when(z == 0)
        def _():
            acts[:, :, 0] = acts[:, :, 1]

        for copy in small:
            copy.wait()
        activate(range(TEAM))
        arrange()
        wait_bytes(w.at[:, 0], giverecv.at[half])
        blend(z)

        @pl.loop(0, NEAR - 1)
        def _(s):
            wait_bytes(w.at[:, pl.ds(0, 4)], giverecv.at[s])
            blend(z - s - 1)
            blend(z + s + 1)

        wait_bytes(w.at[:, pl.ds(0, 4)], giverecv.at[NEAR - 1])
        blend(z - NEAR)
        blend(z + NEAR)

        @pl.loop(1, leaps)
        def _(u):
            wait_bytes(w.at[:, pl.ds(0, 8)], giverecv.at[NEAR - 1 + u])
            for d in (0, -1):
                blend(z - NEAR - 2 * u - d)
                blend(z + NEAR + 2 * u + d)

            @pl.when(u >= leaps - 2)
            def _():
                @pl.when(u == leaps - 2)
                def _():
                    multiply(0, ROWS // 2, 0)

                @pl.when(u == leaps - 1)
                def _():
                    multiply(ROWS // 2, ROWS // 2, 0)

        wait_bytes(w.at[:, pl.ds(0, 4)], giverecv.at[NEAR - 1 + leaps])
        blend(z - half + 1)
        blend(z + half - 1)
        wait_bytes(w.at[:, pl.ds(0, 2)], giverecv.at[NEAR + leaps])
        blend(z + half)

    frame = lax.broadcasted_iota(jnp.int32, (8, LANES), 0) % FRAMES
    which = lax.broadcasted_iota(jnp.int32, (tiles, LANES), 0)
    bias_row = jnp.sum(jnp.where(which == q, bias[...].astype(F32), 0.0), axis=0, keepdims=True)
    row0 = 0
    for few in PARTS:
        multiply(row0, few, 1)
        for r in range(few):
            for cc in range(2):
                for n in range(4):
                    i = ((r * 2 + n // 2) * 2 + cc) * 2 + n % 2
                    for half_tile in range(2):
                        at_row = ((row0 + r) * 2 + cc) * 16 + half_tile * 8
                        old, mid, new = (acc[dt, at_row:at_row + 8, n * LANES:(n + 1) * LANES] for dt in range(3))
                        mid = jnp.where(frame >= 1, pltpu.roll(mid, 1, 0), mid)
                        old = jnp.where(frame >= 2, pltpu.roll(old, 2, 0), jnp.where(frame >= 1, pltpu.roll(old, 1, 0), old))
                        turn[i * TROWS + half_tile * 8:i * TROWS + half_tile * 8 + 8] = old + mid + new + bias_row
        put = slice(row0 * 2, (row0 + few) * 2)
        row0 += few
        for p in range(TEAM):
            for f in range(FRAMES):
                v = turn[pl.ds(p * FRAMES + f, few * 8, stride=TROWS)].astype(BF16)
                mine[p, f, put] = v.reshape(few * 2, 4, LANES)
        here = pl.ds(pl.multiple_of(q * LANES, LANES), LANES)
        out[:, put, :, here] = mine[q, :, put]
        for p in others:
            remote(mine.at[p, :, put], out.at[:, put, :, here], outsend, outrecv, {"groups": group_at(p)}).start()
    @pl.when(c == 1)
    def _():
        wait_bytes(raw.at[0], own.at[0, 0])
        wait_bytes(w.at[:, pl.ds(0, 2 * half - 2)], ringsend.at[0])
        wait_bytes(w.at[0, pl.ds(0, 1), pl.ds(0, 1)], ringsend.at[0])
        wait_bytes(w.at[:, pl.ds(0, 2 * half - 3)], ringsend.at[1])
        wait_bytes(w.at[0, pl.ds(0, 2)], ringsend.at[1])
        wait_bytes(w.at[0, pl.ds(0, 2), pl.ds(0, 4)], ringsend.at[1])
        wait_bytes(w.at[:, pl.ds(0, nd - 1)], give)

    @pl.when(c == 0)
    def _():
        for j in range(3):
            wait_bytes(w.at[j, me], own.at[0, 1 + j])
        wait_bytes(w.at[:, pl.ds(0, 2)], southsend)
        wait_bytes(stats.at[pl.ds(0, nz - 1)], statsend)
        wait_bytes(acts.at[0, pl.ds(0, nz - 1), middle], a2asend)
        wait_bytes(acts.at[pl.ds(0, TEAM - 1), :, middle], partsend)
        wait_bytes(acts.at[:, :, norths], northsend)

        @pl.when(z < nz - 1)
        def _():
            wait_bytes(acts.at[0, :, 0], edgesend.at[0])
            wait_bytes(acts.at[:, :, 5], outersend.at[1])

        @pl.when(z > 0)
        def _():
            wait_bytes(acts.at[0, :, 5], edgesend.at[1])
            wait_bytes(acts.at[pl.ds(0, TEAM - 1), :, 0], outersend.at[0])
        wait_bytes(totals.at[pl.ds(0, TEAM - 1)], totsend.at[0])
        wait_bytes(totals, totsend.at[1])

    wait_bytes(mine.at[pl.ds(0, TEAM - 1)], outrecv)
    wait_bytes(mine.at[pl.ds(0, TEAM - 1)], outsend)


VMEM = pl.BlockSpec(memory_space=pltpu.VMEM)
HBM = pl.BlockSpec(memory_space=pltpu.HBM)


def shards(ny, hidden, norm_gain, norm_shift, conv_weight, conv_bias):
    nd = lax.axis_size("space")
    nz = nd // 2
    wide, channels = hidden.shape
    tiles = channels // LANES
    cin = conv_weight.shape[3]
    batches = len(rounds_of(nz // 2)) + 1
    wq = conv_weight.reshape(3, TAPS, cin, conv_weight.shape[4])
    scratch = [pltpu.VMEM((tiles, 1, LANES), F32)] * 2 + [
        pltpu.VMEM((tiles, LANES), BF16),
        pltpu.VMEM((3, nd, TAPS, cin, LANES), BF16),
        pltpu.VMEM((3, channels, 16 * LANES), BF16),
        pltpu.VMEM((TEAM, nz, 6, 8, LANES), BF16),
        pltpu.VMEM((TEAM, 1, LANES), F32),
        pltpu.VMEM((2, wide, channels), BF16),
        pltpu.VMEM((wide, 8, LANES), BF16),
        pltpu.VMEM((wide * 8 + 8, LANES), F32),
        pltpu.VMEM((nz, 1, LANES), F32),
        pltpu.VMEM((1, LANES), F32),
        pltpu.VMEM((1, LANES), F32),
        pltpu.VMEM((ROWS // 2 * 16 * YROWS + YROWS, LANES), F32),
        pltpu.VMEM((ROWS + 2, 4, 16, channels), BF16),
        pltpu.VMEM((3, ROWS * 32, 4 * LANES), F32),
        pltpu.VMEM((max(PARTS) * 8 * TROWS + TROWS, LANES), F32),
        pltpu.VMEM((TEAM, FRAMES, ROWS * 2, 4, LANES), BF16),
        DMA((5,)), DMA, DMA((2,)), DMA((2, nz // 2, 3)), DMA, DMA((nz // 2 + 1,)), DMA((2, 4)),
        pltpu.SemaphoreType.REGULAR((max(1, batches - 1),)),
        DMA, DMA((batches,)), DMA, DMA, DMA, DMA((batches + 1,)), DMA, DMA, DMA((2,)), DMA((2, batches + 1)), DMA((2,)), DMA, DMA((2,)), DMA((2,)), DMA, DMA,
    ]
    operands = (hidden, wq, norm_gain.reshape(tiles, 1, LANES), norm_shift.reshape(tiles, 1, LANES), conv_bias.reshape(tiles, LANES))
    return pl.pallas_call(
        functools.partial(kernel, ny, nd),
        out_shape=pltpu.VMEM((FRAMES, ROWS * 2, 4, channels), BF16),
        in_specs=[HBM] * 5,
        out_specs=VMEM,
        scratch_shapes=scratch,
        compiler_params=pltpu.CompilerParams(collective_id=0, has_side_effects=True, vmem_limit_bytes=40 * MIB),
        name="decode",
    )(*(pltpu.with_memory_space_constraint(v, pltpu.HBM) for v in operands))


def solution(mesh):
    ny = len({d.coords[1] for d in mesh.devices.flat})
    return jax.shard_map(
        functools.partial(shards, ny),
        mesh=mesh,
        in_specs=(P(("groups", "space"), None), P(), P(), P(None, None, None, "space", None), P()),
        out_specs=P("groups", None, "space", None),
        check_vma=False,
    )
```
